8 devices in a mesh: pod: 1 (over z), dp: 2 (over y), tp: 4 (over x, core).
Axes of the slice: x: 2, y: 2, z: 1, core: 2. Of those that a mesh axis runs over, the one named last changes fastest.
Arguments:
- x_saved: bfloat16 [3072, 1024], P(('pod', 'dp'))
- h_saved: bfloat16 [3072, 1024], P(('pod', 'dp'))
- mean_one: float32 [3072], P(('pod', 'dp'))
- rstd_one: float32 [3072], P(('pod', 'dp'))
- mean_two: float32 [3072], P(('pod', 'dp'))
- rstd_two: float32 [3072], P(('pod', 'dp'))
- gain_one: bfloat16 [1024], replicated
- gain_two: bfloat16 [1024], replicated
- grad_y: bfloat16 [3072, 1024], P(('pod', 'dp'))
- w_qkv: bfloat16 [1024, 3, 16, 64], P(None, None, 'tp')
- w_proj: bfloat16 [16, 64, 1024], P('tp')
- w_up: bfloat16 [1024, 4096], P(None, 'tp')
- w_down: bfloat16 [4096, 1024], P('tp')
Outputs:
- output 1: bfloat16 [3072, 1024], P(('pod', 'dp'))
- output 2: bfloat16 [1024, 3, 16, 64], P('pod', None, 'tp')
- output 3: bfloat16 [16, 64, 1024], P(('pod', 'tp'))
- output 4: bfloat16 [1024, 4096], P('pod', 'tp')
- output 5: bfloat16 [4096, 1024], P(('pod', 'tp'))
All inputs are finite; a program needn't handle non-finite values.
Results may differ from the reference program's by a relative error of at most 0.017085.
Values are sent between devices in bfloat16 or wider.
A program may use at most 1 GiB of HBM per device.

```python
import math
import jax
import jax.numpy as jnp
from jax import lax

MODEL_DIM = 1024
NUM_HEADS = 16
FFN_DIM = 4096
TOKENS = 1536
DATA_WAYS = 2

HEAD_DIM = MODEL_DIM // NUM_HEADS
ROW_COUNT = DATA_WAYS * TOKENS
QK_GAIN = (2.0 * math.log(TOKENS)) ** 0.25
GELU_C = math.sqrt(2.0 / math.pi)


def saved_stats(rows_wide):
    row_mean = jnp.mean(rows_wide, axis=-1)
    row_var = jnp.mean(jnp.square(rows_wide - row_mean[:, None]), axis=-1)
    return row_mean, 1.0 / jnp.sqrt(row_var + 1e-5)


def setup_inputs(seed: int = 0, part: int = 0) -> dict:
    shared_keys = jax.random.split(jax.random.key(seed), 6)
    own_keys = jax.random.split(jax.random.fold_in(jax.random.key(seed + 1), part), 7)
    x_rows = jnp.exp(jax.random.uniform(own_keys[3], (ROW_COUNT, 1), jnp.float32, -0.7, 0.7))
    h_rows = jnp.exp(jax.random.uniform(own_keys[4], (ROW_COUNT, 1), jnp.float32, -0.7, 0.7))
    x_shift = 0.5 * jax.random.normal(own_keys[5], (ROW_COUNT, 1), jnp.float32)
    h_shift = 0.5 * jax.random.normal(own_keys[6], (ROW_COUNT, 1), jnp.float32)
    x_saved = (jax.random.normal(own_keys[0], (ROW_COUNT, MODEL_DIM), jnp.float32) * x_rows + x_shift).astype(jnp.bfloat16)
    h_saved = (jax.random.normal(own_keys[1], (ROW_COUNT, MODEL_DIM), jnp.float32) * h_rows + h_shift).astype(jnp.bfloat16)
    grad_y = jax.random.normal(own_keys[2], (ROW_COUNT, MODEL_DIM), jnp.float32).astype(jnp.bfloat16)
    mean_one, rstd_one = saved_stats(x_saved.astype(jnp.float32))
    mean_two, rstd_two = saved_stats(h_saved.astype(jnp.float32))
    gain_one = (1.0 + 0.3 * jax.random.normal(shared_keys[0], (MODEL_DIM,), jnp.float32)).astype(jnp.bfloat16)
    gain_two = (1.0 + 0.3 * jax.random.normal(shared_keys[1], (MODEL_DIM,), jnp.float32)).astype(jnp.bfloat16)
    qkv_scale = jnp.array([QK_GAIN, QK_GAIN, 1.0], jnp.float32)[None, :, None, None] * MODEL_DIM ** -0.5
    w_qkv = (jax.random.normal(shared_keys[2], (MODEL_DIM, 3, NUM_HEADS, HEAD_DIM), jnp.float32) * qkv_scale).astype(jnp.bfloat16)
    w_proj = (jax.random.normal(shared_keys[3], (NUM_HEADS, HEAD_DIM, MODEL_DIM), jnp.float32) * MODEL_DIM ** -0.5).astype(jnp.bfloat16)
    w_up = (jax.random.normal(shared_keys[4], (MODEL_DIM, FFN_DIM), jnp.float32) * MODEL_DIM ** -0.5).astype(jnp.bfloat16)
    w_down = (jax.random.normal(shared_keys[5], (FFN_DIM, MODEL_DIM), jnp.float32) * FFN_DIM ** -0.5).astype(jnp.bfloat16)
    return {'x_saved': x_saved, 'h_saved': h_saved, 'mean_one': mean_one, 'rstd_one': rstd_one,
            'mean_two': mean_two, 'rstd_two': rstd_two, 'gain_one': gain_one, 'gain_two': gain_two,
            'grad_y': grad_y, 'w_qkv': w_qkv, 'w_proj': w_proj, 'w_up': w_up, 'w_down': w_down}


def layer_norm(row_vals, row_mean, row_rstd, gain_vec):
    x_hat = (row_vals.astype(jnp.float32) - row_mean[:, None]) * row_rstd[:, None]
    return x_hat, (x_hat * gain_vec.astype(jnp.float32)).astype(jnp.bfloat16)


def norm_back(d_norm, x_hat, row_rstd, gain_vec):
    scaled = d_norm * gain_vec.astype(jnp.float32)
    scaled_mean = jnp.mean(scaled, axis=-1, keepdims=True)
    proj_mean = jnp.mean(scaled * x_hat, axis=-1, keepdims=True)
    return row_rstd[:, None] * (scaled - scaled_mean - x_hat * proj_mean)


def gelu_pair(pre_act):
    pre_wide = pre_act.astype(jnp.float32)
    tanh_val = jnp.tanh(GELU_C * (pre_wide + 0.044715 * pre_wide * pre_wide * pre_wide))
    gelu_val = 0.5 * pre_wide * (1.0 + tanh_val)
    gelu_slope = 0.5 * (1.0 + tanh_val) + 0.5 * pre_wide * (1.0 - tanh_val * tanh_val) * GELU_C * (1.0 + 0.134145 * pre_wide * pre_wide)
    return gelu_val, gelu_slope


def head_pass(head_in):
    qkv_head, dout_head = head_in
    q_head = qkv_head[:, 0]
    k_head = qkv_head[:, 1]
    v_head = qkv_head[:, 2]
    scores = jnp.dot(q_head, k_head.T, preferred_element_type=jnp.float32) * HEAD_DIM ** -0.5
    row_ids = lax.broadcasted_iota(jnp.int32, (TOKENS, TOKENS), 0)
    col_ids = lax.broadcasted_iota(jnp.int32, (TOKENS, TOKENS), 1)
    scores = jnp.where(col_ids <= row_ids, scores, -1e30)
    shifted = jnp.exp(scores - jnp.max(scores, axis=-1, keepdims=True))
    prob_mat = shifted / jnp.sum(shifted, axis=-1, keepdims=True)
    prob_lo = prob_mat.astype(jnp.bfloat16)
    head_out = jnp.dot(prob_lo, v_head, preferred_element_type=jnp.float32).astype(jnp.bfloat16)
    dv_head = jnp.dot(prob_lo.T, dout_head, preferred_element_type=jnp.float32).astype(jnp.bfloat16)
    d_probs = jnp.dot(dout_head, v_head.T, preferred_element_type=jnp.float32)
    d_scores = (prob_mat * (d_probs - jnp.sum(prob_mat * d_probs, axis=-1, keepdims=True)) * HEAD_DIM ** -0.5).astype(jnp.bfloat16)
    dq_head = jnp.dot(d_scores, k_head, preferred_element_type=jnp.float32).astype(jnp.bfloat16)
    dk_head = jnp.dot(d_scores.T, q_head, preferred_element_type=jnp.float32).astype(jnp.bfloat16)
    return head_out, jnp.stack([dq_head, dk_head, dv_head], axis=1)


def reference(x_saved, h_saved, mean_one, rstd_one, mean_two, rstd_two, gain_one, gain_two, grad_y, w_qkv, w_proj, w_up, w_down):
    qkv_wide = w_qkv.astype(jnp.float32)
    proj_wide = w_proj.astype(jnp.float32)

    def seq_pass(carry, seq_in):
        acc_qkv, acc_proj, acc_up, acc_down = carry
        x_seq, h_seq, mean_a, rstd_a, mean_b, rstd_b, dy_seq = seq_in
        hat_two, norm_two = layer_norm(h_seq, mean_b, rstd_b, gain_two)
        pre_act = jnp.dot(norm_two, w_up, preferred_element_type=jnp.float32).astype(jnp.bfloat16)
        gelu_val, gelu_slope = gelu_pair(pre_act)
        act_out = gelu_val.astype(jnp.bfloat16)
        d_pre = (jnp.dot(dy_seq, w_down.T, preferred_element_type=jnp.float32) * gelu_slope).astype(jnp.bfloat16)
        acc_up = acc_up + jnp.dot(norm_two.T, d_pre, preferred_element_type=jnp.float32)
        acc_down = acc_down + jnp.dot(act_out.T, dy_seq, preferred_element_type=jnp.float32)
        d_norm_two = jnp.dot(d_pre, w_up.T, preferred_element_type=jnp.float32)
        d_mid = dy_seq.astype(jnp.float32) + norm_back(d_norm_two, hat_two, rstd_b, gain_two)
        d_mid_lo = d_mid.astype(jnp.bfloat16)
        hat_one, norm_one = layer_norm(x_seq, mean_a, rstd_a, gain_one)
        qkv_heads = jnp.einsum('td,dche->tche', norm_one.astype(jnp.float32), qkv_wide).astype(jnp.bfloat16)
        d_attn = jnp.einsum('td,hed->the', d_mid_lo.astype(jnp.float32), proj_wide).astype(jnp.bfloat16)
        head_outs, head_grads = lax.map(head_pass, (jnp.moveaxis(qkv_heads, 2, 0), jnp.moveaxis(d_attn, 1, 0)))
        attn_out = jnp.moveaxis(head_outs, 0, 1)
        d_qkv = jnp.moveaxis(head_grads, 0, 2).astype(jnp.float32)
        acc_proj = acc_proj + jnp.einsum('the,td->hed', attn_out.astype(jnp.float32), d_mid_lo.astype(jnp.float32))
        acc_qkv = acc_qkv + jnp.einsum('td,tche->dche', norm_one.astype(jnp.float32), d_qkv)
        d_norm_one = jnp.einsum('tche,dche->td', d_qkv, qkv_wide)
        grad_x = (d_mid + norm_back(d_norm_one, hat_one, rstd_a, gain_one)).astype(jnp.bfloat16)
        return (acc_qkv, acc_proj, acc_up, acc_down), grad_x

    zero_sums = (jnp.zeros((MODEL_DIM, 3, NUM_HEADS, HEAD_DIM), jnp.float32),
                 jnp.zeros((NUM_HEADS, HEAD_DIM, MODEL_DIM), jnp.float32),
                 jnp.zeros((MODEL_DIM, FFN_DIM), jnp.float32),
                 jnp.zeros((FFN_DIM, MODEL_DIM), jnp.float32))
    seq_inputs = (x_saved.reshape(DATA_WAYS, TOKENS, MODEL_DIM), h_saved.reshape(DATA_WAYS, TOKENS, MODEL_DIM),
                  mean_one.reshape(DATA_WAYS, TOKENS), rstd_one.reshape(DATA_WAYS, TOKENS),
                  mean_two.reshape(DATA_WAYS, TOKENS), rstd_two.reshape(DATA_WAYS, TOKENS),
                  grad_y.reshape(DATA_WAYS, TOKENS, MODEL_DIM))
    grad_sums, grad_rows = lax.scan(seq_pass, zero_sums, seq_inputs)
    acc_qkv, acc_proj, acc_up, acc_down = grad_sums
    return (grad_rows.reshape(ROW_COUNT, MODEL_DIM), acc_qkv.astype(jnp.bfloat16), acc_proj.astype(jnp.bfloat16),
            acc_up.astype(jnp.bfloat16), acc_down.astype(jnp.bfloat16))
```

```python
import functools
import math

import jax
import jax.numpy as jnp
from jax import lax
from jax.experimental import pallas as pl
from jax.experimental.pallas import tpu as pltpu
from jax.sharding import PartitionSpec as P

GELU_C = math.sqrt(2.0 / math.pi)
F32 = jnp.float32
BF16 = jnp.bfloat16
NT = (((1,), (1,)), ((), ()))
TN = (((0,), (0,)), ((), ()))
BLK = 256


def layer_norm(row_vals, row_mean, row_rstd, gain_vec):
    x_hat = (row_vals.astype(F32) - row_mean[:, None]) * row_rstd[:, None]
    return x_hat, (x_hat * gain_vec.astype(F32)).astype(BF16)


def norm_back(d_norm, x_hat, row_rstd, gain_vec):
    scaled = d_norm * gain_vec.astype(F32)
    scaled_mean = jnp.mean(scaled, axis=-1, keepdims=True)
    proj_mean = jnp.mean(scaled * x_hat, axis=-1, keepdims=True)
    return row_rstd[:, None] * (scaled - scaled_mean - x_hat * proj_mean)


def gelu_pair(pre_act):
    pre_wide = pre_act.astype(F32)
    tanh_val = jnp.tanh(GELU_C * (pre_wide + 0.044715 * pre_wide * pre_wide * pre_wide))
    gelu_val = 0.5 * pre_wide * (1.0 + tanh_val)
    gelu_slope = 0.5 * (1.0 + tanh_val) + 0.5 * pre_wide * (1.0 - tanh_val * tanh_val) * GELU_C * (1.0 + 0.134145 * pre_wide * pre_wide)
    return gelu_val, gelu_slope


def fold_rows(op, tile):
    return op(tile.reshape(tile.shape[0] // 8, 8, tile.shape[1]), axis=0)


def attn_kernel(q_ref, k_ref, v_ref, do_ref, ot_ref, dqkv_ref, s_ref, dp_ref, dk_ref, dv_ref, kt_ref, vt_ref):
    step = pl.program_id(0)
    last = pl.num_programs(0) - 1
    qi = last - step

    @pl.when(step == 0)
    def _():
        dk_ref[...] = jnp.zeros_like(dk_ref)
        dv_ref[...] = jnp.zeros_like(dv_ref)
        kt_ref[...] = k_ref[...].T
        vt_ref[...] = v_ref[...].T

    lane = lax.broadcasted_iota(jnp.int32, (BLK, 128), 1)
    q_wide = q_ref[...].astype(F32) * 0.125
    do_wide = do_ref[...].astype(F32)
    qs, dos = [], []
    for h in range(2):
        keep = (lane < 64) if h == 0 else (lane >= 64)
        qs.append(jnp.where(keep, q_wide, 0.0).astype(BF16))
        dos.append(jnp.where(keep, do_wide, 0.0).astype(BF16))

    def score(j, top, masked):
        rows = pl.ds(pl.multiple_of(j * BLK, BLK), BLK)
        k_blk = k_ref[rows, :]
        out = []
        for h in range(2):
            tile = lax.dot_general(k_blk, qs[h], NT, preferred_element_type=F32)
            if masked:
                key = lax.broadcasted_iota(jnp.int32, (BLK, BLK), 0)
                qry = lax.broadcasted_iota(jnp.int32, (BLK, BLK), 1)
                tile = jnp.where(key <= qry, tile, -1e30)
            s_ref[h, rows, :] = tile
            out.append(jnp.maximum(top[h], fold_rows(jnp.max, tile)))
        return tuple(out)

    low = jnp.full((8, BLK), -1e30, F32)
    top = score(qi, (low, low), True)
    top = lax.fori_loop(0, qi, lambda j, t: score(j, t, False), top)
    top = [jnp.max(t, axis=0, keepdims=True) for t in top]

    def expo(j, tot):
        rows = pl.ds(pl.multiple_of(j * BLK, BLK), BLK)
        out = []
        for h in range(2):
            tile = jnp.exp(s_ref[h, rows, :] - top[h])
            s_ref[h, rows, :] = tile
            out.append(tot[h] + fold_rows(jnp.sum, tile))
        return tuple(out)

    zero8 = jnp.zeros((8, BLK), F32)
    tot = lax.fori_loop(0, qi + 1, expo, (zero8, zero8))
    inv = [1.0 / jnp.sum(t, axis=0, keepdims=True) for t in tot]

    def third(j, carry):
        proj, o_acc = carry
        rows = pl.ds(pl.multiple_of(j * BLK, BLK), BLK)
        v_blk = v_ref[rows, :]
        proj_new, o_new = [], []
        dv_add = None
        for h in range(2):
            prob = s_ref[h, rows, :] * inv[h]
            s_ref[h, rows, :] = prob
            prob_lo = prob.astype(BF16)
            d_prob = lax.dot_general(v_blk, dos[h], NT, preferred_element_type=F32)
            dp_ref[h, rows, :] = d_prob
            proj_new.append(proj[h] + fold_rows(jnp.sum, prob * d_prob))
            term = jnp.dot(prob_lo, dos[h], preferred_element_type=F32)
            dv_add = term if h == 0 else dv_add + term
            o_new.append(o_acc[h] + jnp.dot(vt_ref[h * 64:(h + 1) * 64, rows], prob_lo, preferred_element_type=F32))
        dv_ref[rows, :] += dv_add
        return tuple(proj_new), tuple(o_new)

    zero_t = jnp.zeros((64, BLK), F32)
    proj, o_acc = lax.fori_loop(0, qi + 1, third, ((zero8, zero8), (zero_t, zero_t)))
    for h in range(2):
        ot_ref[h * 64:(h + 1) * 64, :] = o_acc[h].astype(BF16)
    proj = [jnp.sum(t, axis=0, keepdims=True) for t in proj]

    def fourth(j, dq_acc):
        rows = pl.ds(pl.multiple_of(j * BLK, BLK), BLK)
        dq_new = []
        dk_add = None
        for h in range(2):
            d_s = (s_ref[h, rows, :] * (dp_ref[h, rows, :] - proj[h])).astype(BF16)
            term = jnp.dot(d_s, qs[h], preferred_element_type=F32)
            dk_add = term if h == 0 else dk_add + term
            dq_new.append(dq_acc[h] + jnp.dot(kt_ref[h * 64:(h + 1) * 64, rows], d_s, preferred_element_type=F32))
        dk_ref[rows, :] += dk_add
        return tuple(dq_new)

    dq = lax.fori_loop(0, qi + 1, fourth, (zero_t, zero_t))
    dq = jnp.concatenate([d * 0.125 for d in dq], axis=0)
    rows = pl.ds(pl.multiple_of(qi * BLK, BLK), BLK)
    dqkv_ref[rows, 0:128] = dq.T.astype(BF16)

    @pl.when(step == last)
    def _():
        dqkv_ref[:, 128:256] = dk_ref[...].astype(BF16)
        dqkv_ref[:, 256:384] = dv_ref[...].astype(BF16)


def attn_pair(pair, qkv, d_attn):
    toks = qkv.shape[0]
    steps = toks // BLK
    return pl.pallas_call(
        attn_kernel,
        grid=(steps,),
        in_specs=[pl.BlockSpec((BLK, 128), lambda s: (steps - 1 - s, pair)),
                  pl.BlockSpec((toks, 128), lambda s: (0, 2 + pair)),
                  pl.BlockSpec((toks, 128), lambda s: (0, 4 + pair)),
                  pl.BlockSpec((BLK, 128), lambda s: (steps - 1 - s, pair))],
        out_specs=[pl.BlockSpec((128, BLK), lambda s: (0, steps - 1 - s)),
                   pl.BlockSpec((toks, 384), lambda s: (0, 0))],
        out_shape=[jax.ShapeDtypeStruct((128, toks), BF16), jax.ShapeDtypeStruct((toks, 384), BF16)],
        scratch_shapes=[pltpu.VMEM((2, toks, BLK), F32), pltpu.VMEM((2, toks, BLK), F32),
                        pltpu.VMEM((toks, 128), F32), pltpu.VMEM((toks, 128), F32),
                        pltpu.VMEM((128, toks), BF16), pltpu.VMEM((128, toks), BF16)],
        compiler_params=pltpu.CompilerParams(dimension_semantics=("arbitrary",), vmem_limit_bytes=40 << 20),
        cost_estimate=pl.CostEstimate(flops=16 * 10**9, bytes_accessed=4 << 20, transcendentals=0),
        name=f"attn_pair{pair}",
    )(qkv, qkv, qkv, d_attn)


def mlp_kernel(na_ref, da_ref, nb_ref, db_ref, wu_ref, wd_ref, pu_hbm, pd_hbm, gu_ref, gd_ref, au_ref, ad_ref, pu_ref, pd_ref, sem):
    step = pl.program_id(0)
    half = pl.num_programs(0) // 2
    load_u = pltpu.make_async_copy(pu_hbm, pu_ref, sem.at[0])
    load_d = pltpu.make_async_copy(pd_hbm, pd_ref, sem.at[1])

    @pl.when(step == 0)
    def _():
        load_u.start()
        load_d.start()
        au_ref[...] = jnp.zeros_like(au_ref)
        ad_ref[...] = jnp.zeros_like(ad_ref)

    def rows_of(n_ref, d_ref):
        n_two = n_ref[...]
        d_y = d_ref[...]
        pre = jnp.dot(n_two, wu_ref[...], preferred_element_type=F32).astype(BF16)
        act, slope = gelu_pair(pre)
        d_act = lax.dot_general(d_y, wd_ref[...], NT, preferred_element_type=F32)
        d_pre = (d_act * slope).astype(BF16)
        au_ref[...] += lax.dot_general(n_two, d_pre, TN, preferred_element_type=F32)
        ad_ref[...] += lax.dot_general(act.astype(BF16), d_y, TN, preferred_element_type=F32)

    @pl.when(step < half)
    def _():
        rows_of(na_ref, da_ref)

    @pl.when(step >= half)
    def _():
        rows_of(nb_ref, db_ref)

    @pl.when(step == pl.num_programs(0) - 1)
    def _():
        load_u.wait()
        load_d.wait()
        gu_ref[...] = (au_ref[...] + pu_ref[...]).astype(BF16)
        gd_ref[...] = (ad_ref[...] + pd_ref[...]).astype(BF16)


def mlp_grad(n_a, d_a, n_b, d_b, w_up, w_down, part_up, part_down):
    rows, dim = n_a.shape
    cols = w_up.shape[1]
    blk = 384
    half = rows // blk
    first = pl.BlockSpec((blk, dim), lambda s: (jnp.minimum(s, half - 1), 0))
    second = pl.BlockSpec((blk, dim), lambda s: (jnp.maximum(s - half, 0), 0))
    whole_up = pl.BlockSpec((dim, cols), lambda s: (0, 0))
    whole_down = pl.BlockSpec((cols, dim), lambda s: (0, 0))
    return pl.pallas_call(
        mlp_kernel,
        grid=(2 * half,),
        in_specs=[first, first, second, second, whole_up, whole_down,
                  pl.BlockSpec(memory_space=pl.ANY), pl.BlockSpec(memory_space=pl.ANY)],
        out_specs=[whole_up, whole_down],
        out_shape=[jax.ShapeDtypeStruct((dim, cols), BF16), jax.ShapeDtypeStruct((cols, dim), BF16)],
        scratch_shapes=[pltpu.VMEM((dim, cols), F32), pltpu.VMEM((cols, dim), F32),
                        pltpu.VMEM((dim, cols), F32), pltpu.VMEM((cols, dim), F32),
                        pltpu.SemaphoreType.DMA((2,))],
        compiler_params=pltpu.CompilerParams(dimension_semantics=("arbitrary",), vmem_limit_bytes=60 << 20),
        cost_estimate=pl.CostEstimate(flops=16 * 10**9, bytes_accessed=24 << 20, transcendentals=0),
        name="mlp_grad",
    )(n_a, d_a, n_b, d_b, w_up, w_down, part_up, part_down)


def solution(mesh):
    row_spec = P(('pod', 'dp'), None)
    stat_spec = P(('pod', 'dp'))
    in_specs = (row_spec, row_spec, stat_spec, stat_spec, stat_spec, stat_spec, P(None), P(None), row_spec,
                P(None, None, 'tp', None), P('tp', None, None), P(None, 'tp'), P('tp', None))
    out_specs = (row_spec, P('pod', None, 'tp', None), P(('pod', 'tp'), None, None), P('pod', 'tp'), P(('pod', 'tp'), None))
    swap_core = functools.partial(lax.ppermute, axis_name='tp', perm=[(0, 1), (1, 0), (2, 3), (3, 2)])
    swap_x = functools.partial(lax.ppermute, axis_name='tp', perm=[(0, 2), (2, 0), (1, 3), (3, 1)])
    swap_dp = functools.partial(lax.ppermute, axis_name='dp', perm=[(0, 1), (1, 0)])

    def take_half(arr, which):
        rows = arr.shape[0] // 2
        return lax.dynamic_slice_in_dim(arr, which * rows, rows, 0)

    def join_halves(mine, other, which):
        return jnp.concatenate([jnp.where(which == 0, mine, other), jnp.where(which == 0, other, mine)], axis=0)

    def local_step(x_saved, h_saved, mean_one, rstd_one, mean_two, rstd_two, gain_one, gain_two, grad_y, w_qkv, w_proj, w_up, w_down):
        core = lax.axis_index('tp') % 2
        dp_idx = lax.axis_index('dp')
        dim = x_saved.shape[1]

        def reduce_rows(part):
            chip = (take_half(part, core).astype(F32) + swap_core(take_half(part, 1 - core)).astype(F32)).astype(BF16)
            return chip.astype(F32) + swap_x(chip).astype(F32)

        hat_two, norm_two = layer_norm(h_saved, mean_two, rstd_two, gain_two)
        norm_y, dy_y = swap_dp(take_half(norm_two, core)), swap_dp(take_half(grad_y, core))
        norm_c, dy_c = swap_core(norm_y), swap_core(dy_y)

        pre_act = jnp.dot(norm_two, w_up, preferred_element_type=F32).astype(BF16)
        gelu_val, gelu_slope = gelu_pair(pre_act)
        act_out = gelu_val.astype(BF16)
        d_act = lax.dot_general(grad_y, w_down, NT, preferred_element_type=F32)
        d_pre = (d_act * gelu_slope).astype(BF16)
        part_two = lax.dot_general(d_pre, w_up, NT, preferred_element_type=F32).astype(BF16)
        part_down = lax.dot_general(act_out, grad_y, TN, preferred_element_type=F32)
        part_up = lax.dot_general(norm_two, d_pre, TN, preferred_element_type=F32)

        w_t = w_qkv.transpose(1, 2, 3, 0).reshape(-1, dim)
        hat_one, norm_one = layer_norm(x_saved, mean_one, rstd_one, gain_one)
        qkv = lax.dot_general(norm_one, w_t, NT, preferred_element_type=F32).astype(BF16)

        h_half, r_half = take_half(h_saved, core), take_half(rstd_two, core)
        hat_half, _ = layer_norm(h_half, take_half(mean_two, core), r_half, gain_two)
        d_mid = take_half(grad_y, core).astype(F32) + norm_back(reduce_rows(part_two), hat_half, r_half, gain_two)
        mid_half = d_mid.astype(BF16)
        d_mid_lo = join_halves(mid_half, swap_core(mid_half), core)

        w_o = w_proj.reshape(-1, dim)
        d_attn = lax.dot_general(d_mid_lo, w_o, NT, preferred_element_type=F32).astype(BF16)

        w_pairs = w_t.reshape(3, 2, 128, dim)
        halves, part_one = [], None
        for pair in range(2):
            o_t, d_qkv = attn_pair(pair, qkv, d_attn)
            g_qkv = lax.dot_general(d_qkv, norm_one, TN, preferred_element_type=F32)
            g_o = jnp.dot(o_t, d_mid_lo, preferred_element_type=F32)
            mine, theirs = [], []
            for g in (g_qkv, g_o):
                mine.append(take_half(g, dp_idx))
                theirs.append(take_half(g, 1 - dp_idx))
            mine, theirs = jnp.concatenate(mine, 0), jnp.concatenate(theirs, 0)
            summed = (mine + swap_dp(theirs)).astype(BF16)
            other = swap_dp(summed)
            halves.append((join_halves(summed[:192], other[:192], dp_idx), join_halves(summed[192:], other[192:], dp_idx)))
            w_p = w_pairs[:, pair].reshape(-1, dim)
            term = jnp.dot(d_qkv, w_p, preferred_element_type=F32)
            part_one = term if pair == 0 else part_one + term
        g_t = jnp.stack([h[0].reshape(3, 2, 64, dim) for h in halves], axis=1).reshape(3, 4, 64, dim)
        grad_qkv = g_t.transpose(3, 0, 1, 2)
        grad_proj = jnp.concatenate([h[1] for h in halves], axis=0).reshape(4, 64, dim)

        x_half, r_one = take_half(x_saved, core), take_half(rstd_one, core)
        hat_x, _ = layer_norm(x_half, take_half(mean_one, core), r_one, gain_one)
        gx_half = (d_mid + norm_back(reduce_rows(part_one.astype(BF16)), hat_x, r_one, gain_one)).astype(BF16)
        grad_x = join_halves(gx_half, swap_core(gx_half), core)

        grad_up, grad_down = mlp_grad(norm_y, dy_y, norm_c, dy_c, w_up, w_down, part_up, part_down)
        return grad_x, grad_qkv, grad_proj, grad_up, grad_down

    return jax.shard_map(local_step, mesh=mesh, in_specs=in_specs, out_specs=out_specs, check_vma=False)
```

```python
import functools
import math

import jax
import jax.numpy as jnp
from jax import lax
from jax.experimental import pallas as pl
from jax.experimental.pallas import tpu as pltpu
from jax.sharding import PartitionSpec as P


GELU_C = math.sqrt(2.0 / math.pi)
F32 = jnp.float32
BF16 = jnp.bfloat16
NT = (((1,), (1,)), ((), ()))
TN = (((0,), (0,)), ((), ()))
BLK = 256


def layer_norm(row_vals, row_mean, row_rstd, gain_vec):
    x_hat = (row_vals.astype(F32) - row_mean[:, None]) * row_rstd[:, None]
    return x_hat, (x_hat * gain_vec.astype(F32)).astype(BF16)


def norm_back(d_norm, x_hat, row_rstd, gain_vec):
    scaled = d_norm * gain_vec.astype(F32)
    scaled_mean = jnp.mean(scaled, axis=-1, keepdims=True)
    proj_mean = jnp.mean(scaled * x_hat, axis=-1, keepdims=True)
    return row_rstd[:, None] * (scaled - scaled_mean - x_hat * proj_mean)


def gelu_pair(pre_act):
    pre_wide = pre_act.astype(F32)
    tanh_val = jnp.tanh(GELU_C * (pre_wide + 0.044715 * pre_wide * pre_wide * pre_wide))
    gelu_val = 0.5 * pre_wide * (1.0 + tanh_val)
    gelu_slope = 0.5 * (1.0 + tanh_val) + 0.5 * pre_wide * (1.0 - tanh_val * tanh_val) * GELU_C * (1.0 + 0.134145 * pre_wide * pre_wide)
    return gelu_val, gelu_slope


def fold_rows(op, tile):
    return op(tile.reshape(tile.shape[0] // 8, 8, tile.shape[1]), axis=0)


def attn_kernel(q_ref, k_ref, v_ref, do_ref, ot_ref, dqkv_ref, s_ref, dp_ref, dk_ref, dv_ref, kt_ref, vt_ref):
    step = pl.program_id(0)
    last = pl.num_programs(0) - 1
    qi = last - step

    @pl.when(step == 0)
    def _():
        dk_ref[...] = jnp.zeros_like(dk_ref)
        dv_ref[...] = jnp.zeros_like(dv_ref)
        kt_ref[...] = k_ref[...].T
        vt_ref[...] = v_ref[...].T

    lane = lax.broadcasted_iota(jnp.int32, (BLK, 128), 1)
    q_wide = q_ref[...].astype(F32) * 0.125
    do_wide = do_ref[...].astype(F32)
    qs, dos = [], []
    for h in range(2):
        keep = (lane < 64) if h == 0 else (lane >= 64)
        qs.append(jnp.where(keep, q_wide, 0.0).astype(BF16))
        dos.append(jnp.where(keep, do_wide, 0.0).astype(BF16))

    def score(j, top, masked):
        rows = pl.ds(pl.multiple_of(j * BLK, BLK), BLK)
        k_blk = k_ref[rows, :]
        out = []
        for h in range(2):
            tile = lax.dot_general(k_blk, qs[h], NT, preferred_element_type=F32)
            if masked:
                key = lax.broadcasted_iota(jnp.int32, (BLK, BLK), 0)
                qry = lax.broadcasted_iota(jnp.int32, (BLK, BLK), 1)
                tile = jnp.where(key <= qry, tile, -1e30)
            s_ref[h, rows, :] = tile
            out.append(jnp.maximum(top[h], fold_rows(jnp.max, tile)))
        return tuple(out)

    low = jnp.full((8, BLK), -1e30, F32)
    top = score(qi, (low, low), True)
    top = lax.fori_loop(0, qi, lambda j, t: score(j, t, False), top)
    top = [jnp.max(t, axis=0, keepdims=True) for t in top]

    def expo(j, tot):
        rows = pl.ds(pl.multiple_of(j * BLK, BLK), BLK)
        out = []
        for h in range(2):
            tile = jnp.exp(s_ref[h, rows, :] - top[h])
            s_ref[h, rows, :] = tile
            out.append(tot[h] + fold_rows(jnp.sum, tile))
        return tuple(out)

    zero8 = jnp.zeros((8, BLK), F32)
    tot = lax.fori_loop(0, qi + 1, expo, (zero8, zero8))
    inv = [1.0 / jnp.sum(t, axis=0, keepdims=True) for t in tot]

    def third(j, carry):
        proj, o_acc = carry
        rows = pl.ds(pl.multiple_of(j * BLK, BLK), BLK)
        v_blk = v_ref[rows, :]
        proj_new, o_new = [], []
        dv_add = None
        for h in range(2):
            prob = s_ref[h, rows, :] * inv[h]
            s_ref[h, rows, :] = prob
            prob_lo = prob.astype(BF16)
            d_prob = lax.dot_general(v_blk, dos[h], NT, preferred_element_type=F32)
            dp_ref[h, rows, :] = d_prob
            proj_new.append(proj[h] + fold_rows(jnp.sum, prob * d_prob))
            term = jnp.dot(prob_lo, dos[h], preferred_element_type=F32)
            dv_add = term if h == 0 else dv_add + term
            o_new.append(o_acc[h] + jnp.dot(vt_ref[h * 64:(h + 1) * 64, rows], prob_lo, preferred_element_type=F32))
        dv_ref[rows, :] += dv_add
        return tuple(proj_new), tuple(o_new)

    zero_t = jnp.zeros((64, BLK), F32)
    proj, o_acc = lax.fori_loop(0, qi + 1, third, ((zero8, zero8), (zero_t, zero_t)))
    for h in range(2):
        ot_ref[h * 64:(h + 1) * 64, :] = o_acc[h].astype(BF16)
    proj = [jnp.sum(t, axis=0, keepdims=True) for t in proj]

    def fourth(j, dq_acc):
        rows = pl.ds(pl.multiple_of(j * BLK, BLK), BLK)
        dq_new = []
        dk_add = None
        for h in range(2):
            d_s = (s_ref[h, rows, :] * (dp_ref[h, rows, :] - proj[h])).astype(BF16)
            term = jnp.dot(d_s, qs[h], preferred_element_type=F32)
            dk_add = term if h == 0 else dk_add + term
            dq_new.append(dq_acc[h] + jnp.dot(kt_ref[h * 64:(h + 1) * 64, rows], d_s, preferred_element_type=F32))
        dk_ref[rows, :] += dk_add
        return tuple(dq_new)

    dq = lax.fori_loop(0, qi + 1, fourth, (zero_t, zero_t))
    dq = jnp.concatenate([d * 0.125 for d in dq], axis=0)
    rows = pl.ds(pl.multiple_of(qi * BLK, BLK), BLK)
    dqkv_ref[rows, 0:128] = dq.T.astype(BF16)

    @pl.when(step == last)
    def _():
        dqkv_ref[:, 128:256] = dk_ref[...].astype(BF16)
        dqkv_ref[:, 256:384] = dv_ref[...].astype(BF16)


def attn_pair(pair, qkv, d_attn):
    toks = qkv.shape[0]
    steps = toks // BLK
    return pl.pallas_call(
        attn_kernel,
        grid=(steps,),
        in_specs=[pl.BlockSpec((BLK, 128), lambda s: (steps - 1 - s, pair)),
                  pl.BlockSpec((toks, 128), lambda s: (0, 2 + pair)),
                  pl.BlockSpec((toks, 128), lambda s: (0, 4 + pair)),
                  pl.BlockSpec((BLK, 128), lambda s: (steps - 1 - s, pair))],
        out_specs=[pl.BlockSpec((128, BLK), lambda s: (0, steps - 1 - s)),
                   pl.BlockSpec((toks, 384), lambda s: (0, 0))],
        out_shape=[jax.ShapeDtypeStruct((128, toks), BF16), jax.ShapeDtypeStruct((toks, 384), BF16)],
        scratch_shapes=[pltpu.VMEM((2, toks, BLK), F32), pltpu.VMEM((2, toks, BLK), F32),
                        pltpu.VMEM((toks, 128), F32), pltpu.VMEM((toks, 128), F32),
                        pltpu.VMEM((128, toks), BF16), pltpu.VMEM((128, toks), BF16)],
        compiler_params=pltpu.CompilerParams(dimension_semantics=("arbitrary",), vmem_limit_bytes=40 << 20),
        cost_estimate=pl.CostEstimate(flops=16 * 10**9, bytes_accessed=4 << 20, transcendentals=0),
    )(qkv, qkv, qkv, d_attn)


def mlp_kernel(na_ref, da_ref, nb_ref, db_ref, wu_ref, wd_ref, pu_hbm, pd_hbm, gu_ref, gd_ref, au_ref, ad_ref, pu_ref, pd_ref, sem):
    step = pl.program_id(0)
    half = pl.num_programs(0) // 2
    load_u = pltpu.make_async_copy(pu_hbm, pu_ref, sem.at[0])
    load_d = pltpu.make_async_copy(pd_hbm, pd_ref, sem.at[1])

    @pl.when(step == 0)
    def _():
        load_u.start()
        load_d.start()
        au_ref[...] = jnp.zeros_like(au_ref)
        ad_ref[...] = jnp.zeros_like(ad_ref)

    def rows_of(n_ref, d_ref):
        n_two = n_ref[...]
        d_y = d_ref[...]
        pre = jnp.dot(n_two, wu_ref[...], preferred_element_type=F32).astype(BF16)
        act, slope = gelu_pair(pre)
        d_act = lax.dot_general(d_y, wd_ref[...], NT, preferred_element_type=F32)
        d_pre = (d_act * slope).astype(BF16)
        au_ref[...] += lax.dot_general(n_two, d_pre, TN, preferred_element_type=F32)
        ad_ref[...] += lax.dot_general(act.astype(BF16), d_y, TN, preferred_element_type=F32)

    @pl.when(step < half)
    def _():
        rows_of(na_ref, da_ref)

    @pl.when(step >= half)
    def _():
        rows_of(nb_ref, db_ref)

    @pl.when(step == pl.num_programs(0) - 1)
    def _():
        load_u.wait()
        load_d.wait()
        gu_ref[...] = (au_ref[...] + pu_ref[...]).astype(BF16)
        gd_ref[...] = (ad_ref[...] + pd_ref[...]).astype(BF16)


def mlp_grad(n_a, d_a, n_b, d_b, w_up, w_down, part_up, part_down):
    rows, dim = n_a.shape
    cols = w_up.shape[1]
    blk = 384
    half = rows // blk
    first = pl.BlockSpec((blk, dim), lambda s: (jnp.minimum(s, half - 1), 0))
    second = pl.BlockSpec((blk, dim), lambda s: (jnp.maximum(s - half, 0), 0))
    whole_up = pl.BlockSpec((dim, cols), lambda s: (0, 0))
    whole_down = pl.BlockSpec((cols, dim), lambda s: (0, 0))
    return pl.pallas_call(
        mlp_kernel,
        grid=(2 * half,),
        in_specs=[first, first, second, second, whole_up, whole_down,
                  pl.BlockSpec(memory_space=pl.ANY), pl.BlockSpec(memory_space=pl.ANY)],
        out_specs=[whole_up, whole_down],
        out_shape=[jax.ShapeDtypeStruct((dim, cols), BF16), jax.ShapeDtypeStruct((cols, dim), BF16)],
        scratch_shapes=[pltpu.VMEM((dim, cols), F32), pltpu.VMEM((cols, dim), F32),
                        pltpu.VMEM((dim, cols), F32), pltpu.VMEM((cols, dim), F32),
                        pltpu.SemaphoreType.DMA((2,))],
        compiler_params=pltpu.CompilerParams(dimension_semantics=("arbitrary",), vmem_limit_bytes=60 << 20),
        cost_estimate=pl.CostEstimate(flops=16 * 10**9, bytes_accessed=24 << 20, transcendentals=0),
        name="mlp_grad",
    )(n_a, d_a, n_b, d_b, w_up, w_down, part_up, part_down)


def solution(mesh):
    row_spec = P(('pod', 'dp'), None)
    stat_spec = P(('pod', 'dp'))
    in_specs = (row_spec, row_spec, stat_spec, stat_spec, stat_spec, stat_spec, P(None), P(None), row_spec,
                P(None, None, 'tp', None), P('tp', None, None), P(None, 'tp'), P('tp', None))
    out_specs = (row_spec, P('pod', None, 'tp', None), P(('pod', 'tp'), None, None), P('pod', 'tp'), P(('pod', 'tp'), None))
    swap_core = functools.partial(lax.ppermute, axis_name='tp', perm=[(0, 1), (1, 0), (2, 3), (3, 2)])
    swap_x = functools.partial(lax.ppermute, axis_name='tp', perm=[(0, 2), (2, 0), (1, 3), (3, 1)])
    swap_dp = functools.partial(lax.ppermute, axis_name='dp', perm=[(0, 1), (1, 0)])

    def take_half(arr, which):
        rows = arr.shape[0] // 2
        return lax.dynamic_slice_in_dim(arr, which * rows, rows, 0)

    def join_halves(mine, other, which):
        return jnp.concatenate([jnp.where(which == 0, mine, other), jnp.where(which == 0, other, mine)], axis=0)

    def inner(x_saved, h_saved, mean_one, rstd_one, mean_two, rstd_two, gain_one, gain_two, grad_y, w_qkv, w_proj, w_up, w_down):
        core = lax.axis_index('tp') % 2
        dp_idx = lax.axis_index('dp')
        dim = x_saved.shape[1]

        def reduce_rows(part):
            chip = (take_half(part, core).astype(F32) + swap_core(take_half(part, 1 - core)).astype(F32)).astype(BF16)
            return chip.astype(F32) + swap_x(chip).astype(F32)

        _, norm_two = layer_norm(h_saved, mean_two, rstd_two, gain_two)
        norm_y, dy_y = swap_dp(take_half(norm_two, core)), swap_dp(take_half(grad_y, core))
        norm_c, dy_c = swap_core(norm_y), swap_core(dy_y)

        pre_act = jnp.dot(norm_two, w_up, preferred_element_type=F32).astype(BF16)
        gelu_val, gelu_slope = gelu_pair(pre_act)
        act_out = gelu_val.astype(BF16)
        d_act = lax.dot_general(grad_y, w_down, NT, preferred_element_type=F32)
        d_pre = (d_act * gelu_slope).astype(BF16)
        part_two = lax.dot_general(d_pre, w_up, NT, preferred_element_type=F32).astype(BF16)
        part_down = lax.dot_general(act_out, grad_y, TN, preferred_element_type=F32)
        part_up = lax.dot_general(norm_two, d_pre, TN, preferred_element_type=F32)

        w_t = w_qkv.transpose(1, 2, 3, 0).reshape(-1, dim)
        _, norm_one = layer_norm(x_saved, mean_one, rstd_one, gain_one)
        qkv = lax.dot_general(norm_one, w_t, NT, preferred_element_type=F32).astype(BF16)

        h_half, r_half = take_half(h_saved, core), take_half(rstd_two, core)
        hat_half, _ = layer_norm(h_half, take_half(mean_two, core), r_half, gain_two)
        d_mid = take_half(grad_y, core).astype(F32) + norm_back(reduce_rows(part_two), hat_half, r_half, gain_two)
        mid_half = d_mid.astype(BF16)
        d_mid_lo = join_halves(mid_half, swap_core(mid_half), core)

        w_o = w_proj.reshape(-1, dim)
        d_attn = lax.dot_general(d_mid_lo, w_o, NT, preferred_element_type=F32).astype(BF16)

        w_pairs = w_t.reshape(3, 2, 128, dim)
        halves, part_one = [], None
        for pair in range(2):
            o_t, d_qkv = attn_pair(pair, qkv, d_attn)
            g_qkv = lax.dot_general(d_qkv, norm_one, TN, preferred_element_type=F32)
            g_o = jnp.dot(o_t, d_mid_lo, preferred_element_type=F32)
            mine, theirs = [], []
            for g in (g_qkv, g_o):
                mine.append(take_half(g, dp_idx))
                theirs.append(take_half(g, 1 - dp_idx))
            mine, theirs = jnp.concatenate(mine, 0), jnp.concatenate(theirs, 0)
            summed = (mine + swap_dp(theirs)).astype(BF16)
            other = swap_dp(summed)
            halves.append((join_halves(summed[:192], other[:192], dp_idx), join_halves(summed[192:], other[192:], dp_idx)))
            w_p = w_pairs[:, pair].reshape(-1, dim)
            term = jnp.dot(d_qkv, w_p, preferred_element_type=F32)
            part_one = term if pair == 0 else part_one + term
        g_t = jnp.stack([h[0].reshape(3, 2, 64, dim) for h in halves], axis=1).reshape(3, 4, 64, dim)
        grad_qkv = g_t.transpose(3, 0, 1, 2)
        grad_proj = jnp.concatenate([h[1] for h in halves], axis=0).reshape(4, 64, dim)

        x_half, r_one = take_half(x_saved, core), take_half(rstd_one, core)
        hat_x, _ = layer_norm(x_half, take_half(mean_one, core), r_one, gain_one)
        gx_half = (d_mid + norm_back(reduce_rows(part_one.astype(BF16)), hat_x, r_one, gain_one)).astype(BF16)
        grad_x = join_halves(gx_half, swap_core(gx_half), core)

        grad_up, grad_down = mlp_grad(norm_y, dy_y, norm_c, dy_c, w_up, w_down, part_up, part_down)
        return grad_x, grad_qkv, grad_proj, grad_up, grad_down

    return jax.shard_map(inner, mesh=mesh, in_specs=in_specs, out_specs=out_specs, check_vma=False)
```

```python
import functools
import math

import jax
import jax.numpy as jnp
from jax import lax
from jax.experimental import pallas as pl
from jax.experimental.pallas import tpu as pltpu
from jax.sharding import PartitionSpec as P


GELU_C = math.sqrt(2.0 / math.pi)
F32 = jnp.float32
BF16 = jnp.bfloat16
NT = (((1,), (1,)), ((), ()))
TN = (((0,), (0,)), ((), ()))
BLK = 256
HI, LO = (4, 1), (0, 2)


def dot(a, b, dims=(((1,), (0,)), ((), ()))):
    return lax.dot_general(a, b, dims, preferred_element_type=F32)


def norm_back(d_norm, x_hat, row_rstd, gain_row):
    scaled = d_norm * gain_row
    scaled_mean = jnp.mean(scaled, axis=-1, keepdims=True)
    proj_mean = jnp.mean(scaled * x_hat, axis=-1, keepdims=True)
    return row_rstd * (scaled - scaled_mean - x_hat * proj_mean)


def gelu_pair(pre_act):
    pre_wide = pre_act.astype(F32)
    square = pre_wide * pre_wide
    tanh_val = jnp.tanh(pre_wide * (GELU_C + (GELU_C * 0.044715) * square))
    half = 0.5 + 0.5 * tanh_val
    gelu_slope = half + (0.5 * pre_wide) * (1.0 - tanh_val * tanh_val) * (GELU_C + (GELU_C * 0.134145) * square)
    return pre_wide * half, gelu_slope


def fold_rows(op, tile):
    return op(tile.reshape(tile.shape[0] // 8, 8, tile.shape[1]), axis=0)


def call(kernel, grid, in_specs, out_specs, out_shape, args, scratch=(), flops=1, vmem=60, aliases=None):
    return pl.pallas_call(
        kernel,
        grid_spec=pltpu.PrefetchScalarGridSpec(num_scalar_prefetch=1, grid=grid, in_specs=in_specs, out_specs=out_specs,
                                               scratch_shapes=list(scratch)),
        out_shape=out_shape,
        input_output_aliases=aliases or {},
        compiler_params=pltpu.CompilerParams(dimension_semantics=("arbitrary",) * len(grid), vmem_limit_bytes=vmem << 20),
        cost_estimate=pl.CostEstimate(flops=int(flops * 10**9), bytes_accessed=4 << 20, transcendentals=0),
    )(*args)


def whole(arr):
    return pl.BlockSpec(arr.shape, lambda s, ids: (0,) * arr.ndim)


def shape(dims, dtype=BF16):
    return jax.ShapeDtypeStruct(dims, dtype)


def theirs_first(s, n, core):
    return 2 * lax.rem(s, n) + lax.rem(1 + s // n + core, 2)


def mlp_kernel(n, ids, n_ref, dy_ref, wu_ref, wd_ref, *rest):
    g_ref, da_ref, send_ref, keep_ref = rest[-4:]
    n_two, d_y = n_ref[...], dy_ref[...]
    for c in range(0, wu_ref.shape[1], BLK):
        cols = slice(c, c + BLK)
        act, slope = gelu_pair(dot(n_two, wu_ref[:, cols]).astype(BF16))
        g_ref[:, cols] = act.astype(BF16)
        da_ref[:, cols] = (dot(d_y, wd_ref[cols, :], NT) * slope).astype(BF16)
    part = dot(da_ref[...], wu_ref[...], NT).astype(BF16)
    step = pl.program_id(0)

    @pl.when(step < n)
    def _():
        send_ref[...] = part

    @pl.when(step >= n)
    def _():
        keep_ref[...] = part


def mlp_part(chunk, ids, norm_two, grad_y, w_up, w_down, prev):
    base, n = chunk
    dim = norm_two.shape[1]
    rows = pl.BlockSpec((BLK, dim), lambda s, ids: (base + theirs_first(s, n, ids[0]), 0))
    blk_send = pl.BlockSpec((BLK, dim), lambda s, ids: (jnp.minimum(s, n - 1), 0))
    blk_keep = pl.BlockSpec((BLK, dim), lambda s, ids: (jnp.maximum(s - n, 0), 0))
    part = shape((n * BLK, dim))
    return call(functools.partial(mlp_kernel, n), (2 * n,),
                [rows, rows, whole(w_up), whole(w_down)] + [pl.BlockSpec(memory_space=pl.ANY)] * len(prev),
                [rows, rows, blk_send, blk_keep], [shape(norm_two.shape), shape(norm_two.shape), part, part],
                (ids, norm_two, grad_y, w_up, w_down) + prev, flops=3.2 * n,
                aliases={5: 0, 6: 1} if prev else None)


def mid_kernel(ids, chip_ref, recv_ref, row_ref, stat_ref, gain_ref, add_ref, *outs, col):
    d_norm = chip_ref[...].astype(F32) + recv_ref[...].astype(F32)
    rstd = stat_ref[:, col + 1:col + 2]
    x_hat = (row_ref[...].astype(F32) - stat_ref[:, col:col + 1]) * rstd
    d_row = add_ref[...].astype(F32) + norm_back(d_norm, x_hat, rstd, gain_ref[...].astype(F32))
    for out in outs:
        out[...] = d_row.astype(out.dtype)


def mid_part(chunk, ids, chip, recv, row_vals, stats, col, gain, add, add_local, out_types):
    base, n = chunk
    dim, sub = chip.shape[1], 128
    per = BLK // sub
    local = pl.BlockSpec((sub, dim), lambda s, ids: (s, 0))
    at = lambda s, ids: ((base + 2 * (s // per) + ids[0]) * per + lax.rem(s, per), 0)
    rows = pl.BlockSpec((sub, dim), at)
    return call(functools.partial(mid_kernel, col=col), (n * per,),
                [local, local, rows, pl.BlockSpec((sub, stats.shape[1]), at), whole(gain), local if add_local else rows],
                [local] * len(out_types), [shape(chip.shape, t) for t in out_types],
                (ids, chip, recv, row_vals, stats, gain, add), flops=0.4 * n)


def attn_kernel(base, n, ids, q_ref, k_ref, v_ref, own_ref, oth_ref, wo_ref, *rest):
    first = base > 0
    if first:
        ot_ref, dqkv_ref, dk_out, dv_out = rest[:4]
        do_ref, s_ref, dp_ref, dk_ref, dv_ref, kt_ref, vt_ref = rest[4:]
    else:
        dk_in, dv_in, ot_ref, dqkv_ref = rest[:4]
        do_ref, s_ref, dp_ref, dk_ref, dv_ref, kt_ref, vt_ref = rest[4:]
    step = pl.program_id(0)
    lb = theirs_first(step, n, 1 - ids[0])
    qi = base + lb

    @pl.when(step == 0)
    def _():
        if first:
            dk_ref[...] = jnp.zeros_like(dk_ref)
            dv_ref[...] = jnp.zeros_like(dv_ref)
        else:
            dk_ref[...] = dk_in[...]
            dv_ref[...] = dv_in[...]
        kt_ref[...] = k_ref[...].T
        vt_ref[...] = v_ref[...].T

    @pl.when(step < n)
    def _():
        do_ref[...] = dot(own_ref[...], wo_ref[...], NT)

    @pl.when(step >= n)
    def _():
        do_ref[...] = dot(oth_ref[...], wo_ref[...], NT)

    lane = lax.broadcasted_iota(jnp.int32, (BLK, 128), 1)
    q_wide = q_ref[...].astype(F32) * 0.125
    do_wide = do_ref[...]
    qs, dos = [], []
    for h in range(2):
        keep = (lane < 64) if h == 0 else (lane >= 64)
        qs.append(jnp.where(keep, q_wide, 0.0).astype(BF16))
        dos.append(jnp.where(keep, do_wide, 0.0).astype(BF16))

    def score(j, top, masked):
        rows = pl.ds(pl.multiple_of(j * BLK, BLK), BLK)
        k_blk = k_ref[rows, :]
        out = []
        for h in range(2):
            tile = dot(k_blk, qs[h], NT)
            if masked:
                key = lax.broadcasted_iota(jnp.int32, (BLK, BLK), 0)
                qry = lax.broadcasted_iota(jnp.int32, (BLK, BLK), 1)
                tile = jnp.where(key <= qry, tile, -1e30)
            s_ref[h, rows, :] = tile
            out.append(jnp.maximum(top[h], fold_rows(jnp.max, tile)))
        return tuple(out)

    low = jnp.full((8, BLK), -1e30, F32)
    top = score(qi, (low, low), True)
    top = lax.fori_loop(0, qi, lambda j, t: score(j, t, False), top)
    top = [jnp.max(t, axis=0, keepdims=True) for t in top]

    def expo(j, tot):
        rows = pl.ds(pl.multiple_of(j * BLK, BLK), BLK)
        out = []
        for h in range(2):
            tile = jnp.exp(s_ref[h, rows, :] - top[h])
            s_ref[h, rows, :] = tile
            out.append(tot[h] + fold_rows(jnp.sum, tile))
        return tuple(out)

    zero8 = jnp.zeros((8, BLK), F32)
    tot = lax.fori_loop(0, qi + 1, expo, (zero8, zero8))
    inv = [1.0 / jnp.sum(t, axis=0, keepdims=True) for t in tot]

    def third(j, carry):
        proj, o_acc = carry
        rows = pl.ds(pl.multiple_of(j * BLK, BLK), BLK)
        v_blk = v_ref[rows, :]
        proj_new, o_new = [], []
        dv_add = None
        for h in range(2):
            prob = s_ref[h, rows, :] * inv[h]
            s_ref[h, rows, :] = prob
            prob_lo = prob.astype(BF16)
            d_prob = dot(v_blk, dos[h], NT)
            dp_ref[h, rows, :] = d_prob
            proj_new.append(proj[h] + fold_rows(jnp.sum, prob * d_prob))
            term = dot(prob_lo, dos[h])
            dv_add = term if h == 0 else dv_add + term
            o_new.append(o_acc[h] + dot(vt_ref[h * 64:(h + 1) * 64, rows], prob_lo))
        dv_ref[rows, :] += dv_add
        return tuple(proj_new), tuple(o_new)

    zero_t = jnp.zeros((64, BLK), F32)
    proj, o_acc = lax.fori_loop(0, qi + 1, third, ((zero8, zero8), (zero_t, zero_t)))
    for h in range(2):
        ot_ref[h * 64:(h + 1) * 64, :] = o_acc[h].astype(BF16)
    proj = [jnp.sum(t, axis=0, keepdims=True) for t in proj]

    def fourth(j, dq_acc):
        rows = pl.ds(pl.multiple_of(j * BLK, BLK), BLK)
        dq_new = []
        dk_add = None
        for h in range(2):
            d_s = (s_ref[h, rows, :] * (dp_ref[h, rows, :] - proj[h])).astype(BF16)
            term = dot(d_s, qs[h])
            dk_add = term if h == 0 else dk_add + term
            dq_new.append(dq_acc[h] + dot(kt_ref[h * 64:(h + 1) * 64, rows], d_s))
        dk_ref[rows, :] += dk_add
        return tuple(dq_new)

    dq = lax.fori_loop(0, qi + 1, fourth, (zero_t, zero_t))
    dq = jnp.concatenate([d * 0.125 for d in dq], axis=0)
    dqkv_ref[pl.ds(pl.multiple_of(lb * BLK, BLK), BLK), 0:128] = dq.T.astype(BF16)

    @pl.when(step == 2 * n - 1)
    def _():
        done = base * BLK
        dqkv_ref[:, 128:256] = dk_ref[done:, :].astype(BF16)
        dqkv_ref[:, 256:384] = dv_ref[done:, :].astype(BF16)
        if first:
            dk_out[...] = dk_ref[:done, :]
            dv_out[...] = dv_ref[:done, :]


def attn_part(pair, chunk, ids, qkv, own, oth, w_o, carry):
    base, n = chunk
    span, new = (base + 2 * n) * BLK, 2 * n * BLK
    dim = own.shape[1]
    kv = lambda col: pl.BlockSpec((span, 128), lambda s, ids: (0, col))
    block = lambda s, ids: theirs_first(s, n, 1 - ids[0])
    in_specs = [pl.BlockSpec((BLK, 128), lambda s, ids: (base + block(s, ids), pair)), kv(2 + pair), kv(4 + pair),
                pl.BlockSpec((BLK, dim), lambda s, ids: (jnp.minimum(s, n - 1), 0)),
                pl.BlockSpec((BLK, dim), lambda s, ids: (jnp.maximum(s - n, 0), 0)),
                pl.BlockSpec((128, dim), lambda s, ids: (pair, 0))] + [whole(c) for c in carry]
    out_specs = [pl.BlockSpec((128, BLK), lambda s, ids: (0, block(s, ids))),
                 pl.BlockSpec((new, 384), lambda s, ids: (0, 0))]
    out_shape = [shape((128, new)), shape((new, 384))]
    if base:
        out_specs += [pl.BlockSpec((base * BLK, 128), lambda s, ids: (0, 0))] * 2
        out_shape += [shape((base * BLK, 128), F32)] * 2
    scratch = [pltpu.VMEM((BLK, 128), F32), pltpu.VMEM((2, span, BLK), F32), pltpu.VMEM((2, span, BLK), F32),
               pltpu.VMEM((span, 128), F32), pltpu.VMEM((span, 128), F32),
               pltpu.VMEM((128, span), BF16), pltpu.VMEM((128, span), BF16)]
    return call(functools.partial(attn_kernel, base, n), (2 * n,), in_specs, out_specs, out_shape,
                (ids, qkv, qkv, qkv, own, oth, w_o) + tuple(carry), scratch, flops=11, vmem=40)


def dn_kernel(n, ids, a_ref, b_ref, wa_ref, wb_ref, send_ref, keep_ref):
    part = (dot(a_ref[...], wa_ref[...]) + dot(b_ref[...], wb_ref[...])).astype(BF16)
    step = pl.program_id(0)

    @pl.when(step < n)
    def _():
        send_ref[...] = part

    @pl.when(step >= n)
    def _():
        keep_ref[...] = part


def dn_part(chunk, ids, d_a, d_b, w_a, w_b):
    _, n = chunk
    dim = w_a.shape[1]
    rows = pl.BlockSpec((BLK, 384), lambda s, ids: (theirs_first(s, n, ids[0]), 0))
    return call(functools.partial(dn_kernel, n), (2 * n,), [rows, rows, whole(w_a), whole(w_b)],
                [pl.BlockSpec((BLK, dim), lambda s, ids: (jnp.minimum(s, n - 1), 0)),
                 pl.BlockSpec((BLK, dim), lambda s, ids: (jnp.maximum(s - n, 0), 0))],
                [shape((n * BLK, dim))] * 2, (ids, d_a, d_b, w_a, w_b), flops=0.8 * n)


def attn_dw_kernel(ids, dh_ref, dl_ref, nh_ref, nl_ref, oh_ref, ol_ref, ownh_ref, othh_ref, ownl_ref, othl_ref, send_ref, keep_ref):
    core = ids[0]

    def fill(out_ref):
        out_ref[0:384, :] = dot(dh_ref[...], nh_ref[...], TN) + dot(dl_ref[...], nl_ref[...], TN)
        total = None
        for o_ref, own_ref, oth_ref in ((oh_ref, ownh_ref, othh_ref), (ol_ref, ownl_ref, othl_ref)):
            for m in range(own_ref.shape[0] // BLK):
                for ref, who in ((own_ref, core), (oth_ref, 1 - core)):
                    cols = pl.ds(pl.multiple_of((2 * m + who) * BLK, BLK), BLK)
                    term = dot(o_ref[:, cols], ref[m * BLK:(m + 1) * BLK, :])
                    total = term if total is None else total + term
        out_ref[384:512, :] = total

    step = pl.program_id(0)

    @pl.when(step == 0)
    def _():
        fill(send_ref)

    @pl.when(step == 1)
    def _():
        fill(keep_ref)


def attn_dw(ids, d_hi, d_lo, norm_one, o_hi, o_lo, mids):
    dim = norm_one.shape[1]
    half = dim // 2
    which = lambda s, ids: lax.rem(1 + s + ids[1], 2)
    cols = lambda rows, at: pl.BlockSpec((rows, half), lambda s, ids: (at, which(s, ids)))
    out = pl.BlockSpec((512, half), lambda s, ids: (0, 0))
    return call(attn_dw_kernel, (2,),
                [whole(d_hi), whole(d_lo), cols(512, 2), cols(1024, 0), whole(o_hi), whole(o_lo)] + [cols(m.shape[0], 0) for m in mids],
                [out, out], [shape((512, half), F32)] * 2,
                (ids, d_hi, d_lo, norm_one, norm_one, o_hi, o_lo) + tuple(mids), flops=3)


def mlp_dw_kernel(own_steps, ids, n_ref, g_ref, da_ref, dy_ref, na_ref, nb_ref, nc_ref, nd_ref, dya_ref, dyb_ref, wu_ref, wd_ref, gu_ref, gd_ref, au_ref, ad_ref):
    step = pl.program_id(0)

    @pl.when(step == 0)
    def _():
        au_ref[...] = jnp.zeros_like(au_ref)
        ad_ref[...] = jnp.zeros_like(ad_ref)

    def add(n_two, act, d_pre, d_y):
        au_ref[...] += dot(n_two, d_pre, TN)
        ad_ref[...] += dot(act, d_y, TN)

    @pl.when(step < own_steps)
    def _():
        add(n_ref[...], g_ref[...], da_ref[...], dy_ref[...])

    for i, (o_ref, d_ref) in enumerate(((na_ref, dya_ref), (nb_ref, dya_ref), (nc_ref, dyb_ref), (nd_ref, dyb_ref))):
        @pl.when(step == own_steps + i)
        def _():
            n_two, d_y = o_ref[...], d_ref[...]
            act, slope = gelu_pair(dot(n_two, wu_ref[...]).astype(BF16))
            d_pre = (dot(d_y, wd_ref[...], NT) * slope).astype(BF16)
            add(n_two, act.astype(BF16), d_pre, d_y)

    @pl.when(step == pl.num_programs(0) - 1)
    def _():
        gu_ref[...] = au_ref[...].astype(BF16)
        gd_ref[...] = ad_ref[...].astype(BF16)


def mlp_dw(ids, norm_two, act, d_pre, grad_y, n_pieces, dy_a, dy_b, w_up, w_down):
    dim, cols = w_up.shape
    rows = n_pieces[0].shape[0]
    own = norm_two.shape[0] // rows
    mine = pl.BlockSpec((rows, dim), lambda s, ids: (jnp.minimum(s, own - 1), 0))
    dya = pl.BlockSpec((rows, dim), lambda s, ids: (jnp.clip(s - own, 0, 1), 0))
    dyb = pl.BlockSpec((rows, dim), lambda s, ids: (jnp.clip(s - own - 2, 0, 1), 0))
    return call(functools.partial(mlp_dw_kernel, own), (own + 4,),
                [mine] * 4 + [whole(p) for p in n_pieces] + [dya, dyb, whole(w_up), whole(w_down)],
                [whole(w_up), whole(w_down)], [shape((dim, cols)), shape((cols, dim))],
                (ids, norm_two, act, d_pre, grad_y, *n_pieces, dy_a, dy_b, w_up, w_down),
                [pltpu.VMEM((dim, cols), F32), pltpu.VMEM((cols, dim), F32)], flops=25)


def join_dw_kernel(ids, a0_ref, b0_ref, a1_ref, b1_ref, gq_ref, go_ref):
    half = a0_ref.shape[1]
    mine = pl.ds(pl.multiple_of(ids[1] * half, half), half)
    other = pl.ds(pl.multiple_of((1 - ids[1]) * half, half), half)
    for pair, refs in enumerate(((a0_ref, b0_ref), (a1_ref, b1_ref))):
        for ref, cols in zip(refs, (mine, other)):
            for i in range(3):
                gq_ref[(2 * i + pair) * 128:(2 * i + pair + 1) * 128, cols] = ref[i * 128:(i + 1) * 128, :]
            go_ref[pair * 128:(pair + 1) * 128, cols] = ref[384:512, :]


def join_dw(ids, parts, dim):
    out = [shape((768, dim)), shape((256, dim))]
    return call(join_dw_kernel, (1,), [whole(p) for p in parts], [whole(o) for o in out], out, (ids, *parts), flops=0.2)


def join_rows_kernel(ids, ownh_ref, othh_ref, ownl_ref, othl_ref, out_ref):
    step = pl.program_id(0)
    mine = lax.rem(step, 2) == ids[0]
    for own_ref, oth_ref, here in ((ownl_ref, othl_ref, step < HI[0]), (ownh_ref, othh_ref, step >= HI[0])):
        @pl.when(here & mine)
        def _():
            out_ref[...] = own_ref[...]

        @pl.when(here & jnp.logical_not(mine))
        def _():
            out_ref[...] = oth_ref[...]


def join_rows(ids, own_hi, oth_hi, own_lo, oth_lo):
    dim = own_hi.shape[1]
    hi = pl.BlockSpec((BLK, dim), lambda s, ids: (0, 0))
    lo = pl.BlockSpec((BLK, dim), lambda s, ids: (jnp.minimum(s // 2, 1), 0))
    return call(join_rows_kernel, (6,), [hi, hi, lo, lo], pl.BlockSpec((BLK, dim), lambda s, ids: (s, 0)),
                shape((6 * BLK, dim)), (ids, own_hi, oth_hi, own_lo, oth_lo), flops=0.2)


def solution(mesh):
    row_spec = P(('pod', 'dp'), None)
    stat_spec = P(('pod', 'dp'))
    in_specs = (row_spec, row_spec, stat_spec, stat_spec, stat_spec, stat_spec, P(None), P(None), row_spec,
                P(None, None, 'tp', None), P('tp', None, None), P(None, 'tp'), P('tp', None))
    out_specs = (row_spec, P('pod', None, 'tp', None), P(('pod', 'tp'), None, None), P('pod', 'tp'), P(('pod', 'tp'), None))

    def swap(kind, arr):
        axis, perm = {'c': ('tp', [(0, 1), (1, 0), (2, 3), (3, 2)]), 'x': ('tp', [(0, 2), (2, 0), (1, 3), (3, 1)]),
                      'y': ('dp', [(0, 1), (1, 0)])}[kind]
        return lax.ppermute(arr, axis, perm)

    def normed(row_vals, row_mean, row_rstd, gain_vec):
        x_hat = (row_vals.astype(F32) - row_mean[:, None]) * row_rstd[:, None]
        return (x_hat * gain_vec.astype(F32)).astype(BF16)

    def inner(x_saved, h_saved, mean_one, rstd_one, mean_two, rstd_two, gain_one, gain_two, grad_y, w_qkv, w_proj, w_up, w_down):
        t_idx, dp_idx = lax.axis_index('tp'), lax.axis_index('dp')
        ids = jnp.stack([t_idx % 2, dp_idx]).astype(jnp.int32)
        dim = x_saved.shape[1]
        quarter = x_saved.shape[0] // 4
        cut = lambda arr, i: lax.dynamic_slice_in_dim(arr, i * quarter, quarter, 0)
        far = (t_idx + 2) % 4

        n_mine = normed(cut(h_saved, t_idx), cut(mean_two, t_idx), cut(rstd_two, t_idx), gain_two)
        d_mine = jnp.concatenate([cut(grad_y, t_idx), cut(grad_y, far)], axis=0)
        n_y = swap('y', n_mine)
        d_y = swap('y', d_mine)
        n_x = swap('x', n_y)
        n_cy, n_cx = swap('c', n_y), swap('c', n_x)
        d_c = swap('c', d_y)

        norm_two = normed(h_saved, mean_two, rstd_two, gain_two)
        norm_one = normed(x_saved, mean_one, rstd_one, gain_one)
        stats = jnp.stack([mean_one, rstd_one, mean_two, rstd_two], axis=1)
        gains = [g.reshape(1, dim) for g in (gain_one, gain_two)]
        w_t = w_qkv.transpose(1, 2, 3, 0).reshape(-1, dim)
        w_pairs = w_t.reshape(3, 2, 128, dim)
        w_pair = [w_pairs[:, p].reshape(-1, dim) for p in range(2)]
        w_o = w_proj.reshape(-1, dim)

        def chip_sum(send, keep):
            recv = swap('c', send)
            chip = (keep.astype(F32) + recv.astype(F32)).astype(BF16)
            return chip, swap('x', chip)

        tags = {'hi': HI, 'lo': LO}
        prev, two = (), {}
        for tag in ('hi', 'lo'):
            *prev, send, keep = mlp_part(tags[tag], ids, norm_two, grad_y, w_up, w_down, tuple(prev))
            two[tag] = chip_sum(send, keep)
        act, d_pre = prev
        qkv = dot(norm_one, w_t, NT).astype(BF16)

        mid, own, oth = {}, {}, {}
        for tag in ('hi', 'lo'):
            mid[tag], own[tag] = mid_part(tags[tag], ids, *two[tag], h_saved, stats, 2, gains[1], grad_y, False, (F32, BF16))
            oth[tag] = swap('c', own[tag])

        o_t, d_qkv = {}, {}
        for pair in range(2):
            carry = ()
            for tag in ('hi', 'lo'):
                o_t[pair, tag], d_qkv[pair, tag], *carry = attn_part(pair, tags[tag], ids, qkv, own[tag], oth[tag], w_o, tuple(carry))

        gx, gx_oth = {}, {}
        for tag in ('hi', 'lo'):
            send, keep = dn_part(tags[tag], ids, d_qkv[0, tag], d_qkv[1, tag], *w_pair)
            chip, recv = chip_sum(send, keep)
            gx[tag], = mid_part(tags[tag], ids, chip, recv, x_saved, stats, 0, gains[0], mid[tag], True, (BF16,))
            gx_oth[tag] = swap('c', gx[tag])

        parts = []
        for pair in range(2):
            send, keep = attn_dw(ids, d_qkv[pair, 'hi'], d_qkv[pair, 'lo'], norm_one, o_t[pair, 'hi'], o_t[pair, 'lo'],
                                 (own['hi'], oth['hi'], own['lo'], oth['lo']))
            recv = swap('y', send)
            summed = (keep + recv).astype(BF16)
            parts += [summed, swap('y', summed)]

        grad_up, grad_down = mlp_dw(ids, norm_two, act, d_pre, grad_y, (n_y, n_x, n_cy, n_cx), d_y, d_c, w_up, w_down)
        grad_x = join_rows(ids, gx['hi'], gx_oth['hi'], gx['lo'], gx_oth['lo'])
        g_qkv, g_o = join_dw(ids, parts, dim)
        return grad_x, g_qkv.reshape(3, 4, 64, dim).transpose(3, 0, 1, 2), g_o.reshape(4, 64, dim), grad_up, grad_down

    return jax.shard_map(inner, mesh=mesh, in_specs=in_specs, out_specs=out_specs, check_vma=False)
```

```python
import math

import jax
import jax.numpy as jnp
from jax import lax
from jax.experimental import pallas as pl
from jax.experimental.pallas import tpu as pltpu
from jax.sharding import PartitionSpec as P


GELU_C = math.sqrt(2.0 / math.pi)
F32 = jnp.float32
BF16 = jnp.bfloat16
NT = (((1,), (1,)), ((), ()))
TN = (((0,), (0,)), ((), ()))
BLK = 256


def layer_norm(row_vals, row_mean, row_rstd, gain_vec):
    x_hat = (row_vals.astype(F32) - row_mean[:, None]) * row_rstd[:, None]
    return x_hat, (x_hat * gain_vec.astype(F32)).astype(BF16)


def norm_back(d_norm, x_hat, row_rstd, gain_vec):
    scaled = d_norm * gain_vec.astype(F32)
    scaled_mean = jnp.mean(scaled, axis=-1, keepdims=True)
    proj_mean = jnp.mean(scaled * x_hat, axis=-1, keepdims=True)
    return row_rstd[:, None] * (scaled - scaled_mean - x_hat * proj_mean)


def gelu_pair(pre_act):
    pre_wide = pre_act.astype(F32)
    tanh_val = jnp.tanh(GELU_C * (pre_wide + 0.044715 * pre_wide * pre_wide * pre_wide))
    gelu_val = 0.5 * pre_wide * (1.0 + tanh_val)
    gelu_slope = 0.5 * (1.0 + tanh_val) + 0.5 * pre_wide * (1.0 - tanh_val * tanh_val) * GELU_C * (1.0 + 0.134145 * pre_wide * pre_wide)
    return gelu_val, gelu_slope


def fold_rows(op, tile):
    return op(tile.reshape(tile.shape[0] // 8, 8, tile.shape[1]), axis=0)


def attn_kernel(q_ref, k_ref, v_ref, do_ref, ot_ref, dqkv_ref, s_ref, dp_ref, dk_ref, dv_ref, kt_ref, vt_ref):
    step = pl.program_id(0)
    last = pl.num_programs(0) - 1
    qi = last - step

    @pl.when(step == 0)
    def _():
        dk_ref[...] = jnp.zeros_like(dk_ref)
        dv_ref[...] = jnp.zeros_like(dv_ref)
        kt_ref[...] = k_ref[...].T
        vt_ref[...] = v_ref[...].T

    lane = lax.broadcasted_iota(jnp.int32, (BLK, 128), 1)
    q_wide = q_ref[...].astype(F32) * 0.125
    do_wide = do_ref[...].astype(F32)
    qs, dos = [], []
    for h in range(2):
        keep = (lane < 64) if h == 0 else (lane >= 64)
        qs.append(jnp.where(keep, q_wide, 0.0).astype(BF16))
        dos.append(jnp.where(keep, do_wide, 0.0).astype(BF16))

    def score(j, top, masked):
        rows = pl.ds(pl.multiple_of(j * BLK, BLK), BLK)
        k_blk = k_ref[rows, :]
        out = []
        for h in range(2):
            tile = lax.dot_general(k_blk, qs[h], NT, preferred_element_type=F32)
            if masked:
                key = lax.broadcasted_iota(jnp.int32, (BLK, BLK), 0)
                qry = lax.broadcasted_iota(jnp.int32, (BLK, BLK), 1)
                tile = jnp.where(key <= qry, tile, -1e30)
            s_ref[h, rows, :] = tile
            out.append(jnp.maximum(top[h], fold_rows(jnp.max, tile)))
        return tuple(out)

    low = jnp.full((8, BLK), -1e30, F32)
    top = score(qi, (low, low), True)
    top = lax.fori_loop(0, qi, lambda j, t: score(j, t, False), top)
    top = [jnp.max(t, axis=0, keepdims=True) for t in top]

    def expo(j, tot):
        rows = pl.ds(pl.multiple_of(j * BLK, BLK), BLK)
        out = []
        for h in range(2):
            tile = jnp.exp(s_ref[h, rows, :] - top[h])
            s_ref[h, rows, :] = tile
            out.append(tot[h] + fold_rows(jnp.sum, tile))
        return tuple(out)

    zero8 = jnp.zeros((8, BLK), F32)
    tot = lax.fori_loop(0, qi + 1, expo, (zero8, zero8))
    inv = [1.0 / jnp.sum(t, axis=0, keepdims=True) for t in tot]

    def third(j, carry):
        proj, o_acc = carry
        rows = pl.ds(pl.multiple_of(j * BLK, BLK), BLK)
        v_blk = v_ref[rows, :]
        proj_new, o_new = [], []
        dv_add = None
        for h in range(2):
            prob = s_ref[h, rows, :] * inv[h]
            s_ref[h, rows, :] = prob
            prob_lo = prob.astype(BF16)
            d_prob = lax.dot_general(v_blk, dos[h], NT, preferred_element_type=F32)
            dp_ref[h, rows, :] = d_prob
            proj_new.append(proj[h] + fold_rows(jnp.sum, prob * d_prob))
            term = jnp.dot(prob_lo, dos[h], preferred_element_type=F32)
            dv_add = term if h == 0 else dv_add + term
            o_new.append(o_acc[h] + jnp.dot(vt_ref[h * 64:(h + 1) * 64, rows], prob_lo, preferred_element_type=F32))
        dv_ref[rows, :] += dv_add
        return tuple(proj_new), tuple(o_new)

    zero_t = jnp.zeros((64, BLK), F32)
    proj, o_acc = lax.fori_loop(0, qi + 1, third, ((zero8, zero8), (zero_t, zero_t)))
    for h in range(2):
        ot_ref[h * 64:(h + 1) * 64, :] = o_acc[h].astype(BF16)
    proj = [jnp.sum(t, axis=0, keepdims=True) for t in proj]

    def fourth(j, dq_acc):
        rows = pl.ds(pl.multiple_of(j * BLK, BLK), BLK)
        dq_new = []
        dk_add = None
        for h in range(2):
            d_s = (s_ref[h, rows, :] * (dp_ref[h, rows, :] - proj[h])).astype(BF16)
            term = jnp.dot(d_s, qs[h], preferred_element_type=F32)
            dk_add = term if h == 0 else dk_add + term
            dq_new.append(dq_acc[h] + jnp.dot(kt_ref[h * 64:(h + 1) * 64, rows], d_s, preferred_element_type=F32))
        dk_ref[rows, :] += dk_add
        return tuple(dq_new)

    dq = lax.fori_loop(0, qi + 1, fourth, (zero_t, zero_t))
    dq = jnp.concatenate([d * 0.125 for d in dq], axis=0)
    rows = pl.ds(pl.multiple_of(qi * BLK, BLK), BLK)
    dqkv_ref[rows, 0:128] = dq.T.astype(BF16)

    @pl.when(step == last)
    def _():
        dqkv_ref[:, 128:256] = dk_ref[...].astype(BF16)
        dqkv_ref[:, 256:384] = dv_ref[...].astype(BF16)


def attn_pair(pair, qkv, d_attn):
    toks = qkv.shape[0]
    steps = toks // BLK
    return pl.pallas_call(
        attn_kernel,
        grid=(steps,),
        in_specs=[pl.BlockSpec((BLK, 128), lambda s: (steps - 1 - s, pair)),
                  pl.BlockSpec((toks, 128), lambda s: (0, 2 + pair)),
                  pl.BlockSpec((toks, 128), lambda s: (0, 4 + pair)),
                  pl.BlockSpec((BLK, 128), lambda s: (steps - 1 - s, pair))],
        out_specs=[pl.BlockSpec((128, BLK), lambda s: (0, steps - 1 - s)),
                   pl.BlockSpec((toks, 384), lambda s: (0, 0))],
        out_shape=[jax.ShapeDtypeStruct((128, toks), BF16), jax.ShapeDtypeStruct((toks, 384), BF16)],
        scratch_shapes=[pltpu.VMEM((2, toks, BLK), F32), pltpu.VMEM((2, toks, BLK), F32),
                        pltpu.VMEM((toks, 128), F32), pltpu.VMEM((toks, 128), F32),
                        pltpu.VMEM((128, toks), BF16), pltpu.VMEM((128, toks), BF16)],
        compiler_params=pltpu.CompilerParams(dimension_semantics=("arbitrary",), vmem_limit_bytes=20 << 20),
        cost_estimate=pl.CostEstimate(flops=16 * 10**9, bytes_accessed=4 << 20, transcendentals=0),
    )(qkv, qkv, qkv, d_attn)


def mlp_kernel(na_ref, da_ref, nb_ref, db_ref, wu_ref, wd_ref, pu_hbm, pd_hbm, gu_ref, gd_ref, au_ref, ad_ref, pu_ref, pd_ref, sem):
    step = pl.program_id(0)
    half = pl.num_programs(0) // 2
    load_u = pltpu.make_async_copy(pu_hbm, pu_ref, sem.at[0])
    load_d = pltpu.make_async_copy(pd_hbm, pd_ref, sem.at[1])

    @pl.when(step == 0)
    def _():
        load_u.start()
        load_d.start()
        au_ref[...] = jnp.zeros_like(au_ref)
        ad_ref[...] = jnp.zeros_like(ad_ref)

    def rows_of(n_ref, d_ref):
        n_two = n_ref[...]
        d_y = d_ref[...]
        pre = jnp.dot(n_two, wu_ref[...], preferred_element_type=F32).astype(BF16)
        act, slope = gelu_pair(pre)
        d_act = lax.dot_general(d_y, wd_ref[...], NT, preferred_element_type=F32)
        d_pre = (d_act * slope).astype(BF16)
        au_ref[...] += lax.dot_general(n_two, d_pre, TN, preferred_element_type=F32)
        ad_ref[...] += lax.dot_general(act.astype(BF16), d_y, TN, preferred_element_type=F32)

    @pl.when(step < half)
    def _():
        rows_of(na_ref, da_ref)

    @pl.when(step >= half)
    def _():
        rows_of(nb_ref, db_ref)

    @pl.when(step == pl.num_programs(0) - 1)
    def _():
        load_u.wait()
        load_d.wait()
        gu_ref[...] = (au_ref[...] + pu_ref[...]).astype(BF16)
        gd_ref[...] = (ad_ref[...] + pd_ref[...]).astype(BF16)


def mlp_grad(n_a, d_a, n_b, d_b, w_up, w_down, part_up, part_down):
    rows, dim = n_a.shape
    cols = w_up.shape[1]
    blk = 384
    half = rows // blk
    first = pl.BlockSpec((blk, dim), lambda s: (jnp.minimum(s, half - 1), 0))
    second = pl.BlockSpec((blk, dim), lambda s: (jnp.maximum(s - half, 0), 0))
    whole_up = pl.BlockSpec((dim, cols), lambda s: (0, 0))
    whole_down = pl.BlockSpec((cols, dim), lambda s: (0, 0))
    return pl.pallas_call(
        mlp_kernel,
        grid=(2 * half,),
        in_specs=[first, first, second, second, whole_up, whole_down,
                  pl.BlockSpec(memory_space=pl.ANY), pl.BlockSpec(memory_space=pl.ANY)],
        out_specs=[whole_up, whole_down],
        out_shape=[jax.ShapeDtypeStruct((dim, cols), BF16), jax.ShapeDtypeStruct((cols, dim), BF16)],
        scratch_shapes=[pltpu.VMEM((dim, cols), F32), pltpu.VMEM((cols, dim), F32),
                        pltpu.VMEM((dim, cols), F32), pltpu.VMEM((cols, dim), F32),
                        pltpu.SemaphoreType.DMA((2,))],
        compiler_params=pltpu.CompilerParams(dimension_semantics=("arbitrary",), vmem_limit_bytes=60 << 20),
        cost_estimate=pl.CostEstimate(flops=16 * 10**9, bytes_accessed=24 << 20, transcendentals=0),
        name="mlp_grad",
    )(n_a, d_a, n_b, d_b, w_up, w_down, part_up, part_down)


HALVES = (('hi', 1), ('lo', 0))


def solution(mesh):
    row_spec = P(('pod', 'dp'), None)
    stat_spec = P(('pod', 'dp'))
    in_specs = (row_spec, row_spec, stat_spec, stat_spec, stat_spec, stat_spec, P(None), P(None), row_spec,
                P(None, None, 'tp', None), P('tp', None, None), P(None, 'tp'), P('tp', None))
    out_specs = (row_spec, P('pod', None, 'tp', None), P(('pod', 'tp'), None, None), P('pod', 'tp'), P(('pod', 'tp'), None))

    def swap(kind, arr):
        axis, perm = {'c': ('tp', [(0, 1), (1, 0), (2, 3), (3, 2)]), 'x': ('tp', [(0, 2), (2, 0), (1, 3), (3, 1)]),
                      'y': ('dp', [(0, 1), (1, 0)])}[kind]
        return lax.ppermute(arr, axis, perm)

    def take_half(arr, which):
        rows = arr.shape[0] // 2
        return lax.dynamic_slice_in_dim(arr, which * rows, rows, 0)

    def join_halves(mine, other, which):
        return jnp.concatenate([jnp.where(which == 0, mine, other), jnp.where(which == 0, other, mine)], axis=0)

    def inner(x_saved, h_saved, mean_one, rstd_one, mean_two, rstd_two, gain_one, gain_two, grad_y, w_qkv, w_proj, w_up, w_down):
        core = lax.axis_index('tp') % 2
        dp_idx = lax.axis_index('dp')
        toks, dim = x_saved.shape
        part_of = lambda arr, i: arr[i * (toks // 2):(i + 1) * (toks // 2)]

        n_mine = layer_norm(take_half(h_saved, core), take_half(mean_two, core), take_half(rstd_two, core), gain_two)[1]
        norm_y, dy_y = swap('y', n_mine), swap('y', take_half(grad_y, core))
        norm_c, dy_c = swap('c', norm_y), swap('c', dy_y)

        def tp_sum(part):
            chip = (take_half(part, core).astype(F32) + swap('c', take_half(part, 1 - core)).astype(F32)).astype(BF16)
            return chip.astype(F32) + swap('x', chip).astype(F32)

        def back(total, rows, mean, rstd, gain):
            hat = (rows.astype(F32) - mean[:, None]) * rstd[:, None]
            return norm_back(total, hat, rstd, gain)

        norm_two, act, d_pre, d_norm = {}, {}, {}, {}
        for tag, i in HALVES:
            norm_two[tag] = layer_norm(part_of(h_saved, i), part_of(mean_two, i), part_of(rstd_two, i), gain_two)[1]
            pre_act = jnp.dot(norm_two[tag], w_up, preferred_element_type=F32).astype(BF16)
            gelu_val, gelu_slope = gelu_pair(pre_act)
            act[tag] = gelu_val.astype(BF16)
            d_pre[tag] = (lax.dot_general(part_of(grad_y, i), w_down, NT, preferred_element_type=F32) * gelu_slope).astype(BF16)
            part = lax.dot_general(d_pre[tag], w_up, NT, preferred_element_type=F32).astype(BF16)
            d_norm[tag] = tp_sum(part)

        part_down = sum(lax.dot_general(act[tag], part_of(grad_y, i), TN, preferred_element_type=F32) for tag, i in HALVES)
        part_up = sum(lax.dot_general(norm_two[tag], d_pre[tag], TN, preferred_element_type=F32) for tag, i in HALVES)

        w_t = w_qkv.transpose(1, 2, 3, 0).reshape(-1, dim)
        norm_one = layer_norm(x_saved, mean_one, rstd_one, gain_one)[1]
        qkv = lax.dot_general(norm_one, w_t, NT, preferred_element_type=F32).astype(BF16)

        w_o = w_proj.reshape(-1, dim)
        d_mid, mid_lo, d_attn = {}, {}, {}
        for tag, i in HALVES:
            mine = [take_half(part_of(a, i), core) for a in (grad_y, h_saved, mean_two, rstd_two)]
            if tag == 'lo':
                mine[2], mine[3], low = lax.optimization_barrier((mine[2], mine[3], low))
            d_mid[tag] = mine[0].astype(F32) + back(d_norm[tag], *mine[1:], gain_two)
            low = d_mid[tag].astype(BF16)
            mid_lo[tag] = join_halves(low, swap('c', low), core)
            d_attn[tag] = lax.dot_general(mid_lo[tag], w_o, NT, preferred_element_type=F32).astype(BF16)
        d_attn = jnp.concatenate([d_attn['lo'], d_attn['hi']], axis=0)
        mid_all = jnp.concatenate([mid_lo['lo'], mid_lo['hi']], axis=0)

        w_pairs = w_t.reshape(3, 2, 128, dim)
        halves, d_pair = [], []
        for pair in range(2):
            o_t, d_qkv = attn_pair(pair, qkv, d_attn)
            d_pair.append(d_qkv)
            g_qkv = lax.dot_general(d_qkv, norm_one, TN, preferred_element_type=F32)
            g_o = jnp.dot(o_t, mid_all, preferred_element_type=F32)
            mine = jnp.concatenate([take_half(g, dp_idx) for g in (g_qkv, g_o)], 0)
            theirs = jnp.concatenate([take_half(g, 1 - dp_idx) for g in (g_qkv, g_o)], 0)
            summed = (mine + swap('y', theirs)).astype(BF16)
            other = swap('y', summed)
            halves.append((join_halves(summed[:192], other[:192], dp_idx), join_halves(summed[192:], other[192:], dp_idx)))

        w_pair = [w_pairs[:, p].reshape(-1, dim) for p in range(2)]
        part_one = jnp.dot(d_pair[0], w_pair[0], preferred_element_type=F32)
        grad_x = {}
        for tag, i in HALVES:
            part = (part_of(part_one, i) + jnp.dot(part_of(d_pair[1], i), w_pair[1], preferred_element_type=F32)).astype(BF16)
            total = tp_sum(part)
            mine = [take_half(part_of(a, i), core) for a in (x_saved, mean_one, rstd_one)]
            if tag == 'lo':
                mine[1], mine[2], low = lax.optimization_barrier((mine[1], mine[2], low))
            low = (d_mid[tag] + back(total, *mine, gain_one)).astype(BF16)
            grad_x[tag] = join_halves(low, swap('c', low), core)
        grad_x = jnp.concatenate([grad_x['lo'], grad_x['hi']], axis=0)

        grad_up, grad_down = mlp_grad(norm_y, dy_y, norm_c, dy_c, w_up, w_down, part_up, part_down)
        g_t = jnp.stack([h[0].reshape(3, 2, 64, dim) for h in halves], axis=1).reshape(3, 4, 64, dim)
        grad_qkv = g_t.transpose(3, 0, 1, 2)
        grad_proj = jnp.concatenate([h[1] for h in halves], axis=0).reshape(4, 64, dim)
        return grad_x, grad_qkv, grad_proj, grad_up, grad_down

    return jax.shard_map(inner, mesh=mesh, in_specs=in_specs, out_specs=out_specs, check_vma=False)
```

```python
import functools
import math

import jax
import jax.numpy as jnp
from jax import lax
from jax.experimental import pallas as pl
from jax.experimental.pallas import tpu as pltpu
from jax.sharding import PartitionSpec as P


GELU_C = math.sqrt(2.0 / math.pi)
F32 = jnp.float32
BF16 = jnp.bfloat16
NT = (((1,), (1,)), ((), ()))
TN = (((0,), (0,)), ((), ()))
BLK = 256


def layer_norm(row_vals, row_mean, row_rstd, gain_vec):
    x_hat = (row_vals.astype(F32) - row_mean[:, None]) * row_rstd[:, None]
    return x_hat, (x_hat * gain_vec.astype(F32)).astype(BF16)


def norm_back(d_norm, x_hat, row_rstd, gain_vec):
    scaled = d_norm * gain_vec.astype(F32)
    scaled_mean = jnp.mean(scaled, axis=-1, keepdims=True)
    proj_mean = jnp.mean(scaled * x_hat, axis=-1, keepdims=True)
    return row_rstd[:, None] * (scaled - scaled_mean - x_hat * proj_mean)


def gelu_pair(pre_act):
    pre_wide = pre_act.astype(F32)
    tanh_val = jnp.tanh(GELU_C * (pre_wide + 0.044715 * pre_wide * pre_wide * pre_wide))
    gelu_val = 0.5 * pre_wide * (1.0 + tanh_val)
    gelu_slope = 0.5 * (1.0 + tanh_val) + 0.5 * pre_wide * (1.0 - tanh_val * tanh_val) * GELU_C * (1.0 + 0.134145 * pre_wide * pre_wide)
    return gelu_val, gelu_slope


def fold_rows(op, tile):
    return op(tile.reshape(tile.shape[0] // 8, 8, tile.shape[1]), axis=0)


def attn_kernel(q_ref, k_ref, v_ref, do_ref, ot_ref, dqkv_ref, s_ref, dp_ref, dk_ref, dv_ref, kt_ref, vt_ref, acc_ref):
    step = pl.program_id(0)
    last = pl.num_programs(0) - 1
    qi = last - step

    @pl.when(step == 0)
    def _():
        dk_ref[...] = jnp.zeros_like(dk_ref)
        dv_ref[...] = jnp.zeros_like(dv_ref)
        kt_ref[...] = k_ref[...].T
        vt_ref[...] = v_ref[...].T

    lane = lax.broadcasted_iota(jnp.int32, (BLK, 128), 1)
    q_wide = q_ref[...].astype(F32) * 0.125
    do_wide = do_ref[...].astype(F32)
    qs, dos = [], []
    for h in range(2):
        keep = (lane < 64) if h == 0 else (lane >= 64)
        qs.append(jnp.where(keep, q_wide, 0.0).astype(BF16))
        dos.append(jnp.where(keep, do_wide, 0.0).astype(BF16))

    def score(j, top, masked):
        rows = pl.ds(pl.multiple_of(j * BLK, BLK), BLK)
        k_blk = k_ref[rows, :]
        out = []
        for h in range(2):
            tile = lax.dot_general(k_blk, qs[h], NT, preferred_element_type=F32)
            if masked:
                key = lax.broadcasted_iota(jnp.int32, (BLK, BLK), 0)
                qry = lax.broadcasted_iota(jnp.int32, (BLK, BLK), 1)
                tile = jnp.where(key <= qry, tile, -1e30)
            s_ref[h, rows, :] = tile
            out.append(jnp.maximum(top[h], fold_rows(jnp.max, tile)))
        return tuple(out)

    low = jnp.full((8, BLK), -1e30, F32)
    top = score(qi, (low, low), True)
    top = lax.fori_loop(0, qi, lambda j, t: score(j, t, False), top)
    top = [jnp.max(t, axis=0, keepdims=True) for t in top]

    def expo(j, tot):
        rows = pl.ds(pl.multiple_of(j * BLK, BLK), BLK)
        out = []
        for h in range(2):
            tile = jnp.exp(s_ref[h, rows, :] - top[h])
            s_ref[h, rows, :] = tile
            out.append(tot[h] + fold_rows(jnp.sum, tile))
        return tuple(out)

    zero8 = jnp.zeros((8, BLK), F32)
    tot = lax.fori_loop(0, qi + 1, expo, (zero8, zero8))
    inv = [1.0 / jnp.sum(t, axis=0, keepdims=True) for t in tot]

    acc_ref[...] = jnp.zeros_like(acc_ref)

    def third(j, proj):
        rows = pl.ds(pl.multiple_of(j * BLK, BLK), BLK)
        v_blk = v_ref[rows, :]
        proj_new = []
        for h in range(2):
            prob = s_ref[h, rows, :] * inv[h]
            s_ref[h, rows, :] = prob
            prob_lo = prob.astype(BF16)
            d_prob = lax.dot_general(v_blk, dos[h], NT, preferred_element_type=F32)
            dp_ref[h, rows, :] = d_prob
            proj_new.append(proj[h] + fold_rows(jnp.sum, prob * d_prob))
            dv_ref[rows, :] += jnp.dot(prob_lo, dos[h], preferred_element_type=F32)
            acc_ref[h] += jnp.dot(vt_ref[h * 64:(h + 1) * 64, rows], prob_lo, preferred_element_type=F32)
        return tuple(proj_new)

    proj = lax.fori_loop(0, qi + 1, third, (zero8, zero8))
    for h in range(2):
        ot_ref[h * 64:(h + 1) * 64, :] = acc_ref[h].astype(BF16)
    proj = [jnp.sum(t, axis=0, keepdims=True) for t in proj]

    acc_ref[...] = jnp.zeros_like(acc_ref)

    def fourth(j, none):
        rows = pl.ds(pl.multiple_of(j * BLK, BLK), BLK)
        for h in range(2):
            d_s = (s_ref[h, rows, :] * (dp_ref[h, rows, :] - proj[h])).astype(BF16)
            dk_ref[rows, :] += jnp.dot(d_s, qs[h], preferred_element_type=F32)
            acc_ref[h] += jnp.dot(kt_ref[h * 64:(h + 1) * 64, rows], d_s, preferred_element_type=F32)
        return none

    lax.fori_loop(0, qi + 1, fourth, 0)
    dq = acc_ref[...].reshape(128, BLK) * 0.125
    rows = pl.ds(pl.multiple_of(qi * BLK, BLK), BLK)
    dqkv_ref[rows, 0:128] = dq.T.astype(BF16)

    @pl.when(step == last)
    def _():
        dqkv_ref[:, 128:256] = dk_ref[...].astype(BF16)
        dqkv_ref[:, 256:384] = dv_ref[...].astype(BF16)


def attn_pair(pair, qkv, d_attn):
    toks = qkv.shape[0]
    steps = toks // BLK
    return pl.pallas_call(
        attn_kernel,
        grid=(steps,),
        in_specs=[pl.BlockSpec((BLK, 128), lambda s: (steps - 1 - s, pair)),
                  pl.BlockSpec((toks, 128), lambda s: (0, 2 + pair)),
                  pl.BlockSpec((toks, 128), lambda s: (0, 4 + pair)),
                  pl.BlockSpec((BLK, 128), lambda s: (steps - 1 - s, pair))],
        out_specs=[pl.BlockSpec((128, BLK), lambda s: (0, steps - 1 - s)),
                   pl.BlockSpec((toks, 384), lambda s: (0, 0))],
        out_shape=[jax.ShapeDtypeStruct((128, toks), BF16), jax.ShapeDtypeStruct((toks, 384), BF16)],
        scratch_shapes=[pltpu.VMEM((2, toks, BLK), F32), pltpu.VMEM((2, toks, BLK), F32),
                        pltpu.VMEM((toks, 128), F32), pltpu.VMEM((toks, 128), F32),
                        pltpu.VMEM((128, toks), BF16), pltpu.VMEM((128, toks), BF16), pltpu.VMEM((2, 64, BLK), F32)],
        compiler_params=pltpu.CompilerParams(dimension_semantics=("arbitrary",), vmem_limit_bytes=20 << 20),
        cost_estimate=pl.CostEstimate(flops=16 * 10**9, bytes_accessed=4 << 20, transcendentals=0),
    )(qkv, qkv, qkv, d_attn)


def mlp_kernel(part, na_ref, da_ref, nb_ref, db_ref, wu_ref, wd_ref, pu_hbm, pd_hbm, *rest):
    gu_ref, gd_ref, au_ref, ad_ref, pu_ref, pd_ref, n_ref, nt_ref, d_ref, sem = rest[-10:]
    step = pl.program_id(0)
    half = pl.num_programs(0) // 2
    cols = au_ref.shape[1]
    load_u = pltpu.make_async_copy(pu_hbm.at[:, part * cols:(part + 1) * cols], pu_ref, sem.at[0])
    load_d = pltpu.make_async_copy(pd_hbm.at[part * cols:(part + 1) * cols, :], pd_ref, sem.at[1])

    @pl.when(step == 0)
    def _():
        load_u.start()
        load_d.start()
        au_ref[...] = jnp.zeros_like(au_ref)
        ad_ref[...] = jnp.zeros_like(ad_ref)

    for when, n_in, d_in in ((step < half, na_ref, da_ref), (step >= half, nb_ref, db_ref)):
        @pl.when(when)
        def _():
            n_ref[...] = n_in[...]
            d_ref[...] = d_in[...]

    nt_ref[...] = n_ref[...].T
    for c in range(0, cols, BLK):
        sl = slice(c, c + BLK)
        pre = jnp.dot(n_ref[...], wu_ref[:, sl], preferred_element_type=F32).astype(BF16)
        act, slope = gelu_pair(pre)
        d_act = lax.dot_general(d_ref[...], wd_ref[sl, :], NT, preferred_element_type=F32)
        d_pre = (d_act * slope).astype(BF16)
        au_ref[:, sl] += jnp.dot(nt_ref[...], d_pre, preferred_element_type=F32)
        ad_ref[sl, :] += lax.dot_general(act.astype(BF16), d_ref[...], TN, preferred_element_type=F32)

    @pl.when(step == pl.num_programs(0) - 1)
    def _():
        load_u.wait()
        load_d.wait()
        gu_ref[...] = (au_ref[...] + pu_ref[...]).astype(BF16)
        gd_ref[...] = (ad_ref[...] + pd_ref[...]).astype(BF16)


def mlp_grad(part, n_a, d_a, n_b, d_b, w_up, w_down, part_up, part_down, prev=()):
    rows, dim = n_a.shape
    cols = w_up.shape[1] // 2
    blk = 384
    half = rows // blk
    first = pl.BlockSpec((blk, dim), lambda s: (jnp.minimum(s, half - 1), 0))
    second = pl.BlockSpec((blk, dim), lambda s: (jnp.maximum(s - half, 0), 0))
    half_up = pl.BlockSpec((dim, cols), lambda s: (0, part))
    half_down = pl.BlockSpec((cols, dim), lambda s: (part, 0))
    any_spec = pl.BlockSpec(memory_space=pl.ANY)
    return pl.pallas_call(
        functools.partial(mlp_kernel, part),
        grid=(2 * half,),
        in_specs=[first, first, second, second, half_up, half_down, any_spec, any_spec] + [any_spec] * len(prev),
        out_specs=[half_up, half_down],
        out_shape=[jax.ShapeDtypeStruct(w_up.shape, BF16), jax.ShapeDtypeStruct(w_down.shape, BF16)],
        scratch_shapes=[pltpu.VMEM((dim, cols), F32), pltpu.VMEM((cols, dim), F32),
                        pltpu.VMEM((dim, cols), F32), pltpu.VMEM((cols, dim), F32),
                        pltpu.VMEM((blk, dim), BF16), pltpu.VMEM((dim, blk), BF16), pltpu.VMEM((blk, dim), BF16),
                        pltpu.SemaphoreType.DMA((2,))],
        input_output_aliases={8: 0, 9: 1} if prev else {},
        compiler_params=pltpu.CompilerParams(dimension_semantics=("arbitrary",), vmem_limit_bytes=44 << 20),
        cost_estimate=pl.CostEstimate(flops=8 * 10**9, bytes_accessed=14 << 20, transcendentals=0),
    )(n_a, d_a, n_b, d_b, w_up, w_down, part_up, part_down, *prev)


HALVES = (('hi', 1), ('lo', 0))


def solution(mesh):
    row_spec = P(('pod', 'dp'), None)
    stat_spec = P(('pod', 'dp'))
    in_specs = (row_spec, row_spec, stat_spec, stat_spec, stat_spec, stat_spec, P(None), P(None), row_spec,
                P(None, None, 'tp', None), P('tp', None, None), P(None, 'tp'), P('tp', None))
    out_specs = (row_spec, P('pod', None, 'tp', None), P(('pod', 'tp'), None, None), P('pod', 'tp'), P(('pod', 'tp'), None))

    def swap(kind, arr):
        axis, perm = {'c': ('tp', [(0, 1), (1, 0), (2, 3), (3, 2)]), 'x': ('tp', [(0, 2), (2, 0), (1, 3), (3, 1)]),
                      'y': ('dp', [(0, 1), (1, 0)])}[kind]
        return lax.ppermute(arr, axis, perm)

    def take_half(arr, which):
        rows = arr.shape[0] // 2
        return lax.dynamic_slice_in_dim(arr, which * rows, rows, 0)

    def join_halves(mine, other, which):
        return jnp.concatenate([jnp.where(which == 0, mine, other), jnp.where(which == 0, other, mine)], axis=0)

    def inner(x_saved, h_saved, mean_one, rstd_one, mean_two, rstd_two, gain_one, gain_two, grad_y, w_qkv, w_proj, w_up, w_down):
        core = lax.axis_index('tp') % 2
        dp_idx = lax.axis_index('dp')
        toks, dim = x_saved.shape
        part_of = lambda arr, i: arr[i * (toks // 2):(i + 1) * (toks // 2)]

        n_mine = layer_norm(take_half(h_saved, core), take_half(mean_two, core), take_half(rstd_two, core), gain_two)[1]
        norm_y, dy_y = swap('y', n_mine), swap('y', take_half(grad_y, core))
        norm_c, dy_c = swap('c', norm_y), swap('c', dy_y)

        def tp_sum(part):
            chip = (take_half(part, core).astype(F32) + swap('c', take_half(part, 1 - core)).astype(F32)).astype(BF16)
            return chip.astype(F32) + swap('x', chip).astype(F32)

        def back(total, rows, mean, rstd, gain):
            hat = (rows.astype(F32) - mean[:, None]) * rstd[:, None]
            return norm_back(total, hat, rstd, gain)

        norm_two, act, d_pre, d_norm = {}, {}, {}, {}
        for tag, i in HALVES:
            norm_two[tag] = layer_norm(part_of(h_saved, i), part_of(mean_two, i), part_of(rstd_two, i), gain_two)[1]
            pre_act = jnp.dot(norm_two[tag], w_up, preferred_element_type=F32).astype(BF16)
            gelu_val, gelu_slope = gelu_pair(pre_act)
            act[tag] = gelu_val.astype(BF16)
            d_pre[tag] = (lax.dot_general(part_of(grad_y, i), w_down, NT, preferred_element_type=F32) * gelu_slope).astype(BF16)
            part = lax.dot_general(d_pre[tag], w_up, NT, preferred_element_type=F32).astype(BF16)
            d_norm[tag] = tp_sum(part)

        part_down = sum(lax.dot_general(act[tag], part_of(grad_y, i), TN, preferred_element_type=F32) for tag, i in HALVES)
        part_up = sum(lax.dot_general(norm_two[tag], d_pre[tag], TN, preferred_element_type=F32) for tag, i in HALVES)

        w_t = w_qkv.transpose(1, 2, 3, 0).reshape(-1, dim)
        norm_one = layer_norm(x_saved, mean_one, rstd_one, gain_one)[1]
        qkv = lax.dot_general(norm_one, w_t, NT, preferred_element_type=F32).astype(BF16)

        w_o = w_proj.reshape(-1, dim)
        d_mid, mid_lo, d_attn = {}, {}, {}
        for tag, i in HALVES:
            mine = [take_half(part_of(a, i), core) for a in (grad_y, h_saved, mean_two, rstd_two)]
            if tag == 'lo':
                mine[2], mine[3], low = lax.optimization_barrier((mine[2], mine[3], low))
            d_mid[tag] = mine[0].astype(F32) + back(d_norm[tag], *mine[1:], gain_two)
            low = d_mid[tag].astype(BF16)
            mid_lo[tag] = join_halves(low, swap('c', low), core)
            d_attn[tag] = lax.dot_general(mid_lo[tag], w_o, NT, preferred_element_type=F32).astype(BF16)
        d_attn = jnp.concatenate([d_attn['lo'], d_attn['hi']], axis=0)
        mid_all = jnp.concatenate([mid_lo['lo'], mid_lo['hi']], axis=0)

        w_pairs = w_t.reshape(3, 2, 128, dim)
        halves, d_pair = [], []
        for pair in range(2):
            o_t, d_qkv = attn_pair(pair, qkv, d_attn)
            d_pair.append(d_qkv)
            g_qkv = lax.dot_general(d_qkv, norm_one, TN, preferred_element_type=F32)
            g_o = jnp.dot(o_t, mid_all, preferred_element_type=F32)
            mine = jnp.concatenate([take_half(g, dp_idx) for g in (g_qkv, g_o)], 0)
            theirs = jnp.concatenate([take_half(g, 1 - dp_idx) for g in (g_qkv, g_o)], 0)
            summed = (mine + swap('y', theirs)).astype(BF16)
            other = swap('y', summed)
            halves.append((join_halves(summed[:192], other[:192], dp_idx), join_halves(summed[192:], other[192:], dp_idx)))

        w_pair = [w_pairs[:, p].reshape(-1, dim) for p in range(2)]
        part_one = jnp.dot(d_pair[0], w_pair[0], preferred_element_type=F32)
        grad_x = {}
        for tag, i in HALVES:
            part = (part_of(part_one, i) + jnp.dot(part_of(d_pair[1], i), w_pair[1], preferred_element_type=F32)).astype(BF16)
            total = tp_sum(part)
            mine = [take_half(part_of(a, i), core) for a in (x_saved, mean_one, rstd_one)]
            if tag == 'lo':
                mine[1], mine[2], low = lax.optimization_barrier((mine[1], mine[2], low))
            low = (d_mid[tag] + back(total, *mine, gain_one)).astype(BF16)
            grad_x[tag] = join_halves(low, swap('c', low), core)
        grad_x = jnp.concatenate([grad_x['lo'], grad_x['hi']], axis=0)

        grads = ()
        for part in range(2):
            grads = mlp_grad(part, norm_y, dy_y, norm_c, dy_c, w_up, w_down, part_up, part_down, tuple(grads))
        grad_up, grad_down = grads
        g_t = jnp.stack([h[0].reshape(3, 2, 64, dim) for h in halves], axis=1).reshape(3, 4, 64, dim)
        grad_qkv = g_t.transpose(3, 0, 1, 2)
        grad_proj = jnp.concatenate([h[1] for h in halves], axis=0).reshape(4, 64, dim)
        return grad_x, grad_qkv, grad_proj, grad_up, grad_down

    return jax.shard_map(inner, mesh=mesh, in_specs=in_specs, out_specs=out_specs, check_vma=False)
```

```python
import functools
import math

import jax
import jax.numpy as jnp
from jax import lax
from jax.experimental import pallas as pl
from jax.experimental.pallas import tpu as pltpu
from jax.sharding import PartitionSpec as P


GELU_C = math.sqrt(2.0 / math.pi)
F32 = jnp.float32
BF16 = jnp.bfloat16
NT = (((1,), (1,)), ((), ()))
TN = (((0,), (0,)), ((), ()))
BLK = 256


def layer_norm(row_vals, row_mean, row_rstd, gain_vec):
    x_hat = (row_vals.astype(F32) - row_mean[:, None]) * row_rstd[:, None]
    return x_hat, (x_hat * gain_vec.astype(F32)).astype(BF16)


def norm_back(d_norm, x_hat, row_rstd, gain_vec):
    scaled = d_norm * gain_vec.astype(F32)
    scaled_mean = jnp.mean(scaled, axis=-1, keepdims=True)
    proj_mean = jnp.mean(scaled * x_hat, axis=-1, keepdims=True)
    return row_rstd[:, None] * (scaled - scaled_mean - x_hat * proj_mean)


def gelu_pair(pre_act):
    pre_wide = pre_act.astype(F32)
    tanh_val = jnp.tanh(GELU_C * (pre_wide + 0.044715 * pre_wide * pre_wide * pre_wide))
    gelu_val = 0.5 * pre_wide * (1.0 + tanh_val)
    gelu_slope = 0.5 * (1.0 + tanh_val) + 0.5 * pre_wide * (1.0 - tanh_val * tanh_val) * GELU_C * (1.0 + 0.134145 * pre_wide * pre_wide)
    return gelu_val, gelu_slope


def fold_rows(op, tile):
    return op(tile.reshape(tile.shape[0] // 8, 8, tile.shape[1]), axis=0)


def attn_kernel(q_ref, k_ref, v_ref, do_ref, ot_ref, dqkv_ref, s_ref, dp_ref, dk_ref, dv_ref, kt_ref, vt_ref, acc_ref):
    step = pl.program_id(0)
    last = pl.num_programs(0) - 1
    qi = last - step

    @pl.when(step == 0)
    def _():
        dk_ref[...] = jnp.zeros_like(dk_ref)
        dv_ref[...] = jnp.zeros_like(dv_ref)
        kt_ref[...] = k_ref[...].T
        vt_ref[...] = v_ref[...].T

    lane = lax.broadcasted_iota(jnp.int32, (BLK, 128), 1)
    q_wide = q_ref[...].astype(F32) * 0.125
    do_wide = do_ref[...].astype(F32)
    qs, dos = [], []
    for h in range(2):
        keep = (lane < 64) if h == 0 else (lane >= 64)
        qs.append(jnp.where(keep, q_wide, 0.0).astype(BF16))
        dos.append(jnp.where(keep, do_wide, 0.0).astype(BF16))

    def score(j, top, masked):
        rows = pl.ds(pl.multiple_of(j * BLK, BLK), BLK)
        k_blk = k_ref[rows, :]
        out = []
        for h in range(2):
            tile = lax.dot_general(k_blk, qs[h], NT, preferred_element_type=F32)
            if masked:
                key = lax.broadcasted_iota(jnp.int32, (BLK, BLK), 0)
                qry = lax.broadcasted_iota(jnp.int32, (BLK, BLK), 1)
                tile = jnp.where(key <= qry, tile, -1e30)
            s_ref[h, rows, :] = tile
            out.append(jnp.maximum(top[h], fold_rows(jnp.max, tile)))
        return tuple(out)

    low = jnp.full((8, BLK), -1e30, F32)
    top = score(qi, (low, low), True)
    top = lax.fori_loop(0, qi, lambda j, t: score(j, t, False), top)
    top = [jnp.max(t, axis=0, keepdims=True) for t in top]

    def expo(j, tot):
        rows = pl.ds(pl.multiple_of(j * BLK, BLK), BLK)
        out = []
        for h in range(2):
            tile = jnp.exp(s_ref[h, rows, :] - top[h])
            s_ref[h, rows, :] = tile
            out.append(tot[h] + fold_rows(jnp.sum, tile))
        return tuple(out)

    zero8 = jnp.zeros((8, BLK), F32)
    tot = lax.fori_loop(0, qi + 1, expo, (zero8, zero8))
    inv = [1.0 / jnp.sum(t, axis=0, keepdims=True) for t in tot]

    acc_ref[...] = jnp.zeros_like(acc_ref)

    def third(j, proj):
        rows = pl.ds(pl.multiple_of(j * BLK, BLK), BLK)
        v_blk = v_ref[rows, :]
        proj_new = []
        for h in range(2):
            prob = s_ref[h, rows, :] * inv[h]
            s_ref[h, rows, :] = prob
            prob_lo = prob.astype(BF16)
            d_prob = lax.dot_general(v_blk, dos[h], NT, preferred_element_type=F32)
            dp_ref[h, rows, :] = d_prob
            proj_new.append(proj[h] + fold_rows(jnp.sum, prob * d_prob))
            dv_ref[rows, :] += jnp.dot(prob_lo, dos[h], preferred_element_type=F32)
            acc_ref[h] += jnp.dot(vt_ref[h * 64:(h + 1) * 64, rows], prob_lo, preferred_element_type=F32)
        return tuple(proj_new)

    proj = lax.fori_loop(0, qi + 1, third, (zero8, zero8))
    for h in range(2):
        ot_ref[h * 64:(h + 1) * 64, :] = acc_ref[h].astype(BF16)
    proj = [jnp.sum(t, axis=0, keepdims=True) for t in proj]

    acc_ref[...] = jnp.zeros_like(acc_ref)

    def fourth(j, none):
        rows = pl.ds(pl.multiple_of(j * BLK, BLK), BLK)
        for h in range(2):
            d_s = (s_ref[h, rows, :] * (dp_ref[h, rows, :] - proj[h])).astype(BF16)
            dk_ref[rows, :] += jnp.dot(d_s, qs[h], preferred_element_type=F32)
            acc_ref[h] += jnp.dot(kt_ref[h * 64:(h + 1) * 64, rows], d_s, preferred_element_type=F32)
        return none

    lax.fori_loop(0, qi + 1, fourth, 0)
    dq = acc_ref[...].reshape(128, BLK) * 0.125
    rows = pl.ds(pl.multiple_of(qi * BLK, BLK), BLK)
    dqkv_ref[rows, 0:128] = dq.T.astype(BF16)

    @pl.when(step == last)
    def _():
        dqkv_ref[:, 128:256] = dk_ref[...].astype(BF16)
        dqkv_ref[:, 256:384] = dv_ref[...].astype(BF16)


def attn_pair(pair, qkv, d_attn):
    toks = qkv.shape[0]
    steps = toks // BLK
    return pl.pallas_call(
        attn_kernel,
        grid=(steps,),
        in_specs=[pl.BlockSpec((BLK, 128), lambda s: (steps - 1 - s, pair)),
                  pl.BlockSpec((toks, 128), lambda s: (0, 2 + pair)),
                  pl.BlockSpec((toks, 128), lambda s: (0, 4 + pair)),
                  pl.BlockSpec((BLK, 128), lambda s: (steps - 1 - s, pair))],
        out_specs=[pl.BlockSpec((128, BLK), lambda s: (0, steps - 1 - s)),
                   pl.BlockSpec((toks, 384), lambda s: (0, 0))],
        out_shape=[jax.ShapeDtypeStruct((128, toks), BF16), jax.ShapeDtypeStruct((toks, 384), BF16)],
        scratch_shapes=[pltpu.VMEM((2, toks, BLK), F32), pltpu.VMEM((2, toks, BLK), F32),
                        pltpu.VMEM((toks, 128), F32), pltpu.VMEM((toks, 128), F32),
                        pltpu.VMEM((128, toks), BF16), pltpu.VMEM((128, toks), BF16), pltpu.VMEM((2, 64, BLK), F32)],
        compiler_params=pltpu.CompilerParams(dimension_semantics=("arbitrary",), vmem_limit_bytes=20 << 20),
        cost_estimate=pl.CostEstimate(flops=16 * 10**9, bytes_accessed=4 << 20, transcendentals=0),
    )(qkv, qkv, qkv, d_attn)


def mlp_kernel(part, na_ref, da_ref, nb_ref, db_ref, wu_ref, wd_ref, pu_hbm, pd_hbm, *rest):
    gu_ref, gd_ref, au_ref, ad_ref, pu_ref, pd_ref, n_ref, nt_ref, d_ref, sem = rest[-10:]
    step = pl.program_id(0)
    half = pl.num_programs(0) // 2
    cols = au_ref.shape[1]
    load_u = pltpu.make_async_copy(pu_hbm.at[:, part * cols:(part + 1) * cols], pu_ref, sem.at[0])
    load_d = pltpu.make_async_copy(pd_hbm.at[part * cols:(part + 1) * cols, :], pd_ref, sem.at[1])

    @pl.when(step == 0)
    def _():
        load_u.start()
        load_d.start()
        au_ref[...] = jnp.zeros_like(au_ref)
        ad_ref[...] = jnp.zeros_like(ad_ref)

    for when, n_in, d_in in ((step < half, na_ref, da_ref), (step >= half, nb_ref, db_ref)):
        @pl.when(when)
        def _():
            n_ref[...] = n_in[...]
            d_ref[...] = d_in[...]

    nt_ref[...] = n_ref[...].T
    for c in range(0, cols, BLK):
        sl = slice(c, c + BLK)
        pre = jnp.dot(n_ref[...], wu_ref[:, sl], preferred_element_type=F32).astype(BF16)
        act, slope = gelu_pair(pre)
        d_act = lax.dot_general(d_ref[...], wd_ref[sl, :], NT, preferred_element_type=F32)
        d_pre = (d_act * slope).astype(BF16)
        au_ref[:, sl] += jnp.dot(nt_ref[...], d_pre, preferred_element_type=F32)
        ad_ref[sl, :] += lax.dot_general(act.astype(BF16), d_ref[...], TN, preferred_element_type=F32)

    @pl.when(step == pl.num_programs(0) - 1)
    def _():
        load_u.wait()
        load_d.wait()
        gu_ref[...] = (au_ref[...] + pu_ref[...]).astype(BF16)
        gd_ref[...] = (ad_ref[...] + pd_ref[...]).astype(BF16)


def mlp_grad(part, n_a, d_a, n_b, d_b, w_up, w_down, part_up, part_down, prev=()):
    rows, dim = n_a.shape
    cols = w_up.shape[1] // 2
    blk = 384
    half = rows // blk
    first = pl.BlockSpec((blk, dim), lambda s: (jnp.minimum(s, half - 1), 0))
    second = pl.BlockSpec((blk, dim), lambda s: (jnp.maximum(s - half, 0), 0))
    half_up = pl.BlockSpec((dim, cols), lambda s: (0, part))
    half_down = pl.BlockSpec((cols, dim), lambda s: (part, 0))
    any_spec = pl.BlockSpec(memory_space=pl.ANY)
    return pl.pallas_call(
        functools.partial(mlp_kernel, part),
        grid=(2 * half,),
        in_specs=[first, first, second, second, half_up, half_down, any_spec, any_spec] + [any_spec] * len(prev),
        out_specs=[half_up, half_down],
        out_shape=[jax.ShapeDtypeStruct(w_up.shape, BF16), jax.ShapeDtypeStruct(w_down.shape, BF16)],
        scratch_shapes=[pltpu.VMEM((dim, cols), F32), pltpu.VMEM((cols, dim), F32),
                        pltpu.VMEM((dim, cols), F32), pltpu.VMEM((cols, dim), F32),
                        pltpu.VMEM((blk, dim), BF16), pltpu.VMEM((dim, blk), BF16), pltpu.VMEM((blk, dim), BF16),
                        pltpu.SemaphoreType.DMA((2,))],
        input_output_aliases={8: 0, 9: 1} if prev else {},
        compiler_params=pltpu.CompilerParams(dimension_semantics=("arbitrary",), vmem_limit_bytes=44 << 20),
        cost_estimate=pl.CostEstimate(flops=8 * 10**9, bytes_accessed=14 << 20, transcendentals=0),
    )(n_a, d_a, n_b, d_b, w_up, w_down, part_up, part_down, *prev)


HALVES = (('hi', 1), ('lo', 0))


def solution(mesh):
    row_spec = P(('pod', 'dp'), None)
    stat_spec = P(('pod', 'dp'))
    in_specs = (row_spec, row_spec, stat_spec, stat_spec, stat_spec, stat_spec, P(None), P(None), row_spec,
                P(None, None, 'tp', None), P('tp', None, None), P(None, 'tp'), P('tp', None))
    out_specs = (row_spec, P('pod', None, 'tp', None), P(('pod', 'tp'), None, None), P('pod', 'tp'), P(('pod', 'tp'), None))

    def swap(kind, arr):
        axis, perm = {'c': ('tp', [(0, 1), (1, 0), (2, 3), (3, 2)]), 'x': ('tp', [(0, 2), (2, 0), (1, 3), (3, 1)]),
                      'y': ('dp', [(0, 1), (1, 0)])}[kind]
        return lax.ppermute(arr, axis, perm)

    def take_half(arr, which):
        rows = arr.shape[0] // 2
        return lax.dynamic_slice_in_dim(arr, which * rows, rows, 0)

    def join_halves(mine, other, which):
        return jnp.concatenate([jnp.where(which == 0, mine, other), jnp.where(which == 0, other, mine)], axis=0)

    def inner(x_saved, h_saved, mean_one, rstd_one, mean_two, rstd_two, gain_one, gain_two, grad_y, w_qkv, w_proj, w_up, w_down):
        core = lax.axis_index('tp') % 2
        dp_idx = lax.axis_index('dp')
        toks, dim = x_saved.shape
        part_of = lambda arr, i: arr[i * (toks // 2):(i + 1) * (toks // 2)]
        own_rows = lambda arr, i: lax.dynamic_slice_in_dim(arr, i * (toks // 2) + core * (toks // 4), toks // 4, 0)

        n_mine = layer_norm(take_half(h_saved, core), take_half(mean_two, core), take_half(rstd_two, core), gain_two)[1]
        norm_y, dy_y = swap('y', n_mine), swap('y', take_half(grad_y, core))
        norm_c, dy_c = swap('c', norm_y), swap('c', dy_y)

        def tp_sum(part):
            chip = (take_half(part, core).astype(F32) + swap('c', take_half(part, 1 - core)).astype(F32)).astype(BF16)
            return chip.astype(F32) + swap('x', chip).astype(F32)

        def back(total, rows, mean, rstd, gain):
            hat = (rows.astype(F32) - mean[:, None]) * rstd[:, None]
            return norm_back(total, hat, rstd, gain)

        norm_two, act, d_pre, d_norm = {}, {}, {}, {}
        for tag, i in HALVES:
            norm_two[tag] = layer_norm(part_of(h_saved, i), part_of(mean_two, i), part_of(rstd_two, i), gain_two)[1]
            pre_act = jnp.dot(norm_two[tag], w_up, preferred_element_type=F32).astype(BF16)
            gelu_val, gelu_slope = gelu_pair(pre_act)
            act[tag] = gelu_val.astype(BF16)
            d_pre[tag] = (lax.dot_general(part_of(grad_y, i), w_down, NT, preferred_element_type=F32) * gelu_slope).astype(BF16)
            part = lax.dot_general(d_pre[tag], w_up, NT, preferred_element_type=F32).astype(BF16)
            d_norm[tag] = tp_sum(part)

        part_down = sum(lax.dot_general(act[tag], part_of(grad_y, i), TN, preferred_element_type=F32) for tag, i in HALVES)
        part_up = sum(lax.dot_general(norm_two[tag], d_pre[tag], TN, preferred_element_type=F32) for tag, i in HALVES)

        w_t = w_qkv.transpose(1, 2, 3, 0).reshape(-1, dim)
        norm_one = layer_norm(x_saved, mean_one, rstd_one, gain_one)[1]
        qkv = lax.dot_general(norm_one, w_t, NT, preferred_element_type=F32).astype(BF16)

        w_o = w_proj.reshape(-1, dim)
        d_mid, mid_lo, d_attn = {}, {}, {}
        for tag, i in HALVES:
            mine = [own_rows(a, i) for a in (grad_y, h_saved, mean_two, rstd_two)]
            if tag == 'lo':
                mine[2], mine[3], low = lax.optimization_barrier((mine[2], mine[3], low))
            d_mid[tag] = mine[0].astype(F32) + back(d_norm[tag], *mine[1:], gain_two)
            low = d_mid[tag].astype(BF16)
            mid_lo[tag] = join_halves(low, swap('c', low), core)
            d_attn[tag] = lax.dot_general(mid_lo[tag], w_o, NT, preferred_element_type=F32).astype(BF16)
        d_attn = jnp.concatenate([d_attn['lo'], d_attn['hi']], axis=0)
        mid_all = jnp.concatenate([mid_lo['lo'], mid_lo['hi']], axis=0)

        w_pairs = w_t.reshape(3, 2, 128, dim)
        halves, d_pair = [], []
        for pair in range(2):
            o_t, d_qkv = attn_pair(pair, qkv, d_attn)
            d_pair.append(d_qkv)
            g_qkv = lax.dot_general(d_qkv, norm_one, TN, preferred_element_type=F32)
            g_o = jnp.dot(o_t, mid_all, preferred_element_type=F32)
            mine = jnp.concatenate([take_half(g, dp_idx) for g in (g_qkv, g_o)], 0)
            theirs = jnp.concatenate([take_half(g, 1 - dp_idx) for g in (g_qkv, g_o)], 0)
            summed = (mine + swap('y', theirs)).astype(BF16)
            other = swap('y', summed)
            halves.append((join_halves(summed[:192], other[:192], dp_idx), join_halves(summed[192:], other[192:], dp_idx)))

        w_pair = [w_pairs[:, p].reshape(-1, dim) for p in range(2)]
        part_one = jnp.dot(d_pair[0], w_pair[0], preferred_element_type=F32)
        grad_x = {}
        for tag, i in HALVES:
            part = (part_of(part_one, i) + jnp.dot(part_of(d_pair[1], i), w_pair[1], preferred_element_type=F32)).astype(BF16)
            total = tp_sum(part)
            mine = [own_rows(a, i) for a in (x_saved, mean_one, rstd_one)]
            if tag == 'lo':
                mine[1], mine[2], low = lax.optimization_barrier((mine[1], mine[2], low))
            low = (d_mid[tag] + back(total, *mine, gain_one)).astype(BF16)
            grad_x[tag] = join_halves(low, swap('c', low), core)
        grad_x = jnp.concatenate([grad_x['lo'], grad_x['hi']], axis=0)

        grads = ()
        for part in range(2):
            grads = mlp_grad(part, norm_y, dy_y, norm_c, dy_c, w_up, w_down, part_up, part_down, tuple(grads))
        grad_up, grad_down = grads
        g_t = jnp.stack([h[0].reshape(3, 2, 64, dim) for h in halves], axis=1).reshape(3, 4, 64, dim)
        grad_qkv = g_t.transpose(3, 0, 1, 2)
        grad_proj = jnp.concatenate([h[1] for h in halves], axis=0).reshape(4, 64, dim)
        return grad_x, grad_qkv, grad_proj, grad_up, grad_down

    return jax.shard_map(inner, mesh=mesh, in_specs=in_specs, out_specs=out_specs, check_vma=False)
```

```python
import math

import jax
import jax.numpy as jnp
from jax import lax
from jax.experimental import pallas as pl
from jax.experimental.pallas import tpu as pltpu
from jax.sharding import PartitionSpec as P


GELU_C = math.sqrt(2.0 / math.pi)
F32 = jnp.float32
BF16 = jnp.bfloat16
NT = (((1,), (1,)), ((), ()))
TN = (((0,), (0,)), ((), ()))
BLK = 256


def layer_norm(row_vals, row_mean, row_rstd, gain_vec):
    x_hat = (row_vals.astype(F32) - row_mean[:, None]) * row_rstd[:, None]
    return x_hat, (x_hat * gain_vec.astype(F32)).astype(BF16)


def norm_back(d_norm, x_hat, row_rstd, gain_vec):
    scaled = d_norm * gain_vec.astype(F32)
    scaled_mean = jnp.mean(scaled, axis=-1, keepdims=True)
    proj_mean = jnp.mean(scaled * x_hat, axis=-1, keepdims=True)
    return row_rstd[:, None] * (scaled - scaled_mean - x_hat * proj_mean)


def gelu_pair(pre_act):
    pre_wide = pre_act.astype(F32)
    tanh_val = jnp.tanh(GELU_C * (pre_wide + 0.044715 * pre_wide * pre_wide * pre_wide))
    gelu_val = 0.5 * pre_wide * (1.0 + tanh_val)
    gelu_slope = 0.5 * (1.0 + tanh_val) + 0.5 * pre_wide * (1.0 - tanh_val * tanh_val) * GELU_C * (1.0 + 0.134145 * pre_wide * pre_wide)
    return gelu_val, gelu_slope


def fold_rows(op, tile):
    return op(tile.reshape(tile.shape[0] // 8, 8, tile.shape[1]), axis=0)


BQ = 512


def attn_kernel(q_ref, k_ref, v_ref, do_ref, ot_ref, dqkv_ref, s_ref, dp_ref, dk_ref, dv_ref, kt_ref, vt_ref, acc_ref):
    step = pl.program_id(0)
    last = pl.num_programs(0) - 1
    qi = last - step
    per = BQ // BLK
    full = qi * per

    @pl.when(step == 0)
    def _():
        dk_ref[...] = jnp.zeros_like(dk_ref)
        dv_ref[...] = jnp.zeros_like(dv_ref)
        kt_ref[...] = k_ref[...].T
        vt_ref[...] = v_ref[...].T

    lane = lax.broadcasted_iota(jnp.int32, (BQ, 128), 1)
    q_wide = q_ref[...].astype(F32) * 0.125
    do_wide = do_ref[...].astype(F32)
    qs, dos = [], []
    for h in range(2):
        keep = (lane < 64) if h == 0 else (lane >= 64)
        qs.append(jnp.where(keep, q_wide, 0.0).astype(BF16))
        dos.append(jnp.where(keep, do_wide, 0.0).astype(BF16))

    def at(j):
        return pl.ds(pl.multiple_of(j * BLK, BLK), BLK)

    def score(j, top, shift):
        rows = at(j)
        k_blk = k_ref[rows, :]
        out = []
        for h in range(2):
            tile = lax.dot_general(k_blk, qs[h], NT, preferred_element_type=F32)
            if shift is not None:
                key = lax.broadcasted_iota(jnp.int32, (BLK, BQ), 0) + shift
                qry = lax.broadcasted_iota(jnp.int32, (BLK, BQ), 1)
                tile = jnp.where(key <= qry, tile, -1e30)
            s_ref[h, rows, :] = tile
            out.append(jnp.maximum(top[h], fold_rows(jnp.max, tile)))
        return tuple(out)

    low = jnp.full((8, BQ), -1e30, F32)
    top = lax.fori_loop(0, per, lambda i, t: score(full + i, t, i * BLK), (low, low))
    top = lax.fori_loop(0, full, lambda j, t: score(j, t, None), top)
    top = [jnp.max(t, axis=0, keepdims=True) for t in top]

    def expo(j, tot):
        rows = at(j)
        out = []
        for h in range(2):
            tile = jnp.exp(s_ref[h, rows, :] - top[h])
            s_ref[h, rows, :] = tile
            out.append(tot[h] + fold_rows(jnp.sum, tile))
        return tuple(out)

    zero8 = jnp.zeros((8, BQ), F32)
    tot = lax.fori_loop(0, full + per, expo, (zero8, zero8))
    inv = [1.0 / jnp.sum(t, axis=0, keepdims=True) for t in tot]
    acc_ref[...] = jnp.zeros_like(acc_ref)

    def third(j, proj):
        rows = at(j)
        v_blk = v_ref[rows, :]
        proj_new = []
        for h in range(2):
            prob = s_ref[h, rows, :] * inv[h]
            s_ref[h, rows, :] = prob
            prob_lo = prob.astype(BF16)
            d_prob = lax.dot_general(v_blk, dos[h], NT, preferred_element_type=F32)
            dp_ref[h, rows, :] = d_prob
            proj_new.append(proj[h] + fold_rows(jnp.sum, prob * d_prob))
            dv_ref[rows, :] += jnp.dot(prob_lo, dos[h], preferred_element_type=F32)
            acc_ref[h] += jnp.dot(vt_ref[h * 64:(h + 1) * 64, rows], prob_lo, preferred_element_type=F32)
        return tuple(proj_new)

    proj = lax.fori_loop(0, full + per, third, (zero8, zero8))
    for h in range(2):
        ot_ref[h * 64:(h + 1) * 64, :] = acc_ref[h].astype(BF16)
    proj = [jnp.sum(t, axis=0, keepdims=True) for t in proj]
    acc_ref[...] = jnp.zeros_like(acc_ref)

    def fourth(j, none):
        rows = at(j)
        for h in range(2):
            d_s = (s_ref[h, rows, :] * (dp_ref[h, rows, :] - proj[h])).astype(BF16)
            dk_ref[rows, :] += jnp.dot(d_s, qs[h], preferred_element_type=F32)
            acc_ref[h] += jnp.dot(kt_ref[h * 64:(h + 1) * 64, rows], d_s, preferred_element_type=F32)
        return none

    lax.fori_loop(0, full + per, fourth, 0)
    dq = acc_ref[...].reshape(128, BQ) * 0.125
    dqkv_ref[pl.ds(pl.multiple_of(qi * BQ, BQ), BQ), 0:128] = dq.T.astype(BF16)

    @pl.when(step == last)
    def _():
        dqkv_ref[:, 128:256] = dk_ref[...].astype(BF16)
        dqkv_ref[:, 256:384] = dv_ref[...].astype(BF16)


def attn_pair(pair, qkv, d_attn):
    toks = qkv.shape[0]
    steps = toks // BQ
    return pl.pallas_call(
        attn_kernel,
        grid=(steps,),
        in_specs=[pl.BlockSpec((BQ, 128), lambda s: (steps - 1 - s, pair)),
                  pl.BlockSpec((toks, 128), lambda s: (0, 2 + pair)),
                  pl.BlockSpec((toks, 128), lambda s: (0, 4 + pair)),
                  pl.BlockSpec((BQ, 128), lambda s: (steps - 1 - s, pair))],
        out_specs=[pl.BlockSpec((128, BQ), lambda s: (0, steps - 1 - s)),
                   pl.BlockSpec((toks, 384), lambda s: (0, 0))],
        out_shape=[jax.ShapeDtypeStruct((128, toks), BF16), jax.ShapeDtypeStruct((toks, 384), BF16)],
        scratch_shapes=[pltpu.VMEM((2, toks, BQ), F32), pltpu.VMEM((2, toks, BQ), F32),
                        pltpu.VMEM((toks, 128), F32), pltpu.VMEM((toks, 128), F32),
                        pltpu.VMEM((128, toks), BF16), pltpu.VMEM((128, toks), BF16), pltpu.VMEM((2, 64, BQ), F32)],
        compiler_params=pltpu.CompilerParams(dimension_semantics=("arbitrary",), vmem_limit_bytes=30 << 20),
        cost_estimate=pl.CostEstimate(flops=16 * 10**9, bytes_accessed=4 << 20, transcendentals=0),
    )(qkv, qkv, qkv, d_attn)


def mlp_kernel(nh_ref, nl_ref, dy_ref, na_ref, nb_ref, da_ref, db_ref, gh_ref, gl_ref, ph_ref, pl_ref, wu_ref, wd_ref, *rest):
    gu_ref, gd_ref, nt_ref, gt_ref, dp_ref = rest[-5:]
    rows = nh_ref.shape[0]

    @pl.when(pl.program_id(0) == 0)
    def _():
        for i, ref in enumerate((nl_ref, nh_ref, na_ref, nb_ref)):
            nt_ref[:, i * rows:(i + 1) * rows] = ref[...].T

    for i, (g_ref, p_ref) in enumerate(((gl_ref, pl_ref), (gh_ref, ph_ref))):
        gt_ref[:, i * rows:(i + 1) * rows] = g_ref[...].T
        dp_ref[i * rows:(i + 1) * rows, :] = p_ref[...]
    sub = rows // 2
    for i, (n_ref, d_ref) in enumerate(((na_ref, da_ref), (nb_ref, db_ref))):
        for r in range(2):
            sl = slice(r * sub, (r + 1) * sub)
            at = slice((2 + i) * rows + r * sub, (2 + i) * rows + (r + 1) * sub)
            act, slope = gelu_pair(jnp.dot(n_ref[sl, :], wu_ref[...], preferred_element_type=F32).astype(BF16))
            d_act = lax.dot_general(d_ref[sl, :], wd_ref[...], NT, preferred_element_type=F32)
            dp_ref[at, :] = (d_act * slope).astype(BF16)
            gt_ref[:, at] = act.astype(BF16).T
    gu_ref[...] = jnp.dot(nt_ref[...], dp_ref[...], preferred_element_type=F32).astype(BF16)
    total = jnp.dot(gt_ref[:, :2 * rows], dy_ref[...], preferred_element_type=F32)
    total += jnp.dot(gt_ref[:, 2 * rows:3 * rows], da_ref[...], preferred_element_type=F32)
    total += jnp.dot(gt_ref[:, 3 * rows:], db_ref[...], preferred_element_type=F32)
    gd_ref[...] = total.astype(BF16)


def mlp_grad(first, count, own, other, saved, w_up, w_down, prev=()):
    dim = w_up.shape[0]
    rows = own[0].shape[0]
    once = lambda a: pl.BlockSpec(a.shape, lambda s: (0, 0), pipeline_mode=pl.Buffered(1))
    cols = lambda n: pl.BlockSpec((n, BLK), lambda s: (0, first + s))
    down = pl.BlockSpec((BLK, dim), lambda s: (first + s, 0))
    any_spec = pl.BlockSpec(memory_space=pl.ANY)
    return pl.pallas_call(
        mlp_kernel,
        grid=(count,),
        in_specs=[once(a) for a in (*own, *other)] + [cols(rows)] * 4 + [cols(dim), down] + [any_spec] * len(prev),
        out_specs=[cols(dim), down],
        out_shape=[jax.ShapeDtypeStruct(w_up.shape, BF16), jax.ShapeDtypeStruct(w_down.shape, BF16)],
        scratch_shapes=[pltpu.VMEM((dim, 4 * rows), BF16), pltpu.VMEM((BLK, 4 * rows), BF16), pltpu.VMEM((4 * rows, BLK), BF16)],
        input_output_aliases={13: 0, 14: 1} if prev else {},
        compiler_params=pltpu.CompilerParams(dimension_semantics=("arbitrary",), vmem_limit_bytes=44 << 20),
        cost_estimate=pl.CostEstimate(flops=5 * count * 10**9, bytes_accessed=14 << 20, transcendentals=0),
    )(*own, *other, *saved, w_up, w_down, *prev)


HALVES = (('hi', 1), ('lo', 0))
SPLIT = ((0, 3), (3, 1))


def solution(mesh):
    row_spec = P(('pod', 'dp'), None)
    stat_spec = P(('pod', 'dp'))
    in_specs = (row_spec, row_spec, stat_spec, stat_spec, stat_spec, stat_spec, P(None), P(None), row_spec,
                P(None, None, 'tp', None), P('tp', None, None), P(None, 'tp'), P('tp', None))
    out_specs = (row_spec, P('pod', None, 'tp', None), P(('pod', 'tp'), None, None), P('pod', 'tp'), P(('pod', 'tp'), None))

    def swap(kind, arr):
        axis, perm = {'c': ('tp', [(0, 1), (1, 0), (2, 3), (3, 2)]), 'x': ('tp', [(0, 2), (2, 0), (1, 3), (3, 1)]),
                      'y': ('dp', [(0, 1), (1, 0)])}[kind]
        return lax.ppermute(arr, axis, perm)

    def take_half(arr, which):
        rows = arr.shape[0] // 2
        return lax.dynamic_slice_in_dim(arr, which * rows, rows, 0)

    def join_halves(mine, other, which):
        return jnp.concatenate([jnp.where(which == 0, mine, other), jnp.where(which == 0, other, mine)], axis=0)

    def inner(x_saved, h_saved, mean_one, rstd_one, mean_two, rstd_two, gain_one, gain_two, grad_y, w_qkv, w_proj, w_up, w_down):
        core = lax.axis_index('tp') % 2
        dp_idx = lax.axis_index('dp')
        toks, dim = x_saved.shape
        part_of = lambda arr, i: arr[i * (toks // 2):(i + 1) * (toks // 2)]
        own_rows = lambda arr, i: lax.dynamic_slice_in_dim(arr, i * (toks // 2) + core * (toks // 4), toks // 4, 0)

        n_mine = layer_norm(take_half(h_saved, core), take_half(mean_two, core), take_half(rstd_two, core), gain_two)[1]
        norm_y, dy_y = swap('y', n_mine), swap('y', take_half(grad_y, core))
        norm_c, dy_c = swap('c', norm_y), swap('c', dy_y)

        def tp_sum(part):
            chip = (take_half(part, core).astype(F32) + swap('c', take_half(part, 1 - core)).astype(F32)).astype(BF16)
            return chip.astype(F32) + swap('x', chip).astype(F32)

        def back(total, rows, mean, rstd, gain):
            hat = (rows.astype(F32) - mean[:, None]) * rstd[:, None]
            return norm_back(total, hat, rstd, gain)

        norm_two, act, d_pre, d_norm = {}, {}, {}, {}
        for tag, i in HALVES:
            norm_two[tag] = layer_norm(part_of(h_saved, i), part_of(mean_two, i), part_of(rstd_two, i), gain_two)[1]
            pre_act = jnp.dot(norm_two[tag], w_up, preferred_element_type=F32).astype(BF16)
            gelu_val, gelu_slope = gelu_pair(pre_act)
            act[tag] = gelu_val.astype(BF16)
            d_pre[tag] = (lax.dot_general(part_of(grad_y, i), w_down, NT, preferred_element_type=F32) * gelu_slope).astype(BF16)
            part = lax.dot_general(d_pre[tag], w_up, NT, preferred_element_type=F32).astype(BF16)
            d_norm[tag] = tp_sum(part)

        w_t = w_qkv.transpose(1, 2, 3, 0).reshape(-1, dim)
        norm_one = layer_norm(x_saved, mean_one, rstd_one, gain_one)[1]
        qkv = lax.dot_general(norm_one, w_t, NT, preferred_element_type=F32).astype(BF16)

        w_o = w_proj.reshape(-1, dim)
        d_mid, mid_lo, d_attn = {}, {}, {}
        for tag, i in HALVES:
            mine = [own_rows(a, i) for a in (grad_y, h_saved, mean_two, rstd_two)]
            if tag == 'lo':
                mine[2], mine[3], low = lax.optimization_barrier((mine[2], mine[3], low))
            d_mid[tag] = mine[0].astype(F32) + back(d_norm[tag], *mine[1:], gain_two)
            low = d_mid[tag].astype(BF16)
            mid_lo[tag] = join_halves(low, swap('c', low), core)
            d_attn[tag] = lax.dot_general(mid_lo[tag], w_o, NT, preferred_element_type=F32).astype(BF16)
        d_attn = jnp.concatenate([d_attn['lo'], d_attn['hi']], axis=0)
        mid_all = jnp.concatenate([mid_lo['lo'], mid_lo['hi']], axis=0)

        w_pairs = w_t.reshape(3, 2, 128, dim)
        halves, d_pair = [], []
        for pair in range(2):
            o_t, d_qkv = attn_pair(pair, qkv, d_attn)
            d_pair.append(d_qkv)
            g_qkv = lax.dot_general(d_qkv, norm_one, TN, preferred_element_type=F32)
            g_o = jnp.dot(o_t, mid_all, preferred_element_type=F32)
            mine = jnp.concatenate([take_half(g, dp_idx) for g in (g_qkv, g_o)], 0)
            theirs = jnp.concatenate([take_half(g, 1 - dp_idx) for g in (g_qkv, g_o)], 0)
            summed = (mine + swap('y', theirs)).astype(BF16)
            other = swap('y', summed)
            halves.append((join_halves(summed[:192], other[:192], dp_idx), join_halves(summed[192:], other[192:], dp_idx)))

        w_pair = [w_pairs[:, p].reshape(-1, dim) for p in range(2)]
        part_one = jnp.dot(d_pair[0], w_pair[0], preferred_element_type=F32)
        grad_x = {}
        for tag, i in HALVES:
            part = (part_of(part_one, i) + jnp.dot(part_of(d_pair[1], i), w_pair[1], preferred_element_type=F32)).astype(BF16)
            total = tp_sum(part)
            mine = [own_rows(a, i) for a in (x_saved, mean_one, rstd_one)]
            if tag == 'lo':
                mine[1], mine[2], low = lax.optimization_barrier((mine[1], mine[2], low))
            low = (d_mid[tag] + back(total, *mine, gain_one)).astype(BF16)
            grad_x[tag] = join_halves(low, swap('c', low), core)
        grad_x = jnp.concatenate([grad_x['lo'], grad_x['hi']], axis=0)

        own = (norm_two['hi'], norm_two['lo'], grad_y)
        grads = ()
        for part, (first, count) in enumerate(SPLIT):
            grads = mlp_grad(first, count, own, (norm_y, norm_c, dy_y, dy_c), (act['hi'], act['lo'], d_pre['hi'], d_pre['lo']),
                             w_up, w_down, tuple(grads))
        grad_up, grad_down = grads
        g_t = jnp.stack([h[0].reshape(3, 2, 64, dim) for h in halves], axis=1).reshape(3, 4, 64, dim)
        grad_qkv = g_t.transpose(3, 0, 1, 2)
        grad_proj = jnp.concatenate([h[1] for h in halves], axis=0).reshape(4, 64, dim)
        return grad_x, grad_qkv, grad_proj, grad_up, grad_down

    return jax.shard_map(inner, mesh=mesh, in_specs=in_specs, out_specs=out_specs, check_vma=False)
```

```python
import math

import jax
import jax.numpy as jnp
from jax import lax
from jax.experimental import pallas as pl
from jax.experimental.pallas import tpu as pltpu
from jax.sharding import PartitionSpec as P


GELU_C = math.sqrt(2.0 / math.pi)
F32 = jnp.float32
BF16 = jnp.bfloat16
NT = (((1,), (1,)), ((), ()))
TN = (((0,), (0,)), ((), ()))
BLK = 256


def layer_norm(row_vals, row_mean, row_rstd, gain_vec):
    x_hat = (row_vals.astype(F32) - row_mean[:, None]) * row_rstd[:, None]
    return x_hat, (x_hat * gain_vec.astype(F32)).astype(BF16)


def norm_back(d_norm, x_hat, row_rstd, gain_vec):
    scaled = d_norm * gain_vec.astype(F32)
    scaled_mean = jnp.mean(scaled, axis=-1, keepdims=True)
    proj_mean = jnp.mean(scaled * x_hat, axis=-1, keepdims=True)
    return row_rstd[:, None] * (scaled - scaled_mean - x_hat * proj_mean)


def gelu_pair(pre_act):
    pre_wide = pre_act.astype(F32)
    tanh_val = jnp.tanh(GELU_C * (pre_wide + 0.044715 * pre_wide * pre_wide * pre_wide))
    gelu_val = 0.5 * pre_wide * (1.0 + tanh_val)
    gelu_slope = 0.5 * (1.0 + tanh_val) + 0.5 * pre_wide * (1.0 - tanh_val * tanh_val) * GELU_C * (1.0 + 0.134145 * pre_wide * pre_wide)
    return gelu_val, gelu_slope


def fold_rows(op, tile):
    return op(tile.reshape(tile.shape[0] // 8, 8, tile.shape[1]), axis=0)


BQ = 512


def attn_kernel(q_ref, k_ref, v_ref, do_ref, ot_ref, dqkv_ref, s_ref, dp_ref, dk_ref, dv_ref, kt_ref, vt_ref, acc_ref):
    step = pl.program_id(0)
    last = pl.num_programs(0) - 1
    qi = last - step
    per = BQ // BLK
    full = qi * per

    @pl.when(step == 0)
    def _():
        dk_ref[...] = jnp.zeros_like(dk_ref)
        dv_ref[...] = jnp.zeros_like(dv_ref)
        kt_ref[...] = k_ref[...].T
        vt_ref[...] = v_ref[...].T

    lane = lax.broadcasted_iota(jnp.int32, (BQ, 128), 1)
    q_wide = q_ref[...].astype(F32) * 0.125
    do_wide = do_ref[...].astype(F32)
    qs, dos = [], []
    for h in range(2):
        keep = (lane < 64) if h == 0 else (lane >= 64)
        qs.append(jnp.where(keep, q_wide, 0.0).astype(BF16))
        dos.append(jnp.where(keep, do_wide, 0.0).astype(BF16))

    def at(j):
        return pl.ds(pl.multiple_of(j * BLK, BLK), BLK)

    def score(j, top, shift):
        rows = at(j)
        k_blk = k_ref[rows, :]
        out = []
        for h in range(2):
            tile = lax.dot_general(k_blk, qs[h], NT, preferred_element_type=F32)
            if shift is not None:
                key = lax.broadcasted_iota(jnp.int32, (BLK, BQ), 0) + shift
                qry = lax.broadcasted_iota(jnp.int32, (BLK, BQ), 1)
                tile = jnp.where(key <= qry, tile, -1e30)
            s_ref[h, rows, :] = tile
            out.append(jnp.maximum(top[h], fold_rows(jnp.max, tile)))
        return tuple(out)

    low = jnp.full((8, BQ), -1e30, F32)
    top = lax.fori_loop(0, per, lambda i, t: score(full + i, t, i * BLK), (low, low))
    top = lax.fori_loop(0, full, lambda j, t: score(j, t, None), top)
    top = [jnp.max(t, axis=0, keepdims=True) for t in top]

    def expo(j, tot):
        rows = at(j)
        out = []
        for h in range(2):
            tile = jnp.exp(s_ref[h, rows, :] - top[h])
            s_ref[h, rows, :] = tile
            out.append(tot[h] + fold_rows(jnp.sum, tile))
        return tuple(out)

    zero8 = jnp.zeros((8, BQ), F32)
    tot = lax.fori_loop(0, full + per, expo, (zero8, zero8))
    inv = [1.0 / jnp.sum(t, axis=0, keepdims=True) for t in tot]
    acc_ref[...] = jnp.zeros_like(acc_ref)

    def third(j, proj):
        rows = at(j)
        v_blk = v_ref[rows, :]
        proj_new = []
        for h in range(2):
            prob = s_ref[h, rows, :] * inv[h]
            s_ref[h, rows, :] = prob
            prob_lo = prob.astype(BF16)
            d_prob = lax.dot_general(v_blk, dos[h], NT, preferred_element_type=F32)
            dp_ref[h, rows, :] = d_prob
            proj_new.append(proj[h] + fold_rows(jnp.sum, prob * d_prob))
            dv_ref[rows, :] += jnp.dot(prob_lo, dos[h], preferred_element_type=F32)
            acc_ref[h] += jnp.dot(vt_ref[h * 64:(h + 1) * 64, rows], prob_lo, preferred_element_type=F32)
        return tuple(proj_new)

    proj = lax.fori_loop(0, full + per, third, (zero8, zero8))
    for h in range(2):
        ot_ref[h * 64:(h + 1) * 64, :] = acc_ref[h].astype(BF16)
    proj = [jnp.sum(t, axis=0, keepdims=True) for t in proj]
    acc_ref[...] = jnp.zeros_like(acc_ref)

    def fourth(j, none):
        rows = at(j)
        for h in range(2):
            d_s = (s_ref[h, rows, :] * (dp_ref[h, rows, :] - proj[h])).astype(BF16)
            dk_ref[rows, :] += jnp.dot(d_s, qs[h], preferred_element_type=F32)
            acc_ref[h] += jnp.dot(kt_ref[h * 64:(h + 1) * 64, rows], d_s, preferred_element_type=F32)
        return none

    lax.fori_loop(0, full + per, fourth, 0)
    dq = acc_ref[...].reshape(128, BQ) * 0.125
    dqkv_ref[pl.ds(pl.multiple_of(qi * BQ, BQ), BQ), 0:128] = dq.T.astype(BF16)

    @pl.when(step == last)
    def _():
        dqkv_ref[:, 128:256] = dk_ref[...].astype(BF16)
        dqkv_ref[:, 256:384] = dv_ref[...].astype(BF16)


def attn_pair(pair, qkv, d_attn):
    toks = qkv.shape[0]
    steps = toks // BQ
    return pl.pallas_call(
        attn_kernel,
        grid=(steps,),
        in_specs=[pl.BlockSpec((BQ, 128), lambda s: (steps - 1 - s, pair)),
                  pl.BlockSpec((toks, 128), lambda s: (0, 2 + pair)),
                  pl.BlockSpec((toks, 128), lambda s: (0, 4 + pair)),
                  pl.BlockSpec((BQ, 128), lambda s: (steps - 1 - s, pair))],
        out_specs=[pl.BlockSpec((128, BQ), lambda s: (0, steps - 1 - s)),
                   pl.BlockSpec((toks, 384), lambda s: (0, 0))],
        out_shape=[jax.ShapeDtypeStruct((128, toks), BF16), jax.ShapeDtypeStruct((toks, 384), BF16)],
        scratch_shapes=[pltpu.VMEM((2, toks, BQ), F32), pltpu.VMEM((2, toks, BQ), F32),
                        pltpu.VMEM((toks, 128), F32), pltpu.VMEM((toks, 128), F32),
                        pltpu.VMEM((128, toks), BF16), pltpu.VMEM((128, toks), BF16), pltpu.VMEM((2, 64, BQ), F32)],
        compiler_params=pltpu.CompilerParams(dimension_semantics=("arbitrary",), vmem_limit_bytes=30 << 20),
        cost_estimate=pl.CostEstimate(flops=16 * 10**9, bytes_accessed=4 << 20, transcendentals=0),
    )(qkv, qkv, qkv, d_attn)


def own_kernel(nh_ref, nl_ref, dy_ref, ah_ref, pd_ref, al_ref, ph_ref, pl_ref, pu_ref, gu_ref, gd_ref, nt_ref, gt_ref, dp_ref):
    rows = nh_ref.shape[0]

    @pl.when(pl.program_id(0) == 0)
    def _():
        for i, ref in enumerate((nl_ref, nh_ref)):
            nt_ref[:, i * rows:(i + 1) * rows] = ref[...].T

    for i, (a_ref, p_ref) in enumerate(((al_ref, pl_ref), (ah_ref, ph_ref))):
        gt_ref[:, i * rows:(i + 1) * rows] = gelu_pair(a_ref[...])[0].astype(BF16).T
        dp_ref[i * rows:(i + 1) * rows, :] = p_ref[...]
    gu_ref[...] = (jnp.dot(nt_ref[...], dp_ref[...], preferred_element_type=F32) + pu_ref[...]).astype(BF16)
    gd_ref[...] = (jnp.dot(gt_ref[...], dy_ref[...], preferred_element_type=F32) + pd_ref[...]).astype(BF16)


def other_kernel(na_ref, nb_ref, da_ref, db_ref, wu_ref, wd_ref, gu_ref, gd_ref, nt_ref, gt_ref, dp_ref):
    rows = na_ref.shape[0]

    @pl.when(pl.program_id(0) == 0)
    def _():
        for i, ref in enumerate((na_ref, nb_ref)):
            nt_ref[:, i * rows:(i + 1) * rows] = ref[...].T

    sub = rows // 2
    for i, (n_ref, d_ref) in enumerate(((na_ref, da_ref), (nb_ref, db_ref))):
        for r in range(2):
            sl = slice(r * sub, (r + 1) * sub)
            at = slice(i * rows + r * sub, i * rows + (r + 1) * sub)
            act, slope = gelu_pair(jnp.dot(n_ref[sl, :], wu_ref[...], preferred_element_type=F32).astype(BF16))
            d_act = lax.dot_general(d_ref[sl, :], wd_ref[...], NT, preferred_element_type=F32)
            dp_ref[at, :] = (d_act * slope).astype(BF16)
            gt_ref[:, at] = act.astype(BF16).T
    gu_ref[...] = jnp.dot(nt_ref[...], dp_ref[...], preferred_element_type=F32)
    total = jnp.dot(gt_ref[:, :rows], da_ref[...], preferred_element_type=F32)
    total += jnp.dot(gt_ref[:, rows:], db_ref[...], preferred_element_type=F32)
    gd_ref[...] = total


def mlp_columns(kernel, whole, by_col, by_row, dim, cols, rows, out_type):
    once = lambda a: pl.BlockSpec(a.shape, lambda s: (0, 0), pipeline_mode=pl.Buffered(1))
    col = lambda n: pl.BlockSpec((n, BLK), lambda s: (0, s))
    row = lambda n: pl.BlockSpec((BLK, n), lambda s: (s, 0))
    args = whole + by_col[:1] + by_row[:1] + by_col[1:] + by_row[1:] if by_row else whole + by_col
    specs = [col(a.shape[0]) for a in by_col[:1]] + [row(a.shape[1]) for a in by_row[:1]] + [col(a.shape[0]) for a in by_col[1:]] + [row(a.shape[1]) for a in by_row[1:]]
    return pl.pallas_call(
        kernel,
        grid=(cols // BLK,),
        in_specs=[once(a) for a in whole] + specs,
        out_specs=[col(dim), row(dim)],
        out_shape=[jax.ShapeDtypeStruct((dim, cols), out_type), jax.ShapeDtypeStruct((cols, dim), out_type)],
        scratch_shapes=[pltpu.VMEM((dim, rows), BF16), pltpu.VMEM((BLK, rows), BF16), pltpu.VMEM((rows, BLK), BF16)],
        compiler_params=pltpu.CompilerParams(dimension_semantics=("arbitrary",), vmem_limit_bytes=36 << 20),
        cost_estimate=pl.CostEstimate(flops=16 * 10**9, bytes_accessed=14 << 20, transcendentals=0),
    )(*args)


HALVES = (('hi', 1), ('lo', 0))


def solution(mesh):
    row_spec = P(('pod', 'dp'), None)
    stat_spec = P(('pod', 'dp'))
    in_specs = (row_spec, row_spec, stat_spec, stat_spec, stat_spec, stat_spec, P(None), P(None), row_spec,
                P(None, None, 'tp', None), P('tp', None, None), P(None, 'tp'), P('tp', None))
    out_specs = (row_spec, P('pod', None, 'tp', None), P(('pod', 'tp'), None, None), P('pod', 'tp'), P(('pod', 'tp'), None))

    def swap(kind, arr):
        axis, perm = {'c': ('tp', [(0, 1), (1, 0), (2, 3), (3, 2)]), 'x': ('tp', [(0, 2), (2, 0), (1, 3), (3, 1)]),
                      'y': ('dp', [(0, 1), (1, 0)])}[kind]
        return lax.ppermute(arr, axis, perm)

    def take_half(arr, which):
        rows = arr.shape[0] // 2
        return lax.dynamic_slice_in_dim(arr, which * rows, rows, 0)

    def join_halves(mine, other, which):
        return jnp.concatenate([jnp.where(which == 0, mine, other), jnp.where(which == 0, other, mine)], axis=0)

    def inner(x_saved, h_saved, mean_one, rstd_one, mean_two, rstd_two, gain_one, gain_two, grad_y, w_qkv, w_proj, w_up, w_down):
        core = lax.axis_index('tp') % 2
        dp_idx = lax.axis_index('dp')
        toks, dim = x_saved.shape
        part_of = lambda arr, i: arr[i * (toks // 2):(i + 1) * (toks // 2)]
        own_rows = lambda arr, i: lax.dynamic_slice_in_dim(arr, i * (toks // 2) + core * (toks // 4), toks // 4, 0)

        n_mine = layer_norm(take_half(h_saved, core), take_half(mean_two, core), take_half(rstd_two, core), gain_two)[1]
        norm_y, dy_y = swap('y', n_mine), swap('y', take_half(grad_y, core))
        norm_c, dy_c = swap('c', norm_y), swap('c', dy_y)

        def tp_sum(part):
            chip = (take_half(part, core).astype(F32) + swap('c', take_half(part, 1 - core)).astype(F32)).astype(BF16)
            return chip.astype(F32) + swap('x', chip).astype(F32)

        def back(total, rows, mean, rstd, gain):
            hat = (rows.astype(F32) - mean[:, None]) * rstd[:, None]
            return norm_back(total, hat, rstd, gain)

        norm_two, pre, d_pre, d_norm = {}, {}, {}, {}
        for tag, i in HALVES:
            norm_two[tag] = layer_norm(part_of(h_saved, i), part_of(mean_two, i), part_of(rstd_two, i), gain_two)[1]
            pre_act = jnp.dot(norm_two[tag], w_up, preferred_element_type=F32).astype(BF16)
            pre[tag] = pre_act
            gelu_slope = gelu_pair(pre_act)[1]
            d_pre[tag] = (lax.dot_general(part_of(grad_y, i), w_down, NT, preferred_element_type=F32) * gelu_slope).astype(BF16)
            part = lax.dot_general(d_pre[tag], w_up, NT, preferred_element_type=F32).astype(BF16)
            d_norm[tag] = tp_sum(part)

        w_t = w_qkv.transpose(1, 2, 3, 0).reshape(-1, dim)
        norm_one = layer_norm(x_saved, mean_one, rstd_one, gain_one)[1]
        qkv = lax.dot_general(norm_one, w_t, NT, preferred_element_type=F32).astype(BF16)

        w_o = w_proj.reshape(-1, dim)
        d_mid, mid_lo, d_attn = {}, {}, {}
        for tag, i in HALVES:
            mine = [own_rows(a, i) for a in (grad_y, h_saved, mean_two, rstd_two)]
            if tag == 'lo':
                mine[2], mine[3], low = lax.optimization_barrier((mine[2], mine[3], low))
            d_mid[tag] = mine[0].astype(F32) + back(d_norm[tag], *mine[1:], gain_two)
            low = d_mid[tag].astype(BF16)
            mid_lo[tag] = join_halves(low, swap('c', low), core)
            d_attn[tag] = lax.dot_general(mid_lo[tag], w_o, NT, preferred_element_type=F32).astype(BF16)
        d_attn = jnp.concatenate([d_attn['lo'], d_attn['hi']], axis=0)
        mid_all = jnp.concatenate([mid_lo['lo'], mid_lo['hi']], axis=0)

        w_pairs = w_t.reshape(3, 2, 128, dim)
        halves, d_pair = [], []
        for pair in range(2):
            o_t, d_qkv = attn_pair(pair, qkv, d_attn)
            d_pair.append(d_qkv)
            g_qkv = lax.dot_general(d_qkv, norm_one, TN, preferred_element_type=F32)
            g_o = jnp.dot(o_t, mid_all, preferred_element_type=F32)
            mine = jnp.concatenate([take_half(g, dp_idx) for g in (g_qkv, g_o)], 0)
            theirs = jnp.concatenate([take_half(g, 1 - dp_idx) for g in (g_qkv, g_o)], 0)
            summed = (mine + swap('y', theirs)).astype(BF16)
            other = swap('y', summed)
            halves.append((join_halves(summed[:192], other[:192], dp_idx), join_halves(summed[192:], other[192:], dp_idx)))

        w_pair = [w_pairs[:, p].reshape(-1, dim) for p in range(2)]
        part_one = jnp.dot(d_pair[0], w_pair[0], preferred_element_type=F32)
        grad_x = {}
        for tag, i in HALVES:
            part = (part_of(part_one, i) + jnp.dot(part_of(d_pair[1], i), w_pair[1], preferred_element_type=F32)).astype(BF16)
            total = tp_sum(part)
            mine = [own_rows(a, i) for a in (x_saved, mean_one, rstd_one)]
            if tag == 'lo':
                mine[1], mine[2], low = lax.optimization_barrier((mine[1], mine[2], low))
            low = (d_mid[tag] + back(total, *mine, gain_one)).astype(BF16)
            grad_x[tag] = join_halves(low, swap('c', low), core)
        grad_x = jnp.concatenate([grad_x['lo'], grad_x['hi']], axis=0)

        part_up, part_down = mlp_columns(other_kernel, [norm_y, norm_c, dy_y, dy_c], [w_up], [w_down], dim, w_up.shape[1], toks, F32)
        grad_up, grad_down = mlp_columns(own_kernel, [norm_two['hi'], norm_two['lo'], grad_y],
                                         [pre['hi'], pre['lo'], d_pre['hi'], d_pre['lo'], part_up], [part_down], dim, w_up.shape[1], toks, BF16)
        g_t = jnp.stack([h[0].reshape(3, 2, 64, dim) for h in halves], axis=1).reshape(3, 4, 64, dim)
        grad_qkv = g_t.transpose(3, 0, 1, 2)
        grad_proj = jnp.concatenate([h[1] for h in halves], axis=0).reshape(4, 64, dim)
        return grad_x, grad_qkv, grad_proj, grad_up, grad_down

    return jax.shard_map(inner, mesh=mesh, in_specs=in_specs, out_specs=out_specs, check_vma=False)
```

```python
import math

import jax
import jax.numpy as jnp
from jax import lax
from jax.experimental import pallas as pl
from jax.experimental.pallas import tpu as pltpu
from jax.sharding import PartitionSpec as P


GELU_C = math.sqrt(2.0 / math.pi)
F32 = jnp.float32
BF16 = jnp.bfloat16
NT = (((1,), (1,)), ((), ()))
TN = (((0,), (0,)), ((), ()))
BLK = 256


def layer_norm(row_vals, row_mean, row_rstd, gain_vec):
    x_hat = (row_vals.astype(F32) - row_mean[:, None]) * row_rstd[:, None]
    return x_hat, (x_hat * gain_vec.astype(F32)).astype(BF16)


def norm_back(d_norm, x_hat, row_rstd, gain_vec):
    scaled = d_norm * gain_vec.astype(F32)
    scaled_mean = jnp.mean(scaled, axis=-1, keepdims=True)
    proj_mean = jnp.mean(scaled * x_hat, axis=-1, keepdims=True)
    return row_rstd[:, None] * (scaled - scaled_mean - x_hat * proj_mean)


def gelu_pair(pre_act):
    pre_wide = pre_act.astype(F32)
    tanh_val = jnp.tanh(GELU_C * (pre_wide + 0.044715 * pre_wide * pre_wide * pre_wide))
    gelu_val = 0.5 * pre_wide * (1.0 + tanh_val)
    gelu_slope = 0.5 * (1.0 + tanh_val) + 0.5 * pre_wide * (1.0 - tanh_val * tanh_val) * GELU_C * (1.0 + 0.134145 * pre_wide * pre_wide)
    return gelu_val, gelu_slope


def fold_rows(op, tile):
    return op(tile.reshape(tile.shape[0] // 8, 8, tile.shape[1]), axis=0)


BQ = 512


def attn_kernel(q_ref, k_ref, v_ref, do_ref, ot_ref, dqkv_ref, s_ref, dp_ref, dk_ref, dv_ref, kt_ref, vt_ref, acc_ref):
    step = pl.program_id(0)
    last = pl.num_programs(0) - 1
    qi = last - step
    per = BQ // BLK
    full = qi * per

    @pl.when(step == 0)
    def _():
        dk_ref[...] = jnp.zeros_like(dk_ref)
        dv_ref[...] = jnp.zeros_like(dv_ref)
        kt_ref[...] = k_ref[...].T
        vt_ref[...] = v_ref[...].T

    lane = lax.broadcasted_iota(jnp.int32, (BQ, 128), 1)
    q_wide = q_ref[...].astype(F32) * 0.125
    do_wide = do_ref[...].astype(F32)
    qs, dos = [], []
    for h in range(2):
        keep = (lane < 64) if h == 0 else (lane >= 64)
        qs.append(jnp.where(keep, q_wide, 0.0).astype(BF16))
        dos.append(jnp.where(keep, do_wide, 0.0).astype(BF16))

    def at(j):
        return pl.ds(pl.multiple_of(j * BLK, BLK), BLK)

    def score(j, top, shift):
        rows = at(j)
        k_blk = k_ref[rows, :]
        out = []
        for h in range(2):
            tile = lax.dot_general(k_blk, qs[h], NT, preferred_element_type=F32)
            if shift is not None:
                key = lax.broadcasted_iota(jnp.int32, (BLK, BQ), 0) + shift
                qry = lax.broadcasted_iota(jnp.int32, (BLK, BQ), 1)
                tile = jnp.where(key <= qry, tile, -1e30)
            s_ref[h, rows, :] = tile
            out.append(jnp.maximum(top[h], fold_rows(jnp.max, tile)))
        return tuple(out)

    low = jnp.full((8, BQ), -1e30, F32)
    top = lax.fori_loop(0, per, lambda i, t: score(full + i, t, i * BLK), (low, low))
    top = lax.fori_loop(0, full, lambda j, t: score(j, t, None), top)
    top = [jnp.max(t, axis=0, keepdims=True) for t in top]

    def expo(j, tot):
        rows = at(j)
        out = []
        for h in range(2):
            tile = jnp.exp(s_ref[h, rows, :] - top[h])
            s_ref[h, rows, :] = tile
            out.append(tot[h] + fold_rows(jnp.sum, tile))
        return tuple(out)

    zero8 = jnp.zeros((8, BQ), F32)
    tot = lax.fori_loop(0, full + per, expo, (zero8, zero8))
    inv = [1.0 / jnp.sum(t, axis=0, keepdims=True) for t in tot]
    acc_ref[...] = jnp.zeros_like(acc_ref)

    def third(j, proj):
        rows = at(j)
        v_blk = v_ref[rows, :]
        proj_new = []
        for h in range(2):
            prob = s_ref[h, rows, :] * inv[h]
            s_ref[h, rows, :] = prob
            prob_lo = prob.astype(BF16)
            d_prob = lax.dot_general(v_blk, dos[h], NT, preferred_element_type=F32)
            dp_ref[h, rows, :] = d_prob
            proj_new.append(proj[h] + fold_rows(jnp.sum, prob * d_prob))
            dv_ref[rows, :] += jnp.dot(prob_lo, dos[h], preferred_element_type=F32)
            acc_ref[h] += jnp.dot(vt_ref[h * 64:(h + 1) * 64, rows], prob_lo, preferred_element_type=F32)
        return tuple(proj_new)

    proj = lax.fori_loop(0, full + per, third, (zero8, zero8))
    for h in range(2):
        ot_ref[h * 64:(h + 1) * 64, :] = acc_ref[h].astype(BF16)
    proj = [jnp.sum(t, axis=0, keepdims=True) for t in proj]
    acc_ref[...] = jnp.zeros_like(acc_ref)

    def fourth(j, none):
        rows = at(j)
        for h in range(2):
            d_s = (s_ref[h, rows, :] * (dp_ref[h, rows, :] - proj[h])).astype(BF16)
            dk_ref[rows, :] += jnp.dot(d_s, qs[h], preferred_element_type=F32)
            acc_ref[h] += jnp.dot(kt_ref[h * 64:(h + 1) * 64, rows], d_s, preferred_element_type=F32)
        return none

    lax.fori_loop(0, full + per, fourth, 0)
    dq = acc_ref[...].reshape(128, BQ) * 0.125
    dqkv_ref[pl.ds(pl.multiple_of(qi * BQ, BQ), BQ), 0:128] = dq.T.astype(BF16)

    @pl.when(step == last)
    def _():
        dqkv_ref[:, 128:256] = dk_ref[...].astype(BF16)
        dqkv_ref[:, 256:384] = dv_ref[...].astype(BF16)


def attn_pair(pair, qkv, d_attn):
    toks = qkv.shape[0]
    steps = toks // BQ
    return pl.pallas_call(
        attn_kernel,
        grid=(steps,),
        in_specs=[pl.BlockSpec((BQ, 128), lambda s: (steps - 1 - s, pair)),
                  pl.BlockSpec((toks, 128), lambda s: (0, 2 + pair)),
                  pl.BlockSpec((toks, 128), lambda s: (0, 4 + pair)),
                  pl.BlockSpec((BQ, 128), lambda s: (steps - 1 - s, pair))],
        out_specs=[pl.BlockSpec((128, BQ), lambda s: (0, steps - 1 - s)),
                   pl.BlockSpec((toks, 384), lambda s: (0, 0))],
        out_shape=[jax.ShapeDtypeStruct((128, toks), BF16), jax.ShapeDtypeStruct((toks, 384), BF16)],
        scratch_shapes=[pltpu.VMEM((2, toks, BQ), F32), pltpu.VMEM((2, toks, BQ), F32),
                        pltpu.VMEM((toks, 128), F32), pltpu.VMEM((toks, 128), F32),
                        pltpu.VMEM((128, toks), BF16), pltpu.VMEM((128, toks), BF16), pltpu.VMEM((2, 64, BQ), F32)],
        compiler_params=pltpu.CompilerParams(dimension_semantics=("arbitrary",), vmem_limit_bytes=30 << 20),
        cost_estimate=pl.CostEstimate(flops=16 * 10**9, bytes_accessed=4 << 20, transcendentals=0),
    )(qkv, qkv, qkv, d_attn)


def own_kernel(nh_ref, nl_ref, dy_ref, ah_ref, al_ref, ph_ref, pl_ref, gu_ref, gd_ref, nt_ref, gt_ref, dp_ref):
    rows = nh_ref.shape[0]

    @pl.when(pl.program_id(0) == 0)
    def _():
        for i, ref in enumerate((nl_ref, nh_ref)):
            nt_ref[:, i * rows:(i + 1) * rows] = ref[...].T

    for i, (a_ref, p_ref) in enumerate(((al_ref, pl_ref), (ah_ref, ph_ref))):
        gt_ref[:, i * rows:(i + 1) * rows] = gelu_pair(a_ref[...])[0].astype(BF16).T
        dp_ref[i * rows:(i + 1) * rows, :] = p_ref[...]
    gu_ref[...] = jnp.dot(nt_ref[...], dp_ref[...], preferred_element_type=F32)
    gd_ref[...] = jnp.dot(gt_ref[...], dy_ref[...], preferred_element_type=F32)


def other_kernel(n0_hbm, n1_hbm, n2_hbm, n3_hbm, da_hbm, db_hbm, wu_ref, wd_ref, pu_ref, pd_ref, gu_ref, gd_ref,
                 nt_ref, gt_ref, dp_ref, n_ref, d_ref, sem):
    sub = n0_hbm.shape[0]

    @pl.when(pl.program_id(0) == 0)
    def _():
        loads, row = [], 0
        for i, (ref, dst) in enumerate([(r, n_ref) for r in (n0_hbm, n1_hbm, n2_hbm, n3_hbm)] + [(r, d_ref) for r in (da_hbm, db_hbm)]):
            row = 0 if i == 4 else row
            loads.append(pltpu.make_async_copy(ref, dst.at[row:row + ref.shape[0]], sem.at[i]))
            row += ref.shape[0]
        for load in loads:
            load.start()
        for load in loads:
            load.wait()
        nt_ref[...] = n_ref[...].T

    @pl.loop(0, 2)
    def _(i):
        for r in range(2):
            at = pl.ds(pl.multiple_of(i * 2 * sub + r * sub, sub), sub)
            act, slope = gelu_pair(jnp.dot(n_ref[at, :], wu_ref[...], preferred_element_type=F32).astype(BF16))
            d_act = lax.dot_general(d_ref[at, :], wd_ref[...], NT, preferred_element_type=F32)
            dp_ref[at, :] = (d_act * slope).astype(BF16)
            gt_ref[:, at] = act.astype(BF16).T

    gu_ref[...] = (jnp.dot(nt_ref[...], dp_ref[...], preferred_element_type=F32) + pu_ref[...]).astype(BF16)
    gd_ref[...] = (jnp.dot(gt_ref[...], d_ref[...], preferred_element_type=F32) + pd_ref[...]).astype(BF16)


def mlp_columns(kernel, whole, by_col, by_row, dim, cols, rows, out_type, copies=0):
    once = lambda a: pl.BlockSpec(a.shape, lambda s: (0, 0), pipeline_mode=pl.Buffered(1))
    if copies:
        once = lambda a: pl.BlockSpec(memory_space=pltpu.MemorySpace.HBM)
    col = lambda n: pl.BlockSpec((n, BLK), lambda s: (0, s))
    row = lambda n: pl.BlockSpec((BLK, n), lambda s: (s, 0))
    args = whole + by_col[:1] + by_row[:1] + by_col[1:] + by_row[1:] if by_row else whole + by_col
    specs = [col(a.shape[0]) for a in by_col[:1]] + [row(a.shape[1]) for a in by_row[:1]] + [col(a.shape[0]) for a in by_col[1:]] + [row(a.shape[1]) for a in by_row[1:]]
    return pl.pallas_call(
        kernel,
        grid=(cols // BLK,),
        in_specs=[once(a) for a in whole] + specs,
        out_specs=[col(dim), row(dim)],
        out_shape=[jax.ShapeDtypeStruct((dim, cols), out_type), jax.ShapeDtypeStruct((cols, dim), out_type)],
        scratch_shapes=[pltpu.VMEM((dim, rows), BF16), pltpu.VMEM((BLK, rows), BF16), pltpu.VMEM((rows, BLK), BF16)]
        + ([pltpu.VMEM((rows, dim), BF16)] * 2 + [pltpu.SemaphoreType.DMA((copies,))] if copies else []),
        compiler_params=pltpu.CompilerParams(dimension_semantics=("arbitrary",), vmem_limit_bytes=36 << 20),
        cost_estimate=pl.CostEstimate(flops=16 * 10**9, bytes_accessed=14 << 20, transcendentals=0),
    )(*args)


HALVES = (('hi', 1), ('lo', 0))


def solution(mesh):
    row_spec = P(('pod', 'dp'), None)
    stat_spec = P(('pod', 'dp'))
    in_specs = (row_spec, row_spec, stat_spec, stat_spec, stat_spec, stat_spec, P(None), P(None), row_spec,
                P(None, None, 'tp', None), P('tp', None, None), P(None, 'tp'), P('tp', None))
    out_specs = (row_spec, P('pod', None, 'tp', None), P(('pod', 'tp'), None, None), P('pod', 'tp'), P(('pod', 'tp'), None))

    def swap(kind, arr):
        axis, perm = {'c': ('tp', [(0, 1), (1, 0), (2, 3), (3, 2)]), 'x': ('tp', [(0, 2), (2, 0), (1, 3), (3, 1)]),
                      'y': ('dp', [(0, 1), (1, 0)])}[kind]
        return lax.ppermute(arr, axis, perm)

    def take_half(arr, which):
        rows = arr.shape[0] // 2
        return lax.dynamic_slice_in_dim(arr, which * rows, rows, 0)

    def join_halves(mine, other, which):
        return jnp.concatenate([jnp.where(which == 0, mine, other), jnp.where(which == 0, other, mine)], axis=0)

    def inner(x_saved, h_saved, mean_one, rstd_one, mean_two, rstd_two, gain_one, gain_two, grad_y, w_qkv, w_proj, w_up, w_down):
        core = lax.axis_index('tp') % 2
        dp_idx = lax.axis_index('dp')
        toks, dim = x_saved.shape
        part_of = lambda arr, i: arr[i * (toks // 2):(i + 1) * (toks // 2)]
        own_rows = lambda arr, i: lax.dynamic_slice_in_dim(arr, i * (toks // 2) + core * (toks // 4), toks // 4, 0)

        t_idx, quarter = lax.axis_index('tp'), toks // 4
        cut = lambda arr, i: lax.dynamic_slice_in_dim(arr, i * quarter, quarter, 0)
        n_mine = layer_norm(cut(h_saved, t_idx), cut(mean_two, t_idx), cut(rstd_two, t_idx), gain_two)[1]
        n_y = swap('y', n_mine)
        dy_y = swap('y', jnp.concatenate([cut(grad_y, t_idx), cut(grad_y, (t_idx + 2) % 4)], axis=0))
        n_x = swap('x', n_y)
        n_cy, n_cx, dy_c = [swap('c', a) for a in (n_y, n_x, dy_y)]

        def tp_sum(part):
            chip = (take_half(part, core).astype(F32) + swap('c', take_half(part, 1 - core)).astype(F32)).astype(BF16)
            return chip.astype(F32) + swap('x', chip).astype(F32)

        def back(total, rows, mean, rstd, gain):
            hat = (rows.astype(F32) - mean[:, None]) * rstd[:, None]
            return norm_back(total, hat, rstd, gain)

        norm_two, pre, d_pre, d_norm = {}, {}, {}, {}
        for tag, i in HALVES:
            norm_two[tag] = layer_norm(part_of(h_saved, i), part_of(mean_two, i), part_of(rstd_two, i), gain_two)[1]
            pre_act = jnp.dot(norm_two[tag], w_up, preferred_element_type=F32).astype(BF16)
            pre[tag] = pre_act
            gelu_slope = gelu_pair(pre_act)[1]
            d_pre[tag] = (lax.dot_general(part_of(grad_y, i), w_down, NT, preferred_element_type=F32) * gelu_slope).astype(BF16)
            part = lax.dot_general(d_pre[tag], w_up, NT, preferred_element_type=F32).astype(BF16)
            d_norm[tag] = tp_sum(part)

        part_up, part_down = mlp_columns(own_kernel, [norm_two['hi'], norm_two['lo'], grad_y],
                                         [pre['hi'], pre['lo'], d_pre['hi'], d_pre['lo']], [], dim, w_up.shape[1], toks, F32)
        w_t = w_qkv.transpose(1, 2, 3, 0).reshape(-1, dim)
        norm_one = layer_norm(x_saved, mean_one, rstd_one, gain_one)[1]
        qkv = lax.dot_general(norm_one, w_t, NT, preferred_element_type=F32).astype(BF16)

        w_o = w_proj.reshape(-1, dim)
        d_mid, mid_lo, d_attn = {}, {}, {}
        for tag, i in HALVES:
            mine = [own_rows(a, i) for a in (grad_y, h_saved, mean_two, rstd_two)]
            if tag == 'hi':
                mine[2], mine[3], n_mine = lax.optimization_barrier((mine[2], mine[3], n_mine))
            else:
                mine[2], mine[3], low = lax.optimization_barrier((mine[2], mine[3], low))
            d_mid[tag] = mine[0].astype(F32) + back(d_norm[tag], *mine[1:], gain_two)
            low = d_mid[tag].astype(BF16)
            mid_lo[tag] = join_halves(low, swap('c', low), core)
            d_attn[tag] = lax.dot_general(mid_lo[tag], w_o, NT, preferred_element_type=F32).astype(BF16)
        d_attn = jnp.concatenate([d_attn['lo'], d_attn['hi']], axis=0)
        mid_all = jnp.concatenate([mid_lo['lo'], mid_lo['hi']], axis=0)

        w_pairs = w_t.reshape(3, 2, 128, dim)
        halves, d_pair = [], []
        for pair in range(2):
            o_t, d_qkv = attn_pair(pair, qkv, d_attn)
            d_pair.append(d_qkv)
            g_qkv = lax.dot_general(d_qkv, norm_one, TN, preferred_element_type=F32)
            g_o = jnp.dot(o_t, mid_all, preferred_element_type=F32)
            mine = jnp.concatenate([take_half(g, dp_idx) for g in (g_qkv, g_o)], 0)
            theirs = jnp.concatenate([take_half(g, 1 - dp_idx) for g in (g_qkv, g_o)], 0)
            recv = swap('y', theirs)
            summed = (mine + recv).astype(BF16)
            other = swap('y', summed)
            halves.append((join_halves(summed[:192], other[:192], dp_idx), join_halves(summed[192:], other[192:], dp_idx)))

        w_pair = [w_pairs[:, p].reshape(-1, dim) for p in range(2)]
        part_one = jnp.dot(d_pair[0], w_pair[0], preferred_element_type=F32)
        grad_x = {}
        for tag, i in HALVES:
            part = (part_of(part_one, i) + jnp.dot(part_of(d_pair[1], i), w_pair[1], preferred_element_type=F32)).astype(BF16)
            total = tp_sum(part)
            mine = [own_rows(a, i) for a in (x_saved, mean_one, rstd_one)]
            if tag == 'lo':
                mine[1], mine[2], low = lax.optimization_barrier((mine[1], mine[2], low))
            low = (d_mid[tag] + back(total, *mine, gain_one)).astype(BF16)
            grad_x[tag] = join_halves(low, swap('c', low), core)
        grad_x = jnp.concatenate([grad_x['lo'], grad_x['hi']], axis=0)

        grad_up, grad_down = mlp_columns(other_kernel, [n_y, n_x, n_cy, n_cx, dy_y, dy_c], [w_up, part_up], [w_down, part_down],
                                         dim, w_up.shape[1], toks, BF16, copies=6)
        g_t = jnp.stack([h[0].reshape(3, 2, 64, dim) for h in halves], axis=1).reshape(3, 4, 64, dim)
        grad_qkv = g_t.transpose(3, 0, 1, 2)
        grad_proj = jnp.concatenate([h[1] for h in halves], axis=0).reshape(4, 64, dim)
        return grad_x, grad_qkv, grad_proj, grad_up, grad_down

    return jax.shard_map(inner, mesh=mesh, in_specs=in_specs, out_specs=out_specs, check_vma=False)
```

```python
import math

import jax
import jax.numpy as jnp
from jax import lax
from jax.experimental import pallas as pl
from jax.experimental.pallas import tpu as pltpu
from jax.sharding import PartitionSpec as P


GELU_C = math.sqrt(2.0 / math.pi)
F32 = jnp.float32
BF16 = jnp.bfloat16
NT = (((1,), (1,)), ((), ()))
TN = (((0,), (0,)), ((), ()))
BLK = 256


def layer_norm(row_vals, row_mean, row_rstd, gain_vec):
    x_hat = (row_vals.astype(F32) - row_mean[:, None]) * row_rstd[:, None]
    return x_hat, (x_hat * gain_vec.astype(F32)).astype(BF16)


def norm_back(d_norm, x_hat, row_rstd, gain_vec):
    scaled = d_norm * gain_vec.astype(F32)
    scaled_mean = jnp.mean(scaled, axis=-1, keepdims=True)
    proj_mean = jnp.mean(scaled * x_hat, axis=-1, keepdims=True)
    return row_rstd[:, None] * (scaled - scaled_mean - x_hat * proj_mean)


def gelu_pair(pre_act):
    pre_wide = pre_act.astype(F32)
    tanh_val = jnp.tanh(GELU_C * (pre_wide + 0.044715 * pre_wide * pre_wide * pre_wide))
    gelu_val = 0.5 * pre_wide * (1.0 + tanh_val)
    gelu_slope = 0.5 * (1.0 + tanh_val) + 0.5 * pre_wide * (1.0 - tanh_val * tanh_val) * GELU_C * (1.0 + 0.134145 * pre_wide * pre_wide)
    return gelu_val, gelu_slope


def fold_rows(op, tile):
    return op(tile.reshape(tile.shape[0] // 8, 8, tile.shape[1]), axis=0)


BQ = 512


def attn_kernel(q_ref, k_ref, v_ref, do_ref, ot_ref, dqkv_ref, s_ref, dp_ref, dk_ref, dv_ref, kt_ref, vt_ref, acc_ref):
    step = pl.program_id(0)
    last = pl.num_programs(0) - 1
    qi = last - step
    per = BQ // BLK
    full = qi * per

    @pl.when(step == 0)
    def _():
        dk_ref[...] = jnp.zeros_like(dk_ref)
        dv_ref[...] = jnp.zeros_like(dv_ref)
        kt_ref[...] = k_ref[...].T
        vt_ref[...] = v_ref[...].T

    lane = lax.broadcasted_iota(jnp.int32, (BQ, 128), 1)
    q_wide = q_ref[...].astype(F32) * 0.125
    do_wide = do_ref[...].astype(F32)
    qs, dos = [], []
    for h in range(2):
        keep = (lane < 64) if h == 0 else (lane >= 64)
        qs.append(jnp.where(keep, q_wide, 0.0).astype(BF16))
        dos.append(jnp.where(keep, do_wide, 0.0).astype(BF16))

    def at(j):
        return pl.ds(pl.multiple_of(j * BLK, BLK), BLK)

    def score(j, top, shift):
        rows = at(j)
        k_blk = k_ref[rows, :]
        out = []
        for h in range(2):
            tile = lax.dot_general(k_blk, qs[h], NT, preferred_element_type=F32)
            if shift is not None:
                key = lax.broadcasted_iota(jnp.int32, (BLK, BQ), 0) + shift
                qry = lax.broadcasted_iota(jnp.int32, (BLK, BQ), 1)
                tile = jnp.where(key <= qry, tile, -1e30)
            s_ref[h, rows, :] = tile
            out.append(jnp.maximum(top[h], fold_rows(jnp.max, tile)))
        return tuple(out)

    low = jnp.full((8, BQ), -1e30, F32)
    top = lax.fori_loop(0, per, lambda i, t: score(full + i, t, i * BLK), (low, low))
    top = lax.fori_loop(0, full, lambda j, t: score(j, t, None), top)
    top = [jnp.max(t, axis=0, keepdims=True) for t in top]

    def expo(j, tot):
        rows = at(j)
        out = []
        for h in range(2):
            tile = jnp.exp(s_ref[h, rows, :] - top[h])
            s_ref[h, rows, :] = tile
            out.append(tot[h] + fold_rows(jnp.sum, tile))
        return tuple(out)

    zero8 = jnp.zeros((8, BQ), F32)
    tot = lax.fori_loop(0, full + per, expo, (zero8, zero8))
    inv = [1.0 / jnp.sum(t, axis=0, keepdims=True) for t in tot]
    acc_ref[...] = jnp.zeros_like(acc_ref)

    def third(j, proj):
        rows = at(j)
        v_blk = v_ref[rows, :]
        proj_new = []
        for h in range(2):
            prob = s_ref[h, rows, :] * inv[h]
            s_ref[h, rows, :] = prob
            prob_lo = prob.astype(BF16)
            d_prob = lax.dot_general(v_blk, dos[h], NT, preferred_element_type=F32)
            dp_ref[h, rows, :] = d_prob
            proj_new.append(proj[h] + fold_rows(jnp.sum, prob * d_prob))
            dv_ref[rows, :] += jnp.dot(prob_lo, dos[h], preferred_element_type=F32)
            acc_ref[h] += jnp.dot(vt_ref[h * 64:(h + 1) * 64, rows], prob_lo, preferred_element_type=F32)
        return tuple(proj_new)

    proj = lax.fori_loop(0, full + per, third, (zero8, zero8))
    for h in range(2):
        ot_ref[h * 64:(h + 1) * 64, :] = acc_ref[h].astype(BF16)
    proj = [jnp.sum(t, axis=0, keepdims=True) for t in proj]
    acc_ref[...] = jnp.zeros_like(acc_ref)

    def fourth(j, none):
        rows = at(j)
        for h in range(2):
            d_s = (s_ref[h, rows, :] * (dp_ref[h, rows, :] - proj[h])).astype(BF16)
            dk_ref[rows, :] += jnp.dot(d_s, qs[h], preferred_element_type=F32)
            acc_ref[h] += jnp.dot(kt_ref[h * 64:(h + 1) * 64, rows], d_s, preferred_element_type=F32)
        return none

    lax.fori_loop(0, full + per, fourth, 0)
    dq = acc_ref[...].reshape(128, BQ) * 0.125
    dqkv_ref[pl.ds(pl.multiple_of(qi * BQ, BQ), BQ), 0:128] = dq.T.astype(BF16)

    @pl.when(step == last)
    def _():
        dqkv_ref[:, 128:256] = dk_ref[...].astype(BF16)
        dqkv_ref[:, 256:384] = dv_ref[...].astype(BF16)


def attn_pair(pair, qkv, d_attn):
    toks = qkv.shape[0]
    steps = toks // BQ
    return pl.pallas_call(
        attn_kernel,
        grid=(steps,),
        in_specs=[pl.BlockSpec((BQ, 128), lambda s: (steps - 1 - s, pair)),
                  pl.BlockSpec((toks, 128), lambda s: (0, 2 + pair)),
                  pl.BlockSpec((toks, 128), lambda s: (0, 4 + pair)),
                  pl.BlockSpec((BQ, 128), lambda s: (steps - 1 - s, pair))],
        out_specs=[pl.BlockSpec((128, BQ), lambda s: (0, steps - 1 - s)),
                   pl.BlockSpec((toks, 384), lambda s: (0, 0))],
        out_shape=[jax.ShapeDtypeStruct((128, toks), BF16), jax.ShapeDtypeStruct((toks, 384), BF16)],
        scratch_shapes=[pltpu.VMEM((2, toks, BQ), F32), pltpu.VMEM((2, toks, BQ), F32),
                        pltpu.VMEM((toks, 128), F32), pltpu.VMEM((toks, 128), F32),
                        pltpu.VMEM((128, toks), BF16), pltpu.VMEM((128, toks), BF16), pltpu.VMEM((2, 64, BQ), F32)],
        compiler_params=pltpu.CompilerParams(dimension_semantics=("arbitrary",), vmem_limit_bytes=30 << 20),
        cost_estimate=pl.CostEstimate(flops=16 * 10**9, bytes_accessed=4 << 20, transcendentals=0),
    )(qkv, qkv, qkv, d_attn)


def own_kernel(nh_ref, nl_ref, dy_ref, ah_ref, al_ref, ph_ref, pl_ref, gu_ref, gd_ref, nt_ref, gt_ref, dp_ref):
    rows = nh_ref.shape[0]

    @pl.when(pl.program_id(0) == 0)
    def _():
        for i, ref in enumerate((nl_ref, nh_ref)):
            nt_ref[:, i * rows:(i + 1) * rows] = ref[...].T

    for i, (a_ref, p_ref) in enumerate(((al_ref, pl_ref), (ah_ref, ph_ref))):
        gt_ref[:, i * rows:(i + 1) * rows] = gelu_pair(a_ref[...])[0].astype(BF16).T
        dp_ref[i * rows:(i + 1) * rows, :] = p_ref[...]
    gu_ref[...] = jnp.dot(nt_ref[...], dp_ref[...], preferred_element_type=F32)
    gd_ref[...] = jnp.dot(gt_ref[...], dy_ref[...], preferred_element_type=F32)


def other_kernel(n0_ref, n1_ref, n2_ref, n3_ref, da_ref, db_ref, wu_ref, wd_ref, pu_ref, pd_ref, gu_ref, gd_ref, nt_ref, gt_ref, dp_ref):
    sub, rows = n0_ref.shape[0], da_ref.shape[0]
    n_refs = (n0_ref, n1_ref, n2_ref, n3_ref)

    @pl.when(pl.program_id(0) == 0)
    def _():
        for i, ref in enumerate(n_refs):
            nt_ref[:, i * sub:(i + 1) * sub] = ref[...].T

    for i, n_ref in enumerate(n_refs):
        d_ref = (da_ref, db_ref)[i // 2]
        at = slice(i * sub, (i + 1) * sub)
        act, slope = gelu_pair(jnp.dot(n_ref[...], wu_ref[...], preferred_element_type=F32).astype(BF16))
        d_act = lax.dot_general(d_ref[(i % 2) * sub:(i % 2 + 1) * sub, :], wd_ref[...], NT, preferred_element_type=F32)
        dp_ref[at, :] = (d_act * slope).astype(BF16)
        gt_ref[:, at] = act.astype(BF16).T
    gu_ref[...] = (jnp.dot(nt_ref[...], dp_ref[...], preferred_element_type=F32) + pu_ref[...]).astype(BF16)
    total = jnp.dot(gt_ref[:, :rows], da_ref[...], preferred_element_type=F32)
    total += jnp.dot(gt_ref[:, rows:], db_ref[...], preferred_element_type=F32)
    gd_ref[...] = (total + pd_ref[...]).astype(BF16)


def mlp_columns(kernel, whole, by_col, by_row, dim, cols, rows, out_type):
    once = lambda a: pl.BlockSpec(a.shape, lambda s: (0, 0), pipeline_mode=pl.Buffered(1))
    col = lambda n: pl.BlockSpec((n, BLK), lambda s: (0, s))
    row = lambda n: pl.BlockSpec((BLK, n), lambda s: (s, 0))
    args = whole + by_col[:1] + by_row[:1] + by_col[1:] + by_row[1:] if by_row else whole + by_col
    specs = [col(a.shape[0]) for a in by_col[:1]] + [row(a.shape[1]) for a in by_row[:1]] + [col(a.shape[0]) for a in by_col[1:]] + [row(a.shape[1]) for a in by_row[1:]]
    return pl.pallas_call(
        kernel,
        grid=(cols // BLK,),
        in_specs=[once(a) for a in whole] + specs,
        out_specs=[col(dim), row(dim)],
        out_shape=[jax.ShapeDtypeStruct((dim, cols), out_type), jax.ShapeDtypeStruct((cols, dim), out_type)],
        scratch_shapes=[pltpu.VMEM((dim, rows), BF16), pltpu.VMEM((BLK, rows), BF16), pltpu.VMEM((rows, BLK), BF16)],
        compiler_params=pltpu.CompilerParams(dimension_semantics=("arbitrary",), vmem_limit_bytes=36 << 20),
        cost_estimate=pl.CostEstimate(flops=16 * 10**9, bytes_accessed=14 << 20, transcendentals=0),
    )(*args)


HALVES = (('hi', 1), ('lo', 0))


def solution(mesh):
    row_spec = P(('pod', 'dp'), None)
    stat_spec = P(('pod', 'dp'))
    in_specs = (row_spec, row_spec, stat_spec, stat_spec, stat_spec, stat_spec, P(None), P(None), row_spec,
                P(None, None, 'tp', None), P('tp', None, None), P(None, 'tp'), P('tp', None))
    out_specs = (row_spec, P('pod', None, 'tp', None), P(('pod', 'tp'), None, None), P('pod', 'tp'), P(('pod', 'tp'), None))

    def swap(kind, arr):
        axis, perm = {'c': ('tp', [(0, 1), (1, 0), (2, 3), (3, 2)]), 'x': ('tp', [(0, 2), (2, 0), (1, 3), (3, 1)]),
                      'y': ('dp', [(0, 1), (1, 0)])}[kind]
        return lax.ppermute(arr, axis, perm)

    def take_half(arr, which):
        rows = arr.shape[0] // 2
        return lax.dynamic_slice_in_dim(arr, which * rows, rows, 0)

    def join_halves(mine, other, which):
        return jnp.concatenate([jnp.where(which == 0, mine, other), jnp.where(which == 0, other, mine)], axis=0)

    def inner(x_saved, h_saved, mean_one, rstd_one, mean_two, rstd_two, gain_one, gain_two, grad_y, w_qkv, w_proj, w_up, w_down):
        core = lax.axis_index('tp') % 2
        dp_idx = lax.axis_index('dp')
        toks, dim = x_saved.shape
        part_of = lambda arr, i: arr[i * (toks // 2):(i + 1) * (toks // 2)]
        own_rows = lambda arr, i: lax.dynamic_slice_in_dim(arr, i * (toks // 2) + core * (toks // 4), toks // 4, 0)

        t_idx, quarter = lax.axis_index('tp'), toks // 4
        cut = lambda arr, i: lax.dynamic_slice_in_dim(arr, i * quarter, quarter, 0)
        n_mine = layer_norm(cut(h_saved, t_idx), cut(mean_two, t_idx), cut(rstd_two, t_idx), gain_two)[1]
        n_y = swap('y', n_mine)
        dy_y = swap('y', jnp.concatenate([cut(grad_y, t_idx), cut(grad_y, (t_idx + 2) % 4)], axis=0))
        n_x = swap('x', n_y)
        n_cy, n_cx, dy_c = swap('c', n_y), swap('c', n_x), swap('c', dy_y)

        def tp_sum(part):
            chip = (take_half(part, core).astype(F32) + swap('c', take_half(part, 1 - core)).astype(F32)).astype(BF16)
            return chip.astype(F32) + swap('x', chip).astype(F32)

        def back(total, rows, mean, rstd, gain):
            hat = (rows.astype(F32) - mean[:, None]) * rstd[:, None]
            return norm_back(total, hat, rstd, gain)

        norm_two, pre, d_pre, d_norm = {}, {}, {}, {}
        for tag, i in HALVES:
            norm_two[tag] = layer_norm(part_of(h_saved, i), part_of(mean_two, i), part_of(rstd_two, i), gain_two)[1]
            pre_act = jnp.dot(norm_two[tag], w_up, preferred_element_type=F32).astype(BF16)
            pre[tag] = pre_act
            gelu_slope = gelu_pair(pre_act)[1]
            d_pre[tag] = (lax.dot_general(part_of(grad_y, i), w_down, NT, preferred_element_type=F32) * gelu_slope).astype(BF16)
            part = lax.dot_general(d_pre[tag], w_up, NT, preferred_element_type=F32).astype(BF16)
            d_norm[tag] = tp_sum(part)

        part_up, part_down = mlp_columns(own_kernel, [norm_two['hi'], norm_two['lo'], grad_y],
                                         [pre['hi'], pre['lo'], d_pre['hi'], d_pre['lo']], [], dim, w_up.shape[1], toks, F32)
        w_t = w_qkv.transpose(1, 2, 3, 0).reshape(-1, dim)
        norm_one = layer_norm(x_saved, mean_one, rstd_one, gain_one)[1]
        qkv = lax.dot_general(norm_one, w_t, NT, preferred_element_type=F32).astype(BF16)

        w_o = w_proj.reshape(-1, dim)
        d_mid, mid_lo, d_attn = {}, {}, {}
        for tag, i in HALVES:
            mine = [own_rows(a, i) for a in (grad_y, h_saved, mean_two, rstd_two)]
            if tag == 'hi':
                mine[2], mine[3], n_mine = lax.optimization_barrier((mine[2], mine[3], n_mine))
            else:
                mine[2], mine[3], low = lax.optimization_barrier((mine[2], mine[3], low))
            d_mid[tag] = mine[0].astype(F32) + back(d_norm[tag], *mine[1:], gain_two)
            low = d_mid[tag].astype(BF16)
            mid_lo[tag] = join_halves(low, swap('c', low), core)
            d_attn[tag] = lax.dot_general(mid_lo[tag], w_o, NT, preferred_element_type=F32).astype(BF16)
        d_attn = jnp.concatenate([d_attn['lo'], d_attn['hi']], axis=0)
        mid_all = jnp.concatenate([mid_lo['lo'], mid_lo['hi']], axis=0)

        w_pairs = w_t.reshape(3, 2, 128, dim)
        halves, d_pair = [], []
        for pair in range(2):
            o_t, d_qkv = attn_pair(pair, qkv, d_attn)
            d_pair.append(d_qkv)
            g_qkv = lax.dot_general(d_qkv, norm_one, TN, preferred_element_type=F32)
            g_o = jnp.dot(o_t, mid_all, preferred_element_type=F32)
            mine = jnp.concatenate([take_half(g, dp_idx) for g in (g_qkv, g_o)], 0)
            theirs = jnp.concatenate([take_half(g, 1 - dp_idx) for g in (g_qkv, g_o)], 0)
            recv = swap('y', theirs)
            summed = (mine + recv).astype(BF16)
            other = swap('y', summed)
            halves.append((join_halves(summed[:192], other[:192], dp_idx), join_halves(summed[192:], other[192:], dp_idx)))

        w_pair = [w_pairs[:, p].reshape(-1, dim) for p in range(2)]
        part_one = jnp.dot(d_pair[0], w_pair[0], preferred_element_type=F32)
        grad_x = {}
        for tag, i in HALVES:
            part = (part_of(part_one, i) + jnp.dot(part_of(d_pair[1], i), w_pair[1], preferred_element_type=F32)).astype(BF16)
            total = tp_sum(part)
            mine = [own_rows(a, i) for a in (x_saved, mean_one, rstd_one)]
            if tag == 'lo':
                mine[1], mine[2], low = lax.optimization_barrier((mine[1], mine[2], low))
            low = (d_mid[tag] + back(total, *mine, gain_one)).astype(BF16)
            grad_x[tag] = join_halves(low, swap('c', low), core)
        grad_x = jnp.concatenate([grad_x['lo'], grad_x['hi']], axis=0)

        grad_up, grad_down = mlp_columns(other_kernel, [n_y, n_x, n_cy, n_cx, dy_y, dy_c], [w_up, part_up], [w_down, part_down],
                                         dim, w_up.shape[1], toks, BF16)
        g_t = jnp.stack([h[0].reshape(3, 2, 64, dim) for h in halves], axis=1).reshape(3, 4, 64, dim)
        grad_qkv = g_t.transpose(3, 0, 1, 2)
        grad_proj = jnp.concatenate([h[1] for h in halves], axis=0).reshape(4, 64, dim)
        return grad_x, grad_qkv, grad_proj, grad_up, grad_down

    return jax.shard_map(inner, mesh=mesh, in_specs=in_specs, out_specs=out_specs, check_vma=False)
```

```python
import math

import jax
import jax.numpy as jnp
from jax import lax
from jax.experimental import pallas as pl
from jax.experimental.pallas import tpu as pltpu
from jax.sharding import PartitionSpec as P


GELU_C = math.sqrt(2.0 / math.pi)
F32 = jnp.float32
BF16 = jnp.bfloat16
NT = (((1,), (1,)), ((), ()))
TN = (((0,), (0,)), ((), ()))
BLK = 256


def layer_norm(row_vals, row_mean, row_rstd, gain_vec):
    x_hat = (row_vals.astype(F32) - row_mean[:, None]) * row_rstd[:, None]
    return x_hat, (x_hat * gain_vec.astype(F32)).astype(BF16)


def norm_back(d_norm, x_hat, row_rstd, gain_vec):
    scaled = d_norm * gain_vec.astype(F32)
    scaled_mean = jnp.mean(scaled, axis=-1, keepdims=True)
    proj_mean = jnp.mean(scaled * x_hat, axis=-1, keepdims=True)
    return row_rstd[:, None] * (scaled - scaled_mean - x_hat * proj_mean)


def gelu_pair(pre_act):
    pre_wide = pre_act.astype(F32)
    tanh_val = jnp.tanh(GELU_C * (pre_wide + 0.044715 * pre_wide * pre_wide * pre_wide))
    gelu_val = 0.5 * pre_wide * (1.0 + tanh_val)
    gelu_slope = 0.5 * (1.0 + tanh_val) + 0.5 * pre_wide * (1.0 - tanh_val * tanh_val) * GELU_C * (1.0 + 0.134145 * pre_wide * pre_wide)
    return gelu_val, gelu_slope


def fold_rows(op, tile):
    return op(tile.reshape(tile.shape[0] // 8, 8, tile.shape[1]), axis=0)


BQ = 512


def attn_kernel(q_ref, k_ref, v_ref, do_ref, ot_ref, dqkv_ref, s_ref, dp_ref, dk_ref, dv_ref, kt_ref, vt_ref, acc_ref):
    step = pl.program_id(0)
    last = pl.num_programs(0) - 1
    qi = last - step
    per = BQ // BLK
    full = qi * per

    @pl.when(step == 0)
    def _():
        dk_ref[...] = jnp.zeros_like(dk_ref)
        dv_ref[...] = jnp.zeros_like(dv_ref)
        kt_ref[...] = k_ref[...].T
        vt_ref[...] = v_ref[...].T

    lane = lax.broadcasted_iota(jnp.int32, (BQ, 128), 1)
    q_wide = q_ref[...].astype(F32) * 0.125
    do_wide = do_ref[...].astype(F32)
    qs, dos = [], []
    for h in range(2):
        keep = (lane < 64) if h == 0 else (lane >= 64)
        qs.append(jnp.where(keep, q_wide, 0.0).astype(BF16))
        dos.append(jnp.where(keep, do_wide, 0.0).astype(BF16))

    def at(j):
        return pl.ds(pl.multiple_of(j * BLK, BLK), BLK)

    def score(j, top, shift):
        rows = at(j)
        k_blk = k_ref[rows, :]
        out = []
        for h in range(2):
            tile = lax.dot_general(k_blk, qs[h], NT, preferred_element_type=F32)
            if shift is not None:
                key = lax.broadcasted_iota(jnp.int32, (BLK, BQ), 0) + shift
                qry = lax.broadcasted_iota(jnp.int32, (BLK, BQ), 1)
                tile = jnp.where(key <= qry, tile, -1e30)
            s_ref[h, rows, :] = tile
            out.append(jnp.maximum(top[h], fold_rows(jnp.max, tile)))
        return tuple(out)

    low = jnp.full((8, BQ), -1e30, F32)
    top = lax.fori_loop(0, per, lambda i, t: score(full + i, t, i * BLK), (low, low))
    top = lax.fori_loop(0, full, lambda j, t: score(j, t, None), top)
    top = [jnp.max(t, axis=0, keepdims=True) for t in top]

    def expo(j, tot):
        rows = at(j)
        out = []
        for h in range(2):
            tile = jnp.exp(s_ref[h, rows, :] - top[h])
            s_ref[h, rows, :] = tile
            out.append(tot[h] + fold_rows(jnp.sum, tile))
        return tuple(out)

    zero8 = jnp.zeros((8, BQ), F32)
    tot = lax.fori_loop(0, full + per, expo, (zero8, zero8))
    inv = [1.0 / jnp.sum(t, axis=0, keepdims=True) for t in tot]
    acc_ref[...] = jnp.zeros_like(acc_ref)

    def third(j, proj):
        rows = at(j)
        v_blk = v_ref[rows, :]
        proj_new = []
        for h in range(2):
            prob = s_ref[h, rows, :] * inv[h]
            s_ref[h, rows, :] = prob
            prob_lo = prob.astype(BF16)
            d_prob = lax.dot_general(v_blk, dos[h], NT, preferred_element_type=F32)
            dp_ref[h, rows, :] = d_prob
            proj_new.append(proj[h] + fold_rows(jnp.sum, prob * d_prob))
            dv_ref[rows, :] += jnp.dot(prob_lo, dos[h], preferred_element_type=F32)
            acc_ref[h] += jnp.dot(vt_ref[h * 64:(h + 1) * 64, rows], prob_lo, preferred_element_type=F32)
        return tuple(proj_new)

    proj = lax.fori_loop(0, full + per, third, (zero8, zero8))
    for h in range(2):
        ot_ref[h * 64:(h + 1) * 64, :] = acc_ref[h].astype(BF16)
    proj = [jnp.sum(t, axis=0, keepdims=True) for t in proj]
    acc_ref[...] = jnp.zeros_like(acc_ref)

    def fourth(j, none):
        rows = at(j)
        for h in range(2):
            d_s = (s_ref[h, rows, :] * (dp_ref[h, rows, :] - proj[h])).astype(BF16)
            dk_ref[rows, :] += jnp.dot(d_s, qs[h], preferred_element_type=F32)
            acc_ref[h] += jnp.dot(kt_ref[h * 64:(h + 1) * 64, rows], d_s, preferred_element_type=F32)
        return none

    lax.fori_loop(0, full + per, fourth, 0)
    dq = acc_ref[...].reshape(128, BQ) * 0.125
    dqkv_ref[pl.ds(pl.multiple_of(qi * BQ, BQ), BQ), 0:128] = dq.T.astype(BF16)

    @pl.when(step == last)
    def _():
        dqkv_ref[:, 128:256] = dk_ref[...].astype(BF16)
        dqkv_ref[:, 256:384] = dv_ref[...].astype(BF16)


def attn_pair(pair, qkv, d_attn):
    toks = qkv.shape[0]
    steps = toks // BQ
    return pl.pallas_call(
        attn_kernel,
        grid=(steps,),
        in_specs=[pl.BlockSpec((BQ, 128), lambda s: (steps - 1 - s, pair)),
                  pl.BlockSpec((toks, 128), lambda s: (0, 2 + pair)),
                  pl.BlockSpec((toks, 128), lambda s: (0, 4 + pair)),
                  pl.BlockSpec((BQ, 128), lambda s: (steps - 1 - s, pair))],
        out_specs=[pl.BlockSpec((128, BQ), lambda s: (0, steps - 1 - s)),
                   pl.BlockSpec((toks, 384), lambda s: (0, 0))],
        out_shape=[jax.ShapeDtypeStruct((128, toks), BF16), jax.ShapeDtypeStruct((toks, 384), BF16)],
        scratch_shapes=[pltpu.VMEM((2, toks, BQ), F32), pltpu.VMEM((2, toks, BQ), F32),
                        pltpu.VMEM((toks, 128), F32), pltpu.VMEM((toks, 128), F32),
                        pltpu.VMEM((128, toks), BF16), pltpu.VMEM((128, toks), BF16), pltpu.VMEM((2, 64, BQ), F32)],
        compiler_params=pltpu.CompilerParams(dimension_semantics=("arbitrary",), vmem_limit_bytes=30 << 20),
        cost_estimate=pl.CostEstimate(flops=16 * 10**9, bytes_accessed=4 << 20, transcendentals=0),
    )(qkv, qkv, qkv, d_attn)


def own_kernel(nh_ref, nl_ref, dy_ref, ah_ref, al_ref, ph_ref, pl_ref, gu_ref, gd_ref, nt_ref, gt_ref, dp_ref):
    rows = nh_ref.shape[0]

    @pl.when(pl.program_id(0) == 0)
    def _():
        for i, ref in enumerate((nl_ref, nh_ref)):
            nt_ref[:, i * rows:(i + 1) * rows] = ref[...].T

    for i, (a_ref, p_ref) in enumerate(((al_ref, pl_ref), (ah_ref, ph_ref))):
        gt_ref[:, i * rows:(i + 1) * rows] = gelu_pair(a_ref[...])[0].astype(BF16).T
        dp_ref[i * rows:(i + 1) * rows, :] = p_ref[...]
    gu_ref[...] = jnp.dot(nt_ref[...], dp_ref[...], preferred_element_type=F32)
    gd_ref[...] = jnp.dot(gt_ref[...], dy_ref[...], preferred_element_type=F32)


def other_kernel(na_ref, nb_ref, da_ref, db_ref, wu_ref, wd_ref, pu_ref, pd_ref, gu_ref, gd_ref, nt_ref, gt_ref, dp_ref):
    rows = na_ref.shape[0]

    @pl.when(pl.program_id(0) == 0)
    def _():
        for i, ref in enumerate((na_ref, nb_ref)):
            nt_ref[:, i * rows:(i + 1) * rows] = ref[...].T

    sub = rows // 2
    for i, (n_ref, d_ref) in enumerate(((na_ref, da_ref), (nb_ref, db_ref))):
        for r in range(2):
            sl = slice(r * sub, (r + 1) * sub)
            at = slice(i * rows + r * sub, i * rows + (r + 1) * sub)
            act, slope = gelu_pair(jnp.dot(n_ref[sl, :], wu_ref[...], preferred_element_type=F32).astype(BF16))
            d_act = lax.dot_general(d_ref[sl, :], wd_ref[...], NT, preferred_element_type=F32)
            dp_ref[at, :] = (d_act * slope).astype(BF16)
            gt_ref[:, at] = act.astype(BF16).T
    gu_ref[...] = (jnp.dot(nt_ref[...], dp_ref[...], preferred_element_type=F32) + pu_ref[...]).astype(BF16)
    total = jnp.dot(gt_ref[:, :rows], da_ref[...], preferred_element_type=F32)
    total += jnp.dot(gt_ref[:, rows:], db_ref[...], preferred_element_type=F32)
    gd_ref[...] = (total + pd_ref[...]).astype(BF16)


def mlp_columns(kernel, whole, by_col, by_row, dim, cols, rows, out_type):
    once = lambda a: pl.BlockSpec(a.shape, lambda s: (0, 0), pipeline_mode=pl.Buffered(1))
    col = lambda n: pl.BlockSpec((n, BLK), lambda s: (0, s))
    row = lambda n: pl.BlockSpec((BLK, n), lambda s: (s, 0))
    args = whole + by_col[:1] + by_row[:1] + by_col[1:] + by_row[1:] if by_row else whole + by_col
    specs = [col(a.shape[0]) for a in by_col[:1]] + [row(a.shape[1]) for a in by_row[:1]] + [col(a.shape[0]) for a in by_col[1:]] + [row(a.shape[1]) for a in by_row[1:]]
    return pl.pallas_call(
        kernel,
        grid=(cols // BLK,),
        in_specs=[once(a) for a in whole] + specs,
        out_specs=[col(dim), row(dim)],
        out_shape=[jax.ShapeDtypeStruct((dim, cols), out_type), jax.ShapeDtypeStruct((cols, dim), out_type)],
        scratch_shapes=[pltpu.VMEM((dim, rows), BF16), pltpu.VMEM((BLK, rows), BF16), pltpu.VMEM((rows, BLK), BF16)],
        compiler_params=pltpu.CompilerParams(dimension_semantics=("arbitrary",), vmem_limit_bytes=36 << 20),
        cost_estimate=pl.CostEstimate(flops=16 * 10**9, bytes_accessed=14 << 20, transcendentals=0),
    )(*args)


HALVES = (('hi', 1), ('lo', 0))


def solution(mesh):
    row_spec = P(('pod', 'dp'), None)
    stat_spec = P(('pod', 'dp'))
    in_specs = (row_spec, row_spec, stat_spec, stat_spec, stat_spec, stat_spec, P(None), P(None), row_spec,
                P(None, None, 'tp', None), P('tp', None, None), P(None, 'tp'), P('tp', None))
    out_specs = (row_spec, P('pod', None, 'tp', None), P(('pod', 'tp'), None, None), P('pod', 'tp'), P(('pod', 'tp'), None))

    def swap(kind, arr):
        axis, perm = {'c': ('tp', [(0, 1), (1, 0), (2, 3), (3, 2)]), 'x': ('tp', [(0, 2), (2, 0), (1, 3), (3, 1)]),
                      'y': ('dp', [(0, 1), (1, 0)])}[kind]
        return lax.ppermute(arr, axis, perm)

    def take_half(arr, which):
        rows = arr.shape[0] // 2
        return lax.dynamic_slice_in_dim(arr, which * rows, rows, 0)

    def join_halves(mine, other, which):
        return jnp.concatenate([jnp.where(which == 0, mine, other), jnp.where(which == 0, other, mine)], axis=0)

    def inner(x_saved, h_saved, mean_one, rstd_one, mean_two, rstd_two, gain_one, gain_two, grad_y, w_qkv, w_proj, w_up, w_down):
        core = lax.axis_index('tp') % 2
        dp_idx = lax.axis_index('dp')
        toks, dim = x_saved.shape
        part_of = lambda arr, i: arr[i * (toks // 2):(i + 1) * (toks // 2)]
        own_rows = lambda arr, i: lax.dynamic_slice_in_dim(arr, i * (toks // 2) + core * (toks // 4), toks // 4, 0)

        n_mine = layer_norm(take_half(h_saved, core), take_half(mean_two, core), take_half(rstd_two, core), gain_two)[1]
        norm_y, dy_y = swap('y', n_mine), swap('y', take_half(grad_y, core))
        norm_c, dy_c = swap('c', norm_y), swap('c', dy_y)

        def tp_sum(part):
            chip = (take_half(part, core).astype(F32) + swap('c', take_half(part, 1 - core)).astype(F32)).astype(BF16)
            return chip.astype(F32) + swap('x', chip).astype(F32)

        def back(total, rows, mean, rstd, gain):
            hat = (rows.astype(F32) - mean[:, None]) * rstd[:, None]
            return norm_back(total, hat, rstd, gain)

        norm_two, pre, d_pre, d_norm = {}, {}, {}, {}
        for tag, i in HALVES:
            norm_two[tag] = layer_norm(part_of(h_saved, i), part_of(mean_two, i), part_of(rstd_two, i), gain_two)[1]
            pre_act = jnp.dot(norm_two[tag], w_up, preferred_element_type=F32).astype(BF16)
            pre[tag] = pre_act
            gelu_slope = gelu_pair(pre_act)[1]
            d_pre[tag] = (lax.dot_general(part_of(grad_y, i), w_down, NT, preferred_element_type=F32) * gelu_slope).astype(BF16)
            part = lax.dot_general(d_pre[tag], w_up, NT, preferred_element_type=F32).astype(BF16)
            d_norm[tag] = tp_sum(part)

        part_up, part_down = mlp_columns(own_kernel, [norm_two['hi'], norm_two['lo'], grad_y],
                                         [pre['hi'], pre['lo'], d_pre['hi'], d_pre['lo']], [], dim, w_up.shape[1], toks, F32)
        w_t = w_qkv.transpose(1, 2, 3, 0).reshape(-1, dim)
        norm_one = layer_norm(x_saved, mean_one, rstd_one, gain_one)[1]
        qkv = lax.dot_general(norm_one, w_t, NT, preferred_element_type=F32).astype(BF16)

        w_o = w_proj.reshape(-1, dim)
        d_mid, mid_lo, d_attn = {}, {}, {}
        for tag, i in HALVES:
            mine = [own_rows(a, i) for a in (grad_y, h_saved, mean_two, rstd_two)]
            if tag == 'lo':
                mine[2], mine[3], low = lax.optimization_barrier((mine[2], mine[3], low))
            d_mid[tag] = mine[0].astype(F32) + back(d_norm[tag], *mine[1:], gain_two)
            low = d_mid[tag].astype(BF16)
            mid_lo[tag] = join_halves(low, swap('c', low), core)
            d_attn[tag] = lax.dot_general(mid_lo[tag], w_o, NT, preferred_element_type=F32).astype(BF16)
        d_attn = jnp.concatenate([d_attn['lo'], d_attn['hi']], axis=0)
        mid_all = jnp.concatenate([mid_lo['lo'], mid_lo['hi']], axis=0)

        w_pairs = w_t.reshape(3, 2, 128, dim)
        halves, d_pair = [], []
        for pair in range(2):
            o_t, d_qkv = attn_pair(pair, qkv, d_attn)
            d_pair.append(d_qkv)
            g_qkv = lax.dot_general(d_qkv, norm_one, TN, preferred_element_type=F32)
            g_o = jnp.dot(o_t, mid_all, preferred_element_type=F32)
            mine = jnp.concatenate([take_half(g, dp_idx) for g in (g_qkv, g_o)], 0)
            theirs = jnp.concatenate([take_half(g, 1 - dp_idx) for g in (g_qkv, g_o)], 0)
            recv = swap('y', theirs)
            summed = (mine + recv).astype(BF16)
            other = swap('y', summed)
            halves.append((join_halves(summed[:192], other[:192], dp_idx), join_halves(summed[192:], other[192:], dp_idx)))

        w_pair = [w_pairs[:, p].reshape(-1, dim) for p in range(2)]
        part_one = jnp.dot(d_pair[0], w_pair[0], preferred_element_type=F32)
        grad_x = {}
        for tag, i in HALVES:
            part = (part_of(part_one, i) + jnp.dot(part_of(d_pair[1], i), w_pair[1], preferred_element_type=F32)).astype(BF16)
            total = tp_sum(part)
            mine = [own_rows(a, i) for a in (x_saved, mean_one, rstd_one)]
            if tag == 'lo':
                mine[1], mine[2], low = lax.optimization_barrier((mine[1], mine[2], low))
            low = (d_mid[tag] + back(total, *mine, gain_one)).astype(BF16)
            grad_x[tag] = join_halves(low, swap('c', low), core)
        grad_x = jnp.concatenate([grad_x['lo'], grad_x['hi']], axis=0)

        grad_up, grad_down = mlp_columns(other_kernel, [norm_y, norm_c, dy_y, dy_c], [w_up, part_up], [w_down, part_down],
                                         dim, w_up.shape[1], toks, BF16)
        g_t = jnp.stack([h[0].reshape(3, 2, 64, dim) for h in halves], axis=1).reshape(3, 4, 64, dim)
        grad_qkv = g_t.transpose(3, 0, 1, 2)
        grad_proj = jnp.concatenate([h[1] for h in halves], axis=0).reshape(4, 64, dim)
        return grad_x, grad_qkv, grad_proj, grad_up, grad_down

    return jax.shard_map(inner, mesh=mesh, in_specs=in_specs, out_specs=out_specs, check_vma=False)
```

```python
import math

import jax
import jax.numpy as jnp
from jax import lax
from jax.experimental import pallas as pl
from jax.experimental.pallas import tpu as pltpu
from jax.sharding import PartitionSpec as P


GELU_C = math.sqrt(2.0 / math.pi)
F32 = jnp.float32
BF16 = jnp.bfloat16
NT = (((1,), (1,)), ((), ()))
TN = (((0,), (0,)), ((), ()))
BLK = 256


def layer_norm(row_vals, row_mean, row_rstd, gain_vec):
    x_hat = (row_vals.astype(F32) - row_mean[:, None]) * row_rstd[:, None]
    return x_hat, (x_hat * gain_vec.astype(F32)).astype(BF16)


def norm_back(d_norm, x_hat, row_rstd, gain_vec):
    scaled = d_norm * gain_vec.astype(F32)
    scaled_mean = jnp.mean(scaled, axis=-1, keepdims=True)
    proj_mean = jnp.mean(scaled * x_hat, axis=-1, keepdims=True)
    return row_rstd[:, None] * (scaled - scaled_mean - x_hat * proj_mean)


def gelu_pair(pre_act):
    pre_wide = pre_act.astype(F32)
    tanh_val = jnp.tanh(GELU_C * (pre_wide + 0.044715 * pre_wide * pre_wide * pre_wide))
    gelu_val = 0.5 * pre_wide * (1.0 + tanh_val)
    gelu_slope = 0.5 * (1.0 + tanh_val) + 0.5 * pre_wide * (1.0 - tanh_val * tanh_val) * GELU_C * (1.0 + 0.134145 * pre_wide * pre_wide)
    return gelu_val, gelu_slope


def fold_rows(op, tile):
    return op(tile.reshape(tile.shape[0] // 8, 8, tile.shape[1]), axis=0)


BQ = 512


KT = 512


def attn_kernel(q_ref, k_ref, v_ref, do_ref, ot_ref, dqkv_ref, s_ref, dp_ref, dk_ref, dv_ref, kt_ref, vt_ref, acc_ref):
    step = pl.program_id(0)
    last = pl.num_programs(0) - 1
    qi = last - step
    per = BQ // KT
    full = qi * per

    @pl.when(step == 0)
    def _():
        dk_ref[...] = jnp.zeros_like(dk_ref)
        dv_ref[...] = jnp.zeros_like(dv_ref)
        kt_ref[...] = k_ref[...].T
        vt_ref[...] = v_ref[...].T

    lane = lax.broadcasted_iota(jnp.int32, (BQ, 128), 1)
    q_wide = q_ref[...].astype(F32) * 0.125
    do_wide = do_ref[...].astype(F32)
    qs, dos = [], []
    for h in range(2):
        keep = (lane < 64) if h == 0 else (lane >= 64)
        qs.append(jnp.where(keep, q_wide, 0.0).astype(BF16))
        dos.append(jnp.where(keep, do_wide, 0.0).astype(BF16))

    def at(j):
        return pl.ds(pl.multiple_of(j * KT, KT), KT)

    def score(j, top, shift):
        rows = at(j)
        k_blk = k_ref[rows, :]
        out = []
        for h in range(2):
            tile = lax.dot_general(k_blk, qs[h], NT, preferred_element_type=F32)
            if shift is not None:
                key = lax.broadcasted_iota(jnp.int32, (KT, BQ), 0) + shift
                qry = lax.broadcasted_iota(jnp.int32, (KT, BQ), 1)
                tile = jnp.where(key <= qry, tile, -1e30)
            s_ref[h, rows, :] = tile
            out.append(jnp.maximum(top[h], fold_rows(jnp.max, tile)))
        return tuple(out)

    low = jnp.full((8, BQ), -1e30, F32)
    top = lax.fori_loop(0, per, lambda i, t: score(full + i, t, i * KT), (low, low))
    top = lax.fori_loop(0, full, lambda j, t: score(j, t, None), top)
    top = [jnp.max(t, axis=0, keepdims=True) for t in top]

    def expo(j, tot):
        rows = at(j)
        out = []
        for h in range(2):
            tile = jnp.exp(s_ref[h, rows, :] - top[h])
            s_ref[h, rows, :] = tile
            out.append(tot[h] + fold_rows(jnp.sum, tile))
        return tuple(out)

    zero8 = jnp.zeros((8, BQ), F32)
    tot = lax.fori_loop(0, full + per, expo, (zero8, zero8))
    inv = [1.0 / jnp.sum(t, axis=0, keepdims=True) for t in tot]
    acc_ref[...] = jnp.zeros_like(acc_ref)

    def third(j, proj):
        rows = at(j)
        v_blk = v_ref[rows, :]
        proj_new = []
        for h in range(2):
            prob = s_ref[h, rows, :] * inv[h]
            s_ref[h, rows, :] = prob
            prob_lo = prob.astype(BF16)
            d_prob = lax.dot_general(v_blk, dos[h], NT, preferred_element_type=F32)
            dp_ref[h, rows, :] = d_prob
            proj_new.append(proj[h] + fold_rows(jnp.sum, prob * d_prob))
            dv_ref[rows, :] += jnp.dot(prob_lo, dos[h], preferred_element_type=F32)
            acc_ref[h] += jnp.dot(vt_ref[h * 64:(h + 1) * 64, rows], prob_lo, preferred_element_type=F32)
        return tuple(proj_new)

    proj = lax.fori_loop(0, full + per, third, (zero8, zero8))
    for h in range(2):
        ot_ref[h * 64:(h + 1) * 64, :] = acc_ref[h].astype(BF16)
    proj = [jnp.sum(t, axis=0, keepdims=True) for t in proj]
    acc_ref[...] = jnp.zeros_like(acc_ref)

    def fourth(j, none):
        rows = at(j)
        for h in range(2):
            d_s = (s_ref[h, rows, :] * (dp_ref[h, rows, :] - proj[h])).astype(BF16)
            dk_ref[rows, :] += jnp.dot(d_s, qs[h], preferred_element_type=F32)
            acc_ref[h] += jnp.dot(kt_ref[h * 64:(h + 1) * 64, rows], d_s, preferred_element_type=F32)
        return none

    lax.fori_loop(0, full + per, fourth, 0)
    dq = acc_ref[...].reshape(128, BQ) * 0.125
    dqkv_ref[pl.ds(pl.multiple_of(qi * BQ, BQ), BQ), 0:128] = dq.T.astype(BF16)

    @pl.when(step == last)
    def _():
        dqkv_ref[:, 128:256] = dk_ref[...].astype(BF16)
        dqkv_ref[:, 256:384] = dv_ref[...].astype(BF16)


def attn_pair(pair, qkv, d_attn):
    toks = qkv.shape[0]
    steps = toks // BQ
    return pl.pallas_call(
        attn_kernel,
        grid=(steps,),
        in_specs=[pl.BlockSpec((BQ, 128), lambda s: (steps - 1 - s, pair)),
                  pl.BlockSpec((toks, 128), lambda s: (0, 2 + pair)),
                  pl.BlockSpec((toks, 128), lambda s: (0, 4 + pair)),
                  pl.BlockSpec((BQ, 128), lambda s: (steps - 1 - s, pair))],
        out_specs=[pl.BlockSpec((128, BQ), lambda s: (0, steps - 1 - s)),
                   pl.BlockSpec((toks, 384), lambda s: (0, 0))],
        out_shape=[jax.ShapeDtypeStruct((128, toks), BF16), jax.ShapeDtypeStruct((toks, 384), BF16)],
        scratch_shapes=[pltpu.VMEM((2, toks, BQ), F32), pltpu.VMEM((2, toks, BQ), F32),
                        pltpu.VMEM((toks, 128), F32), pltpu.VMEM((toks, 128), F32),
                        pltpu.VMEM((128, toks), BF16), pltpu.VMEM((128, toks), BF16), pltpu.VMEM((2, 64, BQ), F32)],
        compiler_params=pltpu.CompilerParams(dimension_semantics=("arbitrary",), vmem_limit_bytes=30 << 20),
        cost_estimate=pl.CostEstimate(flops=16 * 10**9, bytes_accessed=4 << 20, transcendentals=0),
    )(qkv, qkv, qkv, d_attn)


def own_kernel(nh_ref, nl_ref, dy_ref, ah_ref, al_ref, ph_ref, pl_ref, gu_ref, gd_ref, nt_ref, gt_ref, dp_ref):
    rows = nh_ref.shape[0]

    @pl.when(pl.program_id(0) == 0)
    def _():
        for i, ref in enumerate((nl_ref, nh_ref)):
            nt_ref[:, i * rows:(i + 1) * rows] = ref[...].T

    for i, (a_ref, p_ref) in enumerate(((al_ref, pl_ref), (ah_ref, ph_ref))):
        gt_ref[:, i * rows:(i + 1) * rows] = gelu_pair(a_ref[...])[0].astype(BF16).T
        dp_ref[i * rows:(i + 1) * rows, :] = p_ref[...]
    gu_ref[...] = jnp.dot(nt_ref[...], dp_ref[...], preferred_element_type=F32)
    gd_ref[...] = jnp.dot(gt_ref[...], dy_ref[...], preferred_element_type=F32)


def other_kernel(na_ref, nb_ref, da_ref, db_ref, wu_ref, wd_ref, pu_ref, pd_ref, gu_ref, gd_ref, nt_ref, gt_ref, dp_ref):
    rows = na_ref.shape[0]

    @pl.when(pl.program_id(0) == 0)
    def _():
        for i, ref in enumerate((na_ref, nb_ref)):
            nt_ref[:, i * rows:(i + 1) * rows] = ref[...].T

    sub = rows // 2
    for i, (n_ref, d_ref) in enumerate(((na_ref, da_ref), (nb_ref, db_ref))):
        for r in range(2):
            sl = slice(r * sub, (r + 1) * sub)
            at = slice(i * rows + r * sub, i * rows + (r + 1) * sub)
            act, slope = gelu_pair(jnp.dot(n_ref[sl, :], wu_ref[...], preferred_element_type=F32).astype(BF16))
            d_act = lax.dot_general(d_ref[sl, :], wd_ref[...], NT, preferred_element_type=F32)
            dp_ref[at, :] = (d_act * slope).astype(BF16)
            gt_ref[:, at] = act.astype(BF16).T
    gu_ref[...] = (jnp.dot(nt_ref[...], dp_ref[...], preferred_element_type=F32) + pu_ref[...]).astype(BF16)
    total = jnp.dot(gt_ref[:, :rows], da_ref[...], preferred_element_type=F32)
    total += jnp.dot(gt_ref[:, rows:], db_ref[...], preferred_element_type=F32)
    gd_ref[...] = (total + pd_ref[...]).astype(BF16)


def mlp_columns(kernel, whole, by_col, by_row, dim, cols, rows, out_type):
    once = lambda a: pl.BlockSpec(a.shape, lambda s: (0, 0), pipeline_mode=pl.Buffered(1))
    col = lambda n: pl.BlockSpec((n, BLK), lambda s: (0, s))
    row = lambda n: pl.BlockSpec((BLK, n), lambda s: (s, 0))
    args = whole + by_col[:1] + by_row[:1] + by_col[1:] + by_row[1:] if by_row else whole + by_col
    specs = [col(a.shape[0]) for a in by_col[:1]] + [row(a.shape[1]) for a in by_row[:1]] + [col(a.shape[0]) for a in by_col[1:]] + [row(a.shape[1]) for a in by_row[1:]]
    return pl.pallas_call(
        kernel,
        grid=(cols // BLK,),
        in_specs=[once(a) for a in whole] + specs,
        out_specs=[col(dim), row(dim)],
        out_shape=[jax.ShapeDtypeStruct((dim, cols), out_type), jax.ShapeDtypeStruct((cols, dim), out_type)],
        scratch_shapes=[pltpu.VMEM((dim, rows), BF16), pltpu.VMEM((BLK, rows), BF16), pltpu.VMEM((rows, BLK), BF16)],
        compiler_params=pltpu.CompilerParams(dimension_semantics=("arbitrary",), vmem_limit_bytes=36 << 20),
        cost_estimate=pl.CostEstimate(flops=16 * 10**9, bytes_accessed=14 << 20, transcendentals=0),
    )(*args)


HALVES = (('hi', 1), ('lo', 0))


def solution(mesh):
    row_spec = P(('pod', 'dp'), None)
    stat_spec = P(('pod', 'dp'))
    in_specs = (row_spec, row_spec, stat_spec, stat_spec, stat_spec, stat_spec, P(None), P(None), row_spec,
                P(None, None, 'tp', None), P('tp', None, None), P(None, 'tp'), P('tp', None))
    out_specs = (row_spec, P('pod', None, 'tp', None), P(('pod', 'tp'), None, None), P('pod', 'tp'), P(('pod', 'tp'), None))

    def swap(kind, arr):
        axis, perm = {'c': ('tp', [(0, 1), (1, 0), (2, 3), (3, 2)]), 'x': ('tp', [(0, 2), (2, 0), (1, 3), (3, 1)]),
                      'y': ('dp', [(0, 1), (1, 0)])}[kind]
        return lax.ppermute(arr, axis, perm)

    def take_half(arr, which):
        rows = arr.shape[0] // 2
        return lax.dynamic_slice_in_dim(arr, which * rows, rows, 0)

    def join_halves(mine, other, which):
        return jnp.concatenate([jnp.where(which == 0, mine, other), jnp.where(which == 0, other, mine)], axis=0)

    def inner(x_saved, h_saved, mean_one, rstd_one, mean_two, rstd_two, gain_one, gain_two, grad_y, w_qkv, w_proj, w_up, w_down):
        core = lax.axis_index('tp') % 2
        dp_idx = lax.axis_index('dp')
        toks, dim = x_saved.shape
        part_of = lambda arr, i: arr[i * (toks // 2):(i + 1) * (toks // 2)]
        own_rows = lambda arr, i: lax.dynamic_slice_in_dim(arr, i * (toks // 2) + core * (toks // 4), toks // 4, 0)

        n_mine = layer_norm(take_half(h_saved, core), take_half(mean_two, core), take_half(rstd_two, core), gain_two)[1]
        norm_y, dy_y = swap('y', n_mine), swap('y', take_half(grad_y, core))
        norm_c, dy_c = swap('c', norm_y), swap('c', dy_y)

        def tp_sum(part):
            chip = (take_half(part, core).astype(F32) + swap('c', take_half(part, 1 - core)).astype(F32)).astype(BF16)
            return chip.astype(F32) + swap('x', chip).astype(F32)

        def back(total, rows, mean, rstd, gain):
            hat = (rows.astype(F32) - mean[:, None]) * rstd[:, None]
            return norm_back(total, hat, rstd, gain)

        norm_two, pre, d_pre, d_norm = {}, {}, {}, {}
        for tag, i in HALVES:
            norm_two[tag] = layer_norm(part_of(h_saved, i), part_of(mean_two, i), part_of(rstd_two, i), gain_two)[1]
            pre_act = jnp.dot(norm_two[tag], w_up, preferred_element_type=F32).astype(BF16)
            pre[tag] = pre_act
            gelu_slope = gelu_pair(pre_act)[1]
            d_pre[tag] = (lax.dot_general(part_of(grad_y, i), w_down, NT, preferred_element_type=F32) * gelu_slope).astype(BF16)
            part = lax.dot_general(d_pre[tag], w_up, NT, preferred_element_type=F32).astype(BF16)
            d_norm[tag] = tp_sum(part)

        part_up, part_down = mlp_columns(own_kernel, [norm_two['hi'], norm_two['lo'], grad_y],
                                         [pre['hi'], pre['lo'], d_pre['hi'], d_pre['lo']], [], dim, w_up.shape[1], toks, F32)
        w_t = w_qkv.transpose(1, 2, 3, 0).reshape(-1, dim)
        norm_one = layer_norm(x_saved, mean_one, rstd_one, gain_one)[1]
        qkv = lax.dot_general(norm_one, w_t, NT, preferred_element_type=F32).astype(BF16)

        w_o = w_proj.reshape(-1, dim)
        d_mid, mid_lo, d_attn = {}, {}, {}
        for tag, i in HALVES:
            mine = [own_rows(a, i) for a in (grad_y, h_saved, mean_two, rstd_two)]
            if tag == 'lo':
                mine[2], mine[3], low = lax.optimization_barrier((mine[2], mine[3], low))
            d_mid[tag] = mine[0].astype(F32) + back(d_norm[tag], *mine[1:], gain_two)
            low = d_mid[tag].astype(BF16)
            mid_lo[tag] = join_halves(low, swap('c', low), core)
            d_attn[tag] = lax.dot_general(mid_lo[tag], w_o, NT, preferred_element_type=F32).astype(BF16)
        d_attn = jnp.concatenate([d_attn['lo'], d_attn['hi']], axis=0)
        mid_all = jnp.concatenate([mid_lo['lo'], mid_lo['hi']], axis=0)

        w_pairs = w_t.reshape(3, 2, 128, dim)
        halves, d_pair = [], []
        for pair in range(2):
            o_t, d_qkv = attn_pair(pair, qkv, d_attn)
            d_pair.append(d_qkv)
            g_qkv = lax.dot_general(d_qkv, norm_one, TN, preferred_element_type=F32)
            g_o = jnp.dot(o_t, mid_all, preferred_element_type=F32)
            mine = jnp.concatenate([take_half(g, dp_idx) for g in (g_qkv, g_o)], 0)
            theirs = jnp.concatenate([take_half(g, 1 - dp_idx) for g in (g_qkv, g_o)], 0)
            recv = swap('y', theirs)
            summed = (mine + recv).astype(BF16)
            other = swap('y', summed)
            halves.append((join_halves(summed[:192], other[:192], dp_idx), join_halves(summed[192:], other[192:], dp_idx)))

        w_pair = [w_pairs[:, p].reshape(-1, dim) for p in range(2)]
        part_one = jnp.dot(d_pair[0], w_pair[0], preferred_element_type=F32)
        grad_x = {}
        for tag, i in HALVES:
            part = (part_of(part_one, i) + jnp.dot(part_of(d_pair[1], i), w_pair[1], preferred_element_type=F32)).astype(BF16)
            total = tp_sum(part)
            mine = [own_rows(a, i) for a in (x_saved, mean_one, rstd_one)]
            if tag == 'lo':
                mine[1], mine[2], low = lax.optimization_barrier((mine[1], mine[2], low))
            low = (d_mid[tag] + back(total, *mine, gain_one)).astype(BF16)
            grad_x[tag] = join_halves(low, swap('c', low), core)
        grad_x = jnp.concatenate([grad_x['lo'], grad_x['hi']], axis=0)

        grad_up, grad_down = mlp_columns(other_kernel, [norm_y, norm_c, dy_y, dy_c], [w_up, part_up], [w_down, part_down],
                                         dim, w_up.shape[1], toks, BF16)
        g_t = jnp.stack([h[0].reshape(3, 2, 64, dim) for h in halves], axis=1).reshape(3, 4, 64, dim)
        grad_qkv = g_t.transpose(3, 0, 1, 2)
        grad_proj = jnp.concatenate([h[1] for h in halves], axis=0).reshape(4, 64, dim)
        return grad_x, grad_qkv, grad_proj, grad_up, grad_down

    return jax.shard_map(inner, mesh=mesh, in_specs=in_specs, out_specs=out_specs, check_vma=False)
```

```python
import math

import jax
import jax.numpy as jnp
from jax import lax
from jax.experimental import pallas as pl
from jax.experimental.pallas import tpu as pltpu
from jax.sharding import PartitionSpec as P


GELU_C = math.sqrt(2.0 / math.pi)
F32 = jnp.float32
BF16 = jnp.bfloat16
NT = (((1,), (1,)), ((), ()))
TN = (((0,), (0,)), ((), ()))
BLK = 256


def layer_norm(row_vals, row_mean, row_rstd, gain_vec):
    x_hat = (row_vals.astype(F32) - row_mean[:, None]) * row_rstd[:, None]
    return x_hat, (x_hat * gain_vec.astype(F32)).astype(BF16)


def norm_back(d_norm, x_hat, row_rstd, gain_vec):
    scaled = d_norm * gain_vec.astype(F32)
    scaled_mean = jnp.mean(scaled, axis=-1, keepdims=True)
    proj_mean = jnp.mean(scaled * x_hat, axis=-1, keepdims=True)
    return row_rstd[:, None] * (scaled - scaled_mean - x_hat * proj_mean)


def gelu_pair(pre_act):
    pre_wide = pre_act.astype(F32)
    tanh_val = jnp.tanh(GELU_C * (pre_wide + 0.044715 * pre_wide * pre_wide * pre_wide))
    gelu_val = 0.5 * pre_wide * (1.0 + tanh_val)
    gelu_slope = 0.5 * (1.0 + tanh_val) + 0.5 * pre_wide * (1.0 - tanh_val * tanh_val) * GELU_C * (1.0 + 0.134145 * pre_wide * pre_wide)
    return gelu_val, gelu_slope


def fold_rows(op, tile):
    return op(tile.reshape(tile.shape[0] // 8, 8, tile.shape[1]), axis=0)


BQ = 512


KT = 512


def attn_kernel(q_ref, k_ref, v_ref, do_ref, ot_ref, dqkv_ref, s_ref, dp_ref, dk_ref, dv_ref, kt_ref, vt_ref, acc_ref):
    step = pl.program_id(0)
    last = pl.num_programs(0) - 1
    qi = last - step
    per = BQ // KT
    full = qi * per

    @pl.when(step == 0)
    def _():
        dk_ref[...] = jnp.zeros_like(dk_ref)
        dv_ref[...] = jnp.zeros_like(dv_ref)
        kt_ref[...] = k_ref[...].T
        vt_ref[...] = v_ref[...].T

    lane = lax.broadcasted_iota(jnp.int32, (BQ, 128), 1)
    q_wide = q_ref[...].astype(F32) * 0.125
    do_wide = do_ref[...].astype(F32)
    qs, dos = [], []
    for h in range(2):
        keep = (lane < 64) if h == 0 else (lane >= 64)
        qs.append(jnp.where(keep, q_wide, 0.0).astype(BF16))
        dos.append(jnp.where(keep, do_wide, 0.0).astype(BF16))

    def at(j):
        return pl.ds(pl.multiple_of(j * KT, KT), KT)

    def score(j, top, shift):
        rows = at(j)
        k_blk = k_ref[rows, :]
        out = []
        for h in range(2):
            tile = lax.dot_general(k_blk, qs[h], NT, preferred_element_type=F32)
            if shift is not None:
                key = lax.broadcasted_iota(jnp.int32, (KT, BQ), 0) + shift
                qry = lax.broadcasted_iota(jnp.int32, (KT, BQ), 1)
                tile = jnp.where(key <= qry, tile, -1e30)
            s_ref[h, rows, :] = tile
            out.append(jnp.maximum(top[h], fold_rows(jnp.max, tile)))
        return tuple(out)

    low = jnp.full((8, BQ), -1e30, F32)
    top = lax.fori_loop(0, per, lambda i, t: score(full + i, t, i * KT), (low, low))
    top = lax.fori_loop(0, full, lambda j, t: score(j, t, None), top)
    top = [jnp.max(t, axis=0, keepdims=True) for t in top]

    def expo(j, tot):
        rows = at(j)
        out = []
        for h in range(2):
            tile = jnp.exp(s_ref[h, rows, :] - top[h])
            s_ref[h, rows, :] = tile
            out.append(tot[h] + fold_rows(jnp.sum, tile))
        return tuple(out)

    zero8 = jnp.zeros((8, BQ), F32)
    tot = lax.fori_loop(0, full + per, expo, (zero8, zero8))
    inv = [1.0 / jnp.sum(t, axis=0, keepdims=True) for t in tot]
    acc_ref[...] = jnp.zeros_like(acc_ref)

    def third(j, proj):
        rows = at(j)
        v_blk = v_ref[rows, :]
        proj_new = []
        for h in range(2):
            prob = s_ref[h, rows, :] * inv[h]
            s_ref[h, rows, :] = prob
            prob_lo = prob.astype(BF16)
            d_prob = lax.dot_general(v_blk, dos[h], NT, preferred_element_type=F32)
            dp_ref[h, rows, :] = d_prob
            proj_new.append(proj[h] + fold_rows(jnp.sum, prob * d_prob))
            dv_ref[rows, :] += jnp.dot(prob_lo, dos[h], preferred_element_type=F32)
            acc_ref[h] += jnp.dot(vt_ref[h * 64:(h + 1) * 64, rows], prob_lo, preferred_element_type=F32)
        return tuple(proj_new)

    proj = lax.fori_loop(0, full + per, third, (zero8, zero8))
    for h in range(2):
        ot_ref[h * 64:(h + 1) * 64, :] = acc_ref[h].astype(BF16)
    proj = [jnp.sum(t, axis=0, keepdims=True) for t in proj]
    acc_ref[...] = jnp.zeros_like(acc_ref)

    def fourth(j, none):
        rows = at(j)
        for h in range(2):
            d_s = (s_ref[h, rows, :] * (dp_ref[h, rows, :] - proj[h])).astype(BF16)
            dk_ref[rows, :] += jnp.dot(d_s, qs[h], preferred_element_type=F32)
            acc_ref[h] += jnp.dot(kt_ref[h * 64:(h + 1) * 64, rows], d_s, preferred_element_type=F32)
        return none

    lax.fori_loop(0, full + per, fourth, 0)
    dq = acc_ref[...].reshape(128, BQ) * 0.125
    dqkv_ref[pl.ds(pl.multiple_of(qi * BQ, BQ), BQ), 0:128] = dq.T.astype(BF16)

    @pl.when(step == last)
    def _():
        dqkv_ref[:, 128:256] = dk_ref[...].astype(BF16)
        dqkv_ref[:, 256:384] = dv_ref[...].astype(BF16)


def attn_pair(pair, qkv, d_attn):
    toks = qkv.shape[0]
    steps = toks // BQ
    return pl.pallas_call(
        attn_kernel,
        grid=(steps,),
        in_specs=[pl.BlockSpec((BQ, 128), lambda s: (steps - 1 - s, pair)),
                  pl.BlockSpec((toks, 128), lambda s: (0, 2 + pair)),
                  pl.BlockSpec((toks, 128), lambda s: (0, 4 + pair)),
                  pl.BlockSpec((BQ, 128), lambda s: (steps - 1 - s, pair))],
        out_specs=[pl.BlockSpec((128, BQ), lambda s: (0, steps - 1 - s)),
                   pl.BlockSpec((toks, 384), lambda s: (0, 0))],
        out_shape=[jax.ShapeDtypeStruct((128, toks), BF16), jax.ShapeDtypeStruct((toks, 384), BF16)],
        scratch_shapes=[pltpu.VMEM((2, toks, BQ), F32), pltpu.VMEM((2, toks, BQ), F32),
                        pltpu.VMEM((toks, 128), F32), pltpu.VMEM((toks, 128), F32),
                        pltpu.VMEM((128, toks), BF16), pltpu.VMEM((128, toks), BF16), pltpu.VMEM((2, 64, BQ), F32)],
        compiler_params=pltpu.CompilerParams(dimension_semantics=("arbitrary",), vmem_limit_bytes=24 << 20),
        cost_estimate=pl.CostEstimate(flops=16 * 10**9, bytes_accessed=4 << 20, transcendentals=0),
    )(qkv, qkv, qkv, d_attn)


def own_kernel(nh_ref, nl_ref, dy_ref, ah_ref, al_ref, ph_ref, pl_ref, gu_ref, gd_ref, nt_ref, gt_ref, dp_ref):
    rows = nh_ref.shape[0]

    @pl.when(pl.program_id(0) == 0)
    def _():
        for i, ref in enumerate((nl_ref, nh_ref)):
            nt_ref[:, i * rows:(i + 1) * rows] = ref[...].T

    for i, (a_ref, p_ref) in enumerate(((al_ref, pl_ref), (ah_ref, ph_ref))):
        gt_ref[:, i * rows:(i + 1) * rows] = gelu_pair(a_ref[...])[0].astype(BF16).T
        dp_ref[i * rows:(i + 1) * rows, :] = p_ref[...]
    gu_ref[...] = jnp.dot(nt_ref[...], dp_ref[...], preferred_element_type=F32)
    gd_ref[...] = jnp.dot(gt_ref[...], dy_ref[...], preferred_element_type=F32)


def other_kernel(na_ref, nb_ref, da_ref, db_ref, wu_ref, wd_ref, pu_ref, pd_ref, gu_ref, gd_ref, nt_ref, gt_ref, dp_ref):
    rows = na_ref.shape[0]

    @pl.when(pl.program_id(0) == 0)
    def _():
        for i, ref in enumerate((na_ref, nb_ref)):
            nt_ref[:, i * rows:(i + 1) * rows] = ref[...].T

    sub = rows // 2
    for i, (n_ref, d_ref) in enumerate(((na_ref, da_ref), (nb_ref, db_ref))):
        for r in range(2):
            sl = slice(r * sub, (r + 1) * sub)
            at = slice(i * rows + r * sub, i * rows + (r + 1) * sub)
            act, slope = gelu_pair(jnp.dot(n_ref[sl, :], wu_ref[...], preferred_element_type=F32).astype(BF16))
            d_act = lax.dot_general(d_ref[sl, :], wd_ref[...], NT, preferred_element_type=F32)
            dp_ref[at, :] = (d_act * slope).astype(BF16)
            gt_ref[:, at] = act.astype(BF16).T
    gu_ref[...] = (jnp.dot(nt_ref[...], dp_ref[...], preferred_element_type=F32) + pu_ref[...]).astype(BF16)
    total = jnp.dot(gt_ref[:, :rows], da_ref[...], preferred_element_type=F32)
    total += jnp.dot(gt_ref[:, rows:], db_ref[...], preferred_element_type=F32)
    gd_ref[...] = (total + pd_ref[...]).astype(BF16)


def mlp_columns(kernel, whole, by_col, by_row, dim, cols, rows, out_type):
    once = lambda a: pl.BlockSpec(a.shape, lambda s: (0, 0), pipeline_mode=pl.Buffered(1))
    col = lambda n: pl.BlockSpec((n, BLK), lambda s: (0, s))
    row = lambda n: pl.BlockSpec((BLK, n), lambda s: (s, 0))
    args = whole + by_col[:1] + by_row[:1] + by_col[1:] + by_row[1:] if by_row else whole + by_col
    specs = [col(a.shape[0]) for a in by_col[:1]] + [row(a.shape[1]) for a in by_row[:1]] + [col(a.shape[0]) for a in by_col[1:]] + [row(a.shape[1]) for a in by_row[1:]]
    return pl.pallas_call(
        kernel,
        grid=(cols // BLK,),
        in_specs=[once(a) for a in whole] + specs,
        out_specs=[col(dim), row(dim)],
        out_shape=[jax.ShapeDtypeStruct((dim, cols), out_type), jax.ShapeDtypeStruct((cols, dim), out_type)],
        scratch_shapes=[pltpu.VMEM((dim, rows), BF16), pltpu.VMEM((BLK, rows), BF16), pltpu.VMEM((rows, BLK), BF16)],
        compiler_params=pltpu.CompilerParams(dimension_semantics=("arbitrary",), vmem_limit_bytes=30 << 20),
        cost_estimate=pl.CostEstimate(flops=16 * 10**9, bytes_accessed=14 << 20, transcendentals=0),
    )(*args)


HALVES = (('hi', 1), ('lo', 0))


def solution(mesh):
    row_spec = P(('pod', 'dp'), None)
    stat_spec = P(('pod', 'dp'))
    in_specs = (row_spec, row_spec, stat_spec, stat_spec, stat_spec, stat_spec, P(None), P(None), row_spec,
                P(None, None, 'tp', None), P('tp', None, None), P(None, 'tp'), P('tp', None))
    out_specs = (row_spec, P('pod', None, 'tp', None), P(('pod', 'tp'), None, None), P('pod', 'tp'), P(('pod', 'tp'), None))

    def swap(kind, arr):
        axis, perm = {'c': ('tp', [(0, 1), (1, 0), (2, 3), (3, 2)]), 'x': ('tp', [(0, 2), (2, 0), (1, 3), (3, 1)]),
                      'y': ('dp', [(0, 1), (1, 0)])}[kind]
        return lax.ppermute(arr, axis, perm)

    def take_half(arr, which):
        rows = arr.shape[0] // 2
        return lax.dynamic_slice_in_dim(arr, which * rows, rows, 0)

    def join_halves(mine, other, which):
        return jnp.concatenate([jnp.where(which == 0, mine, other), jnp.where(which == 0, other, mine)], axis=0)

    def inner(x_saved, h_saved, mean_one, rstd_one, mean_two, rstd_two, gain_one, gain_two, grad_y, w_qkv, w_proj, w_up, w_down):
        core = lax.axis_index('tp') % 2
        dp_idx = lax.axis_index('dp')
        toks, dim = x_saved.shape
        part_of = lambda arr, i: arr[i * (toks // 2):(i + 1) * (toks // 2)]
        own_rows = lambda arr, i: lax.dynamic_slice_in_dim(arr, i * (toks // 2) + core * (toks // 4), toks // 4, 0)

        n_mine = layer_norm(take_half(h_saved, core), take_half(mean_two, core), take_half(rstd_two, core), gain_two)[1]
        norm_y, dy_y = swap('y', n_mine), swap('y', take_half(grad_y, core))
        norm_c, dy_c = swap('c', norm_y), swap('c', dy_y)

        def tp_sum(part):
            chip = (take_half(part, core).astype(F32) + swap('c', take_half(part, 1 - core)).astype(F32)).astype(BF16)
            return chip.astype(F32) + swap('x', chip).astype(F32)

        def back(total, rows, mean, rstd, gain):
            hat = (rows.astype(F32) - mean[:, None]) * rstd[:, None]
            return norm_back(total, hat, rstd, gain)

        norm_two, pre, d_pre, d_norm = {}, {}, {}, {}
        for tag, i in HALVES:
            norm_two[tag] = layer_norm(part_of(h_saved, i), part_of(mean_two, i), part_of(rstd_two, i), gain_two)[1]
            pre_act = jnp.dot(norm_two[tag], w_up, preferred_element_type=F32).astype(BF16)
            pre[tag] = pre_act
            gelu_slope = gelu_pair(pre_act)[1]
            d_pre[tag] = (lax.dot_general(part_of(grad_y, i), w_down, NT, preferred_element_type=F32) * gelu_slope).astype(BF16)
            part = lax.dot_general(d_pre[tag], w_up, NT, preferred_element_type=F32).astype(BF16)
            d_norm[tag] = tp_sum(part)

        part_up, part_down = mlp_columns(own_kernel, [norm_two['hi'], norm_two['lo'], grad_y],
                                         [pre['hi'], pre['lo'], d_pre['hi'], d_pre['lo']], [], dim, w_up.shape[1], toks, F32)
        w_t = w_qkv.transpose(1, 2, 3, 0).reshape(-1, dim)
        norm_one = layer_norm(x_saved, mean_one, rstd_one, gain_one)[1]
        qkv = lax.dot_general(norm_one, w_t, NT, preferred_element_type=F32).astype(BF16)

        w_o = w_proj.reshape(-1, dim)
        d_mid, mid_lo, d_attn = {}, {}, {}
        for tag, i in HALVES:
            mine = [own_rows(a, i) for a in (grad_y, h_saved, mean_two, rstd_two)]
            if tag == 'lo':
                mine[2], mine[3], low = lax.optimization_barrier((mine[2], mine[3], low))
            d_mid[tag] = mine[0].astype(F32) + back(d_norm[tag], *mine[1:], gain_two)
            low = d_mid[tag].astype(BF16)
            mid_lo[tag] = join_halves(low, swap('c', low), core)
            d_attn[tag] = lax.dot_general(mid_lo[tag], w_o, NT, preferred_element_type=F32).astype(BF16)
        d_attn = jnp.concatenate([d_attn['lo'], d_attn['hi']], axis=0)
        mid_all = jnp.concatenate([mid_lo['lo'], mid_lo['hi']], axis=0)

        w_pairs = w_t.reshape(3, 2, 128, dim)
        d_pair = []
        grad_qkv, grad_proj = jnp.zeros((3, 4, 64, dim), BF16), jnp.zeros((4, 64, dim), BF16)
        for pair in range(2):
            o_t, d_qkv = attn_pair(pair, qkv, d_attn)
            d_pair.append(d_qkv)
            g_qkv = lax.dot_general(d_qkv, norm_one, TN, preferred_element_type=F32)
            g_o = jnp.dot(o_t, mid_all, preferred_element_type=F32)
            g_qkv, g_o = g_qkv.reshape(3, 2, 64, dim), g_o.reshape(2, 64, dim)
            pick = lambda d: jnp.concatenate([lax.dynamic_index_in_dim(g_qkv, d, 1, False).reshape(192, dim), lax.dynamic_index_in_dim(g_o, d, 0, False)], 0)
            mine, theirs = pick(dp_idx), pick(1 - dp_idx)
            recv = swap('y', theirs)
            summed = (mine + recv).astype(BF16)
            other = swap('y', summed)
            for part, d in ((summed, dp_idx), (other, 1 - dp_idx)):
                grad_qkv = lax.dynamic_update_slice(grad_qkv, part[:192].reshape(3, 1, 64, dim), (0, 2 * pair + d, 0, 0))
                grad_proj = lax.dynamic_update_slice(grad_proj, part[192:].reshape(1, 64, dim), (2 * pair + d, 0, 0))

        w_pair = [w_pairs[:, p].reshape(-1, dim) for p in range(2)]
        part_one = jnp.dot(d_pair[0], w_pair[0], preferred_element_type=F32)
        grad_x = jnp.zeros((toks, dim), BF16)
        for tag, i in HALVES:
            part = (part_of(part_one, i) + jnp.dot(part_of(d_pair[1], i), w_pair[1], preferred_element_type=F32)).astype(BF16)
            total = tp_sum(part)
            mine = [own_rows(a, i) for a in (x_saved, mean_one, rstd_one)]
            if tag == 'lo':
                mine[1], mine[2], low = lax.optimization_barrier((mine[1], mine[2], low))
            low = (d_mid[tag] + back(total, *mine, gain_one)).astype(BF16)
            for part, c in ((low, core), (swap('c', low), 1 - core)):
                grad_x = lax.dynamic_update_slice(grad_x, part, (i * (toks // 2) + c * (toks // 4), 0))

        grad_up, grad_down = mlp_columns(other_kernel, [norm_y, norm_c, dy_y, dy_c], [w_up, part_up], [w_down, part_down],
                                         dim, w_up.shape[1], toks, BF16)
        grad_qkv = grad_qkv.transpose(3, 0, 1, 2)
        return grad_x, grad_qkv, grad_proj, grad_up, grad_down

    return jax.shard_map(inner, mesh=mesh, in_specs=in_specs, out_specs=out_specs, check_vma=False)
```
